128 devices in a mesh: tok: 16 (over z_lo, y, core), blk: 8 (over x, z_hi).
Axes of the slice: x: 4, y: 4, z: 4 (z_hi: 2, z_lo: 2; z = z_hi * 2 + z_lo), core: 2. Of those that a mesh axis runs over, the one named last changes fastest.
Arguments:
- activations: bfloat16 [8192, 4096], P('tok', 'blk'), may hold values from -52 to 52, as said below
- out_grads: bfloat16 [8192, 4096], P('tok', 'blk'), may hold values from -52 to 52, as said below
Outputs:
- act_inverse: float32 [4096, 4096], P(('tok', 'blk'))
- grad_inverse: float32 [4096, 4096], P(('tok', 'blk'))
The draws below stay inside these ranges and needn't reach their ends.
Inputs may be any that keep to these rules, and one draw needn't show every extreme that they name: `activations`: real entries. `out_grads`: real entries.
All inputs are finite; a program needn't handle non-finite values.
Results may differ from the reference program's by a relative error of at most 0.02.
Values may be sent and summed in bfloat16 or wider, within the bound.
A program may use at most 64 MiB of HBM per device.

```python
import jax
import jax.numpy as jnp
from jax import lax

D = 4096
TOK_DEV = 512
TOKENS = 8192
N_TOK = 16


def scaled_draw(key):
    row_key, col_key, value_key = jax.random.split(key, 3)
    positions = jnp.arange(TOKENS, dtype=jnp.float32) / TOKENS
    values = jax.random.truncated_normal(value_key, -5.0, 5.0, (TOKENS, D), jnp.float32)
    row_scale = jnp.exp(jax.random.uniform(row_key, (TOKENS, 1), jnp.float32, 0.0, jnp.log(3.0)))
    ramp = jnp.exp(positions * 0.5 * jnp.log(3.0))
    col_scale = jnp.exp(jax.random.uniform(col_key, (1, D), jnp.float32, 0.0, jnp.log(10.0)))
    return values * row_scale * ramp[:, None] * col_scale / 10.0


def draw_activations(key, part):
    return scaled_draw(jax.random.fold_in(key, 11)).astype(jnp.bfloat16)


def draw_out_grads(key, part):
    return scaled_draw(jax.random.fold_in(key, 23)).astype(jnp.bfloat16)


def setup_inputs(seed: int = 0) -> dict:
    streams_of = jax.random.split(jax.random.key(seed), 3)
    activations = draw_activations(jax.random.fold_in(streams_of[2], 71), 0)
    out_grads = draw_out_grads(jax.random.fold_in(streams_of[2], 71), 0)
    return dict(activations=activations, out_grads=out_grads)


damping = 0.3
epsilon = 1e-06
divisor = 2.0

def factor_gram(data):
    shards = data.reshape(N_TOK, TOK_DEV, D)

    def add_shard(total, shard):
        partial_value = jnp.dot(shard.T, shard, preferred_element_type=jnp.float32)
        rounded = lax.optimization_barrier(partial_value.astype(jnp.bfloat16))
        return (total + rounded.astype(jnp.float32), None)
    total, unused = lax.scan(add_shard, jnp.zeros((D, D), jnp.float32), shards)
    return total

def factor_inverse(data):
    gram = factor_gram(data)
    values = data.astype(jnp.float32)
    sums = lax.optimization_barrier(jnp.sum(values * values, axis=0))
    inverse = lax.rsqrt(sums / TOKENS + epsilon)
    identity = jnp.eye(D, dtype=jnp.float32)
    damped = gram / TOKENS * inverse[:, None] * inverse[None, :] + damping * identity
    scaled = damped / divisor
    half = scaled.astype(jnp.bfloat16)
    square = jnp.dot(half, half, preferred_element_type=jnp.float32)
    cube = jnp.dot(half, square.astype(jnp.bfloat16), preferred_element_type=jnp.float32)
    return 4.0 * identity - 6.0 * scaled + 4.0 * square - cube

def reference(activations, out_grads):
    return (factor_inverse(activations), factor_inverse(out_grads))
```

```python
import jax
import jax.numpy as jnp
from jax import lax
from jax.experimental import pallas as pl
from jax.experimental.pallas import tpu as pltpu
from jax.sharding import PartitionSpec as P

D = 4096
TOKENS = 8192
BLOCK = 512
HALF = 256
QUARTER = 128

damping = 0.3
epsilon = 1e-06
divisor = 2.0

MESH = pl.DeviceIdType.MESH
F32 = jnp.float32
BF16 = jnp.bfloat16

X_ID = 0
D_ID = 5
Y1_ID = 9
Y2_ID = 11
Z_ID = 15
ROW_ID = 16
COL_ID = 25
SQ_ID = 44
OUT_ID = 63
N_ID = 71


class Gather:
    def __init__(self, send, wait, base, ref, plus, minus, across, via_z, pass_on=None):
        self.send, self.wait, self.base, self.ref = send, wait, base, ref
        self.plus, self.minus, self.across, self.via_z = plus, minus, across, via_z
        self.pass_on = pass_on

    def incoming(self, k):
        return [
            (3, 0, None), (1, 0, None), (0, 1, None), (2, 0, 0), (2, 0, 1),
            (3, 1, None), (1, 1, None), (2, 1, 0), (2, 1, 1),
        ][k]

    def put(self, k, place, to):
        r = self.ref(*place)
        self.send(self.base + k, r, r, to)

    def take(self, k):
        r = self.ref(*self.incoming(k))
        self.wait(self.base + k, r)
        if self.pass_on is not None:
            self.pass_on(self.base + 10 + k, r)

    def start(self):
        own = (0, 0, None)
        self.put(0, own, self.plus)
        self.put(1, own, self.minus)
        self.put(2, own, self.across)
        if self.pass_on is not None:
            self.pass_on(self.base + 9, self.ref(*own))

    def near(self):
        self.take(0)
        self.put(3, (3, 0, 0), self.plus)
        self.take(1)
        self.put(4, (1, 0, 1), self.minus)

    def other(self):
        self.take(2)
        self.put(5, (0, 1, None), self.plus)
        self.put(6, (0, 1, None), self.minus)

    def far(self):
        if self.via_z:
            self.take(3)
            self.put(7, (2, 0, 0), self.across)
            self.take(4)
            self.put(8, (2, 0, 1), self.across)
        else:
            self.take(5)
            self.put(7, (3, 1, 0), self.plus)
            self.take(6)
            self.put(8, (1, 1, 1), self.minus)

    def finish(self):
        for k in (5, 6, 7, 8) if self.via_z else (3, 4, 7, 8):
            self.take(k)


def kernel(
    act_ref, grad_ref, act_out, grad_out,
    xbuf, zbuf, pown, dsend, drecv, y1s, y1r, y2s, y2r, tot, zs, zr, scaled,
    rowbuf, colbuf, sqrow, sqcol, sq, obuf, orecv, csend, crecv, totbuf,
    ssem, rsem, csem, crsem, tsem, trsem, lsem,
):
    tok, blk = lax.axis_index("tok"), lax.axis_index("blk")
    c, y, zl = tok % 2, (tok // 2) % 4, tok // 8
    x, zh = blk // 2, blk % 2

    def tok_of(zl_, y_, c_):
        return zl_ * 8 + y_ * 2 + c_

    def blk_of(x_, zh_):
        return x_ * 2 + zh_

    x_plus = (tok, blk_of((x + 1) % 4, zh))
    x_minus = (tok, blk_of((x + 3) % 4, zh))
    zh_mate = (tok, blk_of(x, 1 - zh))
    y_plus = (tok_of(zl, (y + 1) % 4, c), blk)
    y_minus = (tok_of(zl, (y + 3) % 4, c), blk)
    zl_mate = (tok_of(1 - zl, y, c), blk)
    sibling = (tok_of(zl, y, 1 - c), blk)

    def place(to):
        return {"tok": to[0], "blk": to[1]}

    out_tok = 4 * y + 2 * zh + c
    home = out_tok == tok
    phi = 2 * x + zl
    row_block = 2 * y + zh

    barrier = pltpu.get_barrier_semaphore()

    def greet_tok(j, carry):
        pl.semaphore_signal(
            barrier, inc=1, device_id=place(((tok + j) % 16, blk)), device_id_type=MESH
        )
        return carry

    def greet_blk(j, carry):
        pl.semaphore_signal(
            barrier, inc=1, device_id=place((tok, (blk + j) % 8)), device_id_type=MESH
        )
        return carry

    lax.fori_loop(1, 16, greet_tok, 0)
    lax.fori_loop(1, 8, greet_blk, 0)

    def source_of(j):
        return (tok_of(j % 2, tok // 4, c), blk_of(j // 2, (tok // 2) % 2))

    def greet_source(j, carry):
        to = source_of(j)
        me = (to[0] == tok) & (to[1] == blk)

        @pl.when(jnp.logical_not(me))
        def _():
            pl.semaphore_signal(barrier, inc=1, device_id=place(to), device_id_type=MESH)

        return carry

    lax.fori_loop(0, 8, greet_source, 0)

    def load_own(f):
        return pltpu.make_async_copy((act_ref, grad_ref)[f], xbuf.at[f, x], lsem.at[f])

    load_own(0).start()
    load_own(1).start()
    pl.semaphore_wait(barrier, 15 + 7 + 8 - home.astype(jnp.int32))

    sent = []

    def sender(f):
        def send(k, src, dst, to):
            copy = pltpu.make_async_remote_copy(
                src_ref=src, dst_ref=dst, send_sem=ssem.at[f, k], recv_sem=rsem.at[f, k],
                device_id=place(to), device_id_type=MESH,
            )
            copy.start()
            sent.append(copy)

        return send

    def waiter(f):
        def wait(k, dst):
            pltpu.make_async_remote_copy(
                src_ref=dst, dst_ref=dst, send_sem=ssem.at[f, k], recv_sem=rsem.at[f, k],
                device_id=place(sibling), device_id_type=MESH,
            ).wait_recv()

        return wait

    sends, waits = (sender(0), sender(1)), (waiter(0), waiter(1))
    low, high = pl.ds(0, HALF), pl.ds(HALF, HALF)

    def x_start(f):
        own = xbuf.at[f, x]
        sends[f](X_ID + 0, own, own, x_plus)
        sends[f](X_ID + 1, own, own, x_minus)
        sends[f](X_ID + 2, own, zbuf.at[f], zh_mate)

    def x_forward(f):
        left, right = (x + 3) % 4, (x + 1) % 4
        waits[f](X_ID + 0, xbuf.at[f, left])
        part = xbuf.at[f, left, low]
        sends[f](X_ID + 3, part, part, x_plus)
        waits[f](X_ID + 1, xbuf.at[f, right])
        part = xbuf.at[f, right, high]
        sends[f](X_ID + 4, part, part, x_minus)

    def x_finish(f):
        far = (x + 2) % 4
        waits[f](X_ID + 2, zbuf.at[f])
        waits[f](X_ID + 3, xbuf.at[f, far, low])
        waits[f](X_ID + 4, xbuf.at[f, far, high])

    def column_sums(f):
        values = xbuf[f, x].astype(F32)
        csend[f : f + 1, :] = jnp.sum(values * values, axis=0, keepdims=True)

    def sum_copy(j):
        return pltpu.make_async_remote_copy(
            src_ref=csend, dst_ref=crecv.at[j], send_sem=csem.at[j], recv_sem=crsem.at[j],
            device_id=place(((tok + j) % 16, blk)), device_id_type=MESH,
        )

    def sums_start():
        def step(j, carry):
            sum_copy(j).start()
            return carry

        lax.fori_loop(1, 16, step, 0)

    total_to = [(tok, blk_of((x + j) % 4, zh)) for j in (1, 2, 3)] + [zh_mate]

    def total_copy(j):
        slot = x if j < 3 else 4
        return pltpu.make_async_remote_copy(
            src_ref=totbuf.at[x], dst_ref=totbuf.at[slot], send_sem=tsem.at[j],
            recv_sem=trsem.at[j], device_id=place(total_to[j]), device_id_type=MESH,
        )

    def totals_start():
        def step(j, carry):
            sum_copy(j).wait_recv()
            return carry

        lax.fori_loop(1, 16, step, 0)
        total = csend[...]
        for j in range(1, 16):
            total = total + crecv[j]
        totbuf[x] = total
        for j in range(4):
            total_copy(j).start()

    def totals_finish():
        for j in range(4):
            total_copy(j).wait_recv()

    def gram(f):
        mine = pl.ds(pl.multiple_of(c * HALF, HALF), HALF)
        theirs = pl.ds(pl.multiple_of((1 - c) * HALF, HALF), HALF)

        def product(left, right):
            return lax.dot_general(
                left, right, (((0,), (0,)), ((), ())), preferred_element_type=F32
            ).astype(BF16)

        def step(i, carry):
            to = (y + 2 + i) % 4
            dsend[f, to, zh] = product(xbuf[f, to, :, theirs], xbuf[f, x])
            dsend[f, to, 1 - zh] = product(xbuf[f, to, :, theirs], zbuf[f])
            d_copy(f, to).start()
            pown[f, to, zh] = product(xbuf[f, to, :, mine], xbuf[f, x])
            pown[f, to, 1 - zh] = product(xbuf[f, to, :, mine], zbuf[f])
            return carry

        lax.fori_loop(0, 4, step, 0)

    def d_copy(f, to):
        return pltpu.make_async_remote_copy(
            src_ref=dsend.at[f, to], dst_ref=drecv.at[f, to], send_sem=ssem.at[f, D_ID + to],
            recv_sem=rsem.at[f, D_ID + to], device_id=place(sibling), device_id_type=MESH,
        )

    def both(f, to, b):
        return pown[f, to, b].astype(F32) + drecv[f, to, b].astype(F32)

    y_far, y_up, y_down = (y + 2) % 4, (y + 1) % 4, (y + 3) % 4

    def reduce_start(f):
        d_copy(f, y_far).wait_recv()
        y1s[f, 0] = both(f, y_far, 0).astype(BF16)
        sends[f](Y1_ID + 0, y1s.at[f, 0], y1r.at[f, 0], y_plus)
        y1s[f, 1] = both(f, y_far, 1).astype(BF16)
        sends[f](Y1_ID + 1, y1s.at[f, 1], y1r.at[f, 1], y_minus)
        d_copy(f, y_down).wait_recv()
        y2s[f, 2] = both(f, y_down, 0).astype(BF16)
        sends[f](Y2_ID + 2, y2s.at[f, 2], y2r.at[f, 2], y_minus)
        d_copy(f, y).wait_recv()
        d_copy(f, y_up).wait_recv()
        y2s[f, 0] = both(f, y_up, 1).astype(BF16)
        sends[f](Y2_ID + 0, y2s.at[f, 0], y2r.at[f, 0], y_plus)

    def reduce_middle(f):
        waits[f](Y1_ID + 0, y1r.at[f, 0])
        y2s[f, 1] = (both(f, y_up, 0) + y1r[f, 0].astype(F32)).astype(BF16)
        sends[f](Y2_ID + 1, y2s.at[f, 1], y2r.at[f, 1], y_plus)
        waits[f](Y1_ID + 1, y1r.at[f, 1])
        y2s[f, 3] = (both(f, y_down, 1) + y1r[f, 1].astype(F32)).astype(BF16)
        sends[f](Y2_ID + 3, y2s.at[f, 3], y2r.at[f, 3], y_minus)

    def reduce_last(f):
        for k in range(4):
            waits[f](Y2_ID + k, y2r.at[f, k])
        tot[f, 0] = both(f, y, 0) + y2r[f, 1].astype(F32) + y2r[f, 2].astype(F32)
        tot[f, 1] = both(f, y, 1) + y2r[f, 0].astype(F32) + y2r[f, 3].astype(F32)
        zs[f] = tot[f, 1 - zl].astype(BF16)
        sends[f](Z_ID, zs.at[f], zr.at[f], zl_mate)

    def eye(rows, start_col):
        r = lax.broadcasted_iota(jnp.int32, (rows, QUARTER), 0) + BLOCK * row_block + HALF * c
        k = lax.broadcasted_iota(jnp.int32, (rows, QUARTER), 1) + BLOCK * phi + start_col
        return (r == k).astype(F32)

    def inverse(sums):
        return lax.rsqrt(sums / TOKENS + epsilon)

    def normalise(f):
        waits[f](Z_ID, zr.at[f])
        of_col = jnp.where(zl == zh, x, 4)
        inv_col = inverse(totbuf[of_col, f : f + 1, :])
        mine = pl.ds(pl.multiple_of(c * HALF, HALF), HALF)
        inv_row = inverse(totbuf[y, f : f + 1, mine])
        inv_row = jnp.transpose(jnp.broadcast_to(inv_row, (QUARTER, HALF)))
        for j in range(4):
            cols = slice(j * QUARTER, (j + 1) * QUARTER)
            g = tot[f, zl, :, cols] + zr[f, :, cols].astype(F32)
            damped = g / TOKENS * inv_row * inv_col[:, cols] + damping * eye(HALF, j * QUARTER)
            value = damped / divisor
            scaled[f, :, cols] = value
            rowbuf[f, phi, :, cols] = value.astype(BF16)
            colbuf[f, row_block, c, :, cols] = value.astype(BF16)

    parts = (pl.ds(0, QUARTER), pl.ds(QUARTER, QUARTER))

    def row_gather(f, buf, base):
        def ref(step, other, part):
            slot = ((x + step) % 4) * 2 + (1 - zl if other else zl)
            piece = buf(slot)
            return piece if part is None else piece.at[parts[part]]

        return Gather(sends[f], waits[f], base, ref, x_plus, x_minus, zl_mate, True)

    def col_gather(f, buf, base):
        def ref(step, other, part):
            slot = ((y + step) % 4) * 2 + (1 - zh if other else zh)
            piece = buf(slot, c)
            return piece if part is None else piece.at[parts[part]]

        def pass_on(k, r):
            sends[f](k, r, r, sibling)

        return Gather(
            sends[f], waits[f], base, ref, y_plus, y_minus, zh_mate, False, pass_on
        )

    def sibling_finish(f, buf, base):
        whole = [9, 10, 11, 12, 15, 16]
        for k in range(9, 19):
            piece = buf(0, 1 - c)
            waits[f](base + k, piece if k in whole else piece.at[parts[0]])

    rows = [row_gather(f, lambda s, f=f: rowbuf.at[f, s], ROW_ID) for f in range(2)]
    cols = [col_gather(f, lambda s, k, f=f: colbuf.at[f, s, k], COL_ID) for f in range(2)]
    sq_rows = row_gather(0, lambda s: sqrow.at[s], SQ_ID)
    sq_cols = col_gather(1, lambda s, k: sqcol.at[s, k], SQ_ID)

    def product(f, left, right):
        sq[f] = jnp.zeros((HALF, BLOCK), F32)

        def step(k, carry):
            sq[f] += jnp.dot(
                left(k), right(k).reshape(BLOCK, BLOCK), preferred_element_type=F32
            )
            return carry

        lax.fori_loop(0, 8, step, 0)

    def square(f):
        product(f, lambda k: rowbuf[f, k], lambda k: colbuf[f, k])
        half = sq[f].astype(BF16)
        if f == 0:
            sqrow[phi] = half
        else:
            sqcol[row_block, c] = half
        for j in range(4):
            k = slice(j * QUARTER, (j + 1) * QUARTER)
            scaled[f, :, k] = (
                4.0 * eye(HALF, j * QUARTER) - 6.0 * scaled[f, :, k] + 4.0 * sq[f, :, k]
            )

    def out_copy(f, b):
        return pltpu.make_async_remote_copy(
            src_ref=obuf.at[f, pl.ds(b * 32, 32)], dst_ref=orecv.at[f, phi],
            send_sem=ssem.at[f, OUT_ID + b], recv_sem=rsem.at[f, OUT_ID + phi],
            device_id=place((out_tok, b)), device_id_type=MESH,
        )

    def cube(f):
        if f == 0:
            product(f, lambda k: sqrow[k], lambda k: colbuf[f, k])
        else:
            product(f, lambda k: rowbuf[f, k], lambda k: sqcol[k])
        obuf[f] = (scaled[f] - sq[f]).astype(BF16)
        for b in range(8):
            me = home & (blk == b)

            @pl.when(me)
            def _():
                orecv[f, phi] = obuf[f, b * 32 : (b + 1) * 32]

            @pl.when(jnp.logical_not(me))
            def _():
                out_copy(f, b).start()

    def emit(f):
        for k in range(8):
            @pl.when(jnp.logical_not(home & (phi == k)))
            def _():
                waits[f](OUT_ID + k, orecv.at[f, k])

        out = (act_out, grad_out)[f]
        for k in range(8):
            out[:, k * BLOCK : (k + 1) * BLOCK] = orecv[f, k].astype(F32)

    load_own(0).wait()
    x_start(0)
    load_own(1).wait()
    column_sums(0)
    column_sums(1)
    sums_start()
    x_forward(0)
    x_start(1)
    totals_start()
    x_finish(0)
    gram(0)
    reduce_start(0)
    x_forward(1)
    reduce_middle(0)
    x_finish(1)
    gram(1)
    reduce_start(1)
    reduce_last(0)
    totals_finish()
    normalise(0)
    rows[0].start()
    cols[0].start()
    reduce_middle(1)
    rows[0].near()
    cols[0].near()
    rows[0].other()
    cols[0].other()
    reduce_last(1)
    rows[0].far()
    cols[0].far()
    normalise(1)
    rows[1].start()
    cols[1].start()
    rows[0].finish()
    cols[0].finish()
    sibling_finish(0, lambda s, k: colbuf.at[0, s, k], COL_ID)
    square(0)
    sq_rows.start()
    rows[1].near()
    cols[1].near()
    rows[1].other()
    cols[1].other()
    sq_rows.near()
    sq_rows.other()
    rows[1].far()
    cols[1].far()
    sq_rows.far()
    rows[1].finish()
    cols[1].finish()
    sibling_finish(1, lambda s, k: colbuf.at[1, s, k], COL_ID)
    square(1)
    sq_cols.start()
    sq_rows.finish()
    cube(0)
    sq_cols.near()
    sq_cols.other()
    sq_cols.far()
    emit(0)
    sq_cols.finish()
    sibling_finish(1, lambda s, k: sqcol.at[s, k], SQ_ID)
    cube(1)
    emit(1)

    for copy in sent:
        copy.wait_send()

    def sums_left(j, carry):
        sum_copy(j).wait_send()
        return carry

    lax.fori_loop(1, 16, sums_left, 0)
    for j in range(4):
        total_copy(j).wait_send()
    for f in range(2):
        for k in range(4):
            d_copy(f, k).wait_send()
        for b in range(8):
            @pl.when(jnp.logical_not(home & (blk == b)))
            def _():
                out_copy(f, b).wait_send()


def body(activations, out_grads):
    hbm = pl.BlockSpec(memory_space=pltpu.HBM)
    vmem = pl.BlockSpec(memory_space=pltpu.VMEM)
    out = jax.ShapeDtypeStruct((32, D), F32)
    tile = (HALF, BLOCK)
    scratch = [
        pltpu.VMEM((2, 4, BLOCK, BLOCK), BF16),
        pltpu.VMEM((2, BLOCK, BLOCK), BF16),
        pltpu.VMEM((2, 4, 2, *tile), BF16),
        pltpu.VMEM((2, 4, 2, *tile), BF16),
        pltpu.VMEM((2, 4, 2, *tile), BF16),
        pltpu.VMEM((2, 2, *tile), BF16),
        pltpu.VMEM((2, 2, *tile), BF16),
        pltpu.VMEM((2, 4, *tile), BF16),
        pltpu.VMEM((2, 4, *tile), BF16),
        pltpu.VMEM((2, 2, *tile), F32),
        pltpu.VMEM((2, *tile), BF16),
        pltpu.VMEM((2, *tile), BF16),
        pltpu.VMEM((2, *tile), F32),
        pltpu.VMEM((2, 8, *tile), BF16),
        pltpu.VMEM((2, 8, 2, *tile), BF16),
        pltpu.VMEM((8, *tile), BF16),
        pltpu.VMEM((8, 2, *tile), BF16),
        pltpu.VMEM((2, *tile), F32),
        pltpu.VMEM((2, *tile), BF16),
        pltpu.VMEM((2, 8, 32, BLOCK), BF16),
        pltpu.VMEM((2, BLOCK), F32),
        pltpu.VMEM((16, 2, BLOCK), F32),
        pltpu.VMEM((5, 2, BLOCK), F32),
        pltpu.SemaphoreType.DMA((2, N_ID)),
        pltpu.SemaphoreType.DMA((2, N_ID)),
        pltpu.SemaphoreType.DMA((16,)),
        pltpu.SemaphoreType.DMA((16,)),
        pltpu.SemaphoreType.DMA((4,)),
        pltpu.SemaphoreType.DMA((4,)),
        pltpu.SemaphoreType.DMA((2,)),
    ]
    return pl.pallas_call(
        kernel,
        out_shape=(out, out),
        in_specs=[hbm, hbm],
        out_specs=(vmem, vmem),
        scratch_shapes=scratch,
        compiler_params=pltpu.CompilerParams(
            collective_id=0, has_side_effects=True, vmem_limit_bytes=62 * 1024 * 1024
        ),
    )(activations, out_grads)


def solution(mesh):
    placed = (P("tok", "blk"), P("tok", "blk"))
    return jax.shard_map(
        body,
        mesh=mesh,
        in_specs=placed,
        out_specs=(P(("tok", "blk"), None), P(("tok", "blk"), None)),
        check_vma=False,
    )
```

```python
import jax
import jax.numpy as jnp
from jax import lax
from jax.experimental import pallas as pl
from jax.experimental.pallas import tpu as pltpu
from jax.sharding import PartitionSpec as P

D = 4096
TOKENS = 8192
BLOCK = 512
HALF = 256
QUARTER = 128

damping = 0.3
epsilon = 1e-06
divisor = 2.0

MESH = pl.DeviceIdType.MESH
F32 = jnp.float32
BF16 = jnp.bfloat16

NX_ID = 20
D_ID = 0
Y1_ID = 4
Y2_ID = 6
ROW_ID = 10
COL_ID = 14
SQ_ID = 33
OUT_ID = 37
N_ID = 45


class Line:
    def __init__(self, send, wait, base, ref, plus, minus):
        self.send, self.wait, self.base, self.ref = send, wait, base, ref
        self.plus, self.minus = plus, minus

    def put(self, k, place, to):
        r = self.ref(*place)
        self.send(self.base + k, r, r, to)

    def take(self, k):
        self.wait(self.base + k, self.ref(*[(3, None), (1, None), (2, 0), (2, 1)][k]))

    def start(self):
        self.put(0, (0, None), self.plus)
        self.put(1, (0, None), self.minus)

    def near(self):
        self.take(0)
        self.put(2, (3, 0), self.plus)
        self.take(1)
        self.put(3, (1, 1), self.minus)

    def finish(self):
        self.take(2)
        self.take(3)


class Gather:
    def __init__(self, send, wait, base, ref, plus, minus, across, via_z, pass_on=None):
        self.send, self.wait, self.base, self.ref = send, wait, base, ref
        self.plus, self.minus, self.across, self.via_z = plus, minus, across, via_z
        self.pass_on = pass_on

    def incoming(self, k):
        return [
            (3, 0, None), (1, 0, None), (0, 1, None), (2, 0, 0), (2, 0, 1),
            (3, 1, None), (1, 1, None), (2, 1, 0), (2, 1, 1),
        ][k]

    def put(self, k, place, to):
        r = self.ref(*place)
        self.send(self.base + k, r, r, to)

    def take(self, k):
        r = self.ref(*self.incoming(k))
        self.wait(self.base + k, r)
        if self.pass_on is not None:
            self.pass_on(self.base + 10 + k, r)

    def start(self):
        own = (0, 0, None)
        self.put(0, own, self.plus)
        self.put(1, own, self.minus)
        self.put(2, own, self.across)
        if self.pass_on is not None:
            self.pass_on(self.base + 9, self.ref(*own))

    def near(self):
        self.take(0)
        self.put(3, (3, 0, 0), self.plus)
        self.take(1)
        self.put(4, (1, 0, 1), self.minus)

    def other(self):
        self.take(2)
        self.put(5, (0, 1, None), self.plus)
        self.put(6, (0, 1, None), self.minus)

    def far(self):
        if self.via_z:
            self.take(3)
            self.put(7, (2, 0, 0), self.across)
            self.take(4)
            self.put(8, (2, 0, 1), self.across)
        else:
            self.take(5)
            self.put(7, (3, 1, 0), self.plus)
            self.take(6)
            self.put(8, (1, 1, 1), self.minus)

    def finish(self):
        for k in (5, 6, 7, 8) if self.via_z else (3, 4, 7, 8):
            self.take(k)


def kernel(
    act_ref, grad_ref, act_out, grad_out,
    xall, give, acc, dsend, drecv, y1s, y1r, y2s, y2r, scaled,
    rowbuf, colbuf, sqrow, sq, obuf, orecv, csend, crecv, totbuf,
    xssem, xrsem, ssem, rsem, csem, crsem, tsem, trsem, lsem,
):
    tok, blk = lax.axis_index("tok"), lax.axis_index("blk")
    c, y, zl = tok % 2, (tok // 2) % 4, tok // 8
    x, zh = blk // 2, blk % 2

    def tok_of(zl_, y_, c_):
        return zl_ * 8 + y_ * 2 + c_

    def blk_of(x_, zh_):
        return x_ * 2 + zh_

    x_plus = (tok, blk_of((x + 1) % 4, zh))
    x_minus = (tok, blk_of((x + 3) % 4, zh))
    zh_mate = (tok, blk_of(x, 1 - zh))
    y_plus = (tok_of(zl, (y + 1) % 4, c), blk)
    y_minus = (tok_of(zl, (y + 3) % 4, c), blk)
    zl_mate = (tok_of(1 - zl, y, c), blk)
    z_cross = (tok_of(1 - zl, y, c), blk_of(x, 1 - zh))
    sibling = (tok_of(zl, y, 1 - c), blk)

    def place(to):
        return {"tok": to[0], "blk": to[1]}

    out_tok = 4 * y + 2 * zh + c
    home = out_tok == tok
    line_slot = 2 * x + zl
    row_block = 2 * y + zh

    barrier = pltpu.get_barrier_semaphore()

    def greet(to):
        pl.semaphore_signal(barrier, inc=1, device_id=place(to), device_id_type=MESH)

    def greet_tok(j, carry):
        greet(((tok + j) % 16, blk))
        return carry

    def greet_blk(j, carry):
        greet((tok, (blk + j) % 8))
        return carry

    lax.fori_loop(1, 16, greet_tok, 0)
    lax.fori_loop(1, 8, greet_blk, 0)
    greet(z_cross)

    def greet_source(j, carry):
        to = (tok_of(j % 2, tok // 4, c), blk_of(j // 2, (tok // 2) % 2))

        @pl.when(jnp.logical_not((to[0] == tok) & (to[1] == blk)))
        def _():
            greet(to)

        return carry

    lax.fori_loop(0, 8, greet_source, 0)

    def load(src, dst, k):
        return pltpu.make_async_copy(src, dst, lsem.at[k])

    @pl.when(zl == 0)
    def _():
        load(act_ref, xall.at[0, x], 0).start()
        load(grad_ref, give, 1).start()

    @pl.when(zl == 1)
    def _():
        load(grad_ref, xall.at[0, x], 0).start()
        load(act_ref, give, 1).start()

    pl.semaphore_wait(barrier, 15 + 7 + 1 + 8 - home.astype(jnp.int32))

    sent = []

    def sender(ss, rs):
        def send(k, src, dst, to):
            copy = pltpu.make_async_remote_copy(
                src_ref=src, dst_ref=dst, send_sem=ss.at[k], recv_sem=rs.at[k],
                device_id=place(to), device_id_type=MESH,
            )
            copy.start()
            sent.append(copy)

        return send

    def waiter(ss, rs):
        def wait(k, dst):
            pltpu.make_async_remote_copy(
                src_ref=dst, dst_ref=dst, send_sem=ss.at[k], recv_sem=rs.at[k],
                device_id=place(sibling), device_id_type=MESH,
            ).wait_recv()

        return wait

    x_send, x_wait = sender(xssem, xrsem), waiter(xssem, xrsem)
    sends = [sender(ssem.at[h], rsem.at[h]) for h in range(2)]
    waits = [waiter(ssem.at[h], rsem.at[h]) for h in range(2)]

    token_half = (pl.ds(0, HALF), pl.ds(HALF, HALF))

    def x_block(t, step, half):
        return xall.at[t, (x + step) % 4, token_half[half]]

    def x_put(t, k):
        step, half, to = [
            (0, 0, x_plus), (0, 1, x_plus), (0, 1, x_minus), (0, 0, x_minus),
            (3, 0, x_plus), (1, 1, x_minus),
        ][k]
        r = x_block(t, step, half)
        x_send(8 * t + k, r, r, to)

    def x_take(t, k):
        step, half = [(3, 0), (3, 1), (1, 1), (1, 0), (2, 0), (2, 1)][k]
        x_wait(8 * t + k, x_block(t, step, half))

    def z_start():
        for half in range(2):
            x_send(18 + half, give.at[token_half[half]], x_block(1, 0, half), zl_mate)

    def z_rest():
        x_send(17, give, xall.at[1, 4], z_cross)
        x_send(16, xall.at[0, x], xall.at[0, 4], zh_mate)

    def column_sums():
        def of(ref):
            values = ref.astype(F32)
            return jnp.sum(values * values, axis=0, keepdims=True)

        csend[zl] = of(xall[0, x])
        csend[1 - zl] = of(give[...])

    def sum_copy(j):
        return pltpu.make_async_remote_copy(
            src_ref=csend, dst_ref=crecv.at[j], send_sem=csem.at[j], recv_sem=crsem.at[j],
            device_id=place(((tok + j) % 16, blk)), device_id_type=MESH,
        )

    def sums_start():
        def step(j, carry):
            sum_copy(j).start()
            return carry

        lax.fori_loop(1, 16, step, 0)

    total_to = [(tok, blk_of((x + j) % 4, zh)) for j in (1, 2, 3)] + [zh_mate]

    def total_copy(j):
        slot = x if j < 3 else 4
        return pltpu.make_async_remote_copy(
            src_ref=totbuf.at[x], dst_ref=totbuf.at[slot], send_sem=tsem.at[j],
            recv_sem=trsem.at[j], device_id=place(total_to[j]), device_id_type=MESH,
        )

    def totals_start():
        def step(j, carry):
            sum_copy(j).wait_recv()
            return carry

        lax.fori_loop(1, 16, step, 0)
        total = csend[...]
        for j in range(1, 16):
            total = total + crecv[j]
        totbuf[x] = total
        for j in range(4):
            total_copy(j).start()

    def totals_finish():
        for j in range(4):
            total_copy(j).wait_recv()

    mine = pl.ds(pl.multiple_of(c * HALF, HALF), HALF)
    theirs = pl.ds(pl.multiple_of((1 - c) * HALF, HALF), HALF)
    col_slot = [jnp.where(zh == h, x, 4) for h in range(2)]

    def product_of(t, to, h, part):
        return lax.dot_general(
            xall[t, to, :, part], xall[t, col_slot[h]], (((0,), (0,)), ((), ())),
            preferred_element_type=F32,
        )

    def gram_first():
        def step(to, carry):
            for h in range(2):
                acc[h, to, 0] = product_of(0, to, h, mine)
                acc[h, to, 1] = product_of(0, to, h, theirs)
            return carry

        lax.fori_loop(0, 4, step, 0)

    def gram_second(begin, end):
        def step(i, carry):
            to = (x + 3 + i) % 4
            for h in range(2):
                dsend[h, to] = (acc[h, to, 1] + product_of(1, to, h, theirs)).astype(BF16)
                d_copy(h, to).start()
            for h in range(2):
                acc[h, to, 0] = acc[h, to, 0] + product_of(1, to, h, mine)
            return carry

        lax.fori_loop(begin, end, step, 0)

    def d_copy(h, to):
        return pltpu.make_async_remote_copy(
            src_ref=dsend.at[h, to], dst_ref=drecv.at[h, to], send_sem=ssem.at[h, D_ID + to],
            recv_sem=rsem.at[h, D_ID + to], device_id=place(sibling), device_id_type=MESH,
        )

    lo, hi = pl.ds(0, QUARTER), pl.ds(QUARTER, QUARTER)

    def both(h, to, part):
        return acc[h, to, 0, part] + drecv[h, to, part].astype(F32)

    y_far, y_up, y_down = (y + 2) % 4, (y + 1) % 4, (y + 3) % 4

    def reduce_start(h):
        d_copy(h, y_far).wait_recv()
        y1s[h, 0] = both(h, y_far, lo).astype(BF16)
        sends[h](Y1_ID + 0, y1s.at[h, 0], y1r.at[h, 0], y_plus)
        y1s[h, 1] = both(h, y_far, hi).astype(BF16)
        sends[h](Y1_ID + 1, y1s.at[h, 1], y1r.at[h, 1], y_minus)
        d_copy(h, y_up).wait_recv()
        y2s[h, 0] = both(h, y_up, hi).astype(BF16)
        sends[h](Y2_ID + 0, y2s.at[h, 0], y2r.at[h, 0], y_plus)
        d_copy(h, y_down).wait_recv()
        y2s[h, 2] = both(h, y_down, lo).astype(BF16)
        sends[h](Y2_ID + 2, y2s.at[h, 2], y2r.at[h, 2], y_minus)
        d_copy(h, y).wait_recv()

    def reduce_middle(h):
        waits[h](Y1_ID + 0, y1r.at[h, 0])
        y2s[h, 1] = (both(h, y_up, lo) + y1r[h, 0].astype(F32)).astype(BF16)
        sends[h](Y2_ID + 1, y2s.at[h, 1], y2r.at[h, 1], y_plus)
        waits[h](Y1_ID + 1, y1r.at[h, 1])
        y2s[h, 3] = (both(h, y_down, hi) + y1r[h, 1].astype(F32)).astype(BF16)
        sends[h](Y2_ID + 3, y2s.at[h, 3], y2r.at[h, 3], y_minus)

    def eye(h, start_col):
        shape = (HALF, QUARTER)
        r = lax.broadcasted_iota(jnp.int32, shape, 0) + BLOCK * row_block + HALF * c
        k = lax.broadcasted_iota(jnp.int32, shape, 1) + BLOCK * (2 * x + h) + start_col
        return (r == k).astype(F32)

    def inverse(sums):
        return lax.rsqrt(sums / TOKENS + epsilon)

    def normalise(h):
        for k in range(4):
            waits[h](Y2_ID + k, y2r.at[h, k])
        inv_col = inverse(totbuf[col_slot[h], zl])
        inv_row = inverse(totbuf[y, zl, :, mine])
        inv_row = jnp.transpose(jnp.broadcast_to(inv_row, (QUARTER, HALF)))
        acc[h, y, 0, lo] = both(h, y, lo) + y2r[h, 1].astype(F32) + y2r[h, 2].astype(F32)
        acc[h, y, 0, hi] = both(h, y, hi) + y2r[h, 0].astype(F32) + y2r[h, 3].astype(F32)
        for j in range(4):
            k = slice(j * QUARTER, (j + 1) * QUARTER)
            g = acc[h, y, 0, :, k]
            damped = g / TOKENS * inv_row * inv_col[:, k] + damping * eye(h, j * QUARTER)
            value = damped / divisor
            scaled[h, :, k] = value
            rowbuf[2 * x + h, :, k] = value.astype(BF16)
            colbuf[h, row_block, c, :, k] = value.astype(BF16)

    parts = (lo, hi)

    def row_line(h, buf, base):
        def ref(step, part):
            piece = buf.at[((x + step) % 4) * 2 + h]
            return piece if part is None else piece.at[parts[part]]

        return Line(sends[h], waits[h], base, ref, x_plus, x_minus)

    def col_gather(h):
        def ref(step, other, part):
            piece = colbuf.at[h, ((y + step) % 4) * 2 + (1 - zh if other else zh), c]
            return piece if part is None else piece.at[parts[part]]

        def pass_on(k, r):
            sends[h](k, r, r, sibling)

        return Gather(
            sends[h], waits[h], COL_ID, ref, y_plus, y_minus, zh_mate, True, pass_on
        )

    def sibling_finish(h):
        whole = [9, 10, 11, 12, 15, 16]
        for k in range(9, 19):
            piece = colbuf.at[h, 0, 1 - c]
            waits[h](COL_ID + k, piece if k in whole else piece.at[lo])

    rows = [row_line(h, rowbuf, ROW_ID) for h in range(2)]
    cols = [col_gather(h) for h in range(2)]
    sq_rows = [row_line(h, sqrow, SQ_ID) for h in range(2)]

    def product(h, left):
        sq[h] = jnp.zeros((HALF, BLOCK), F32)

        def step(k, carry):
            sq[h] += jnp.dot(
                left[k], colbuf[h, k].reshape(BLOCK, BLOCK), preferred_element_type=F32
            )
            return carry

        lax.fori_loop(0, 8, step, 0)

    def square(h):
        product(h, rowbuf)
        sqrow[2 * x + h] = sq[h].astype(BF16)
        sq_rows[h].start()
        for j in range(4):
            k = slice(j * QUARTER, (j + 1) * QUARTER)
            scaled[h, :, k] = (
                4.0 * eye(h, j * QUARTER) - 6.0 * scaled[h, :, k] + 4.0 * sq[h, :, k]
            )

    def out_copy(h, b):
        return pltpu.make_async_remote_copy(
            src_ref=obuf.at[h, pl.ds(b * 32, 32)], dst_ref=orecv.at[h, line_slot],
            send_sem=ssem.at[h, OUT_ID + b], recv_sem=rsem.at[h, OUT_ID + line_slot],
            device_id=place((out_tok, b)), device_id_type=MESH,
        )

    def cube(h):
        product(h, sqrow)
        obuf[h] = (scaled[h] - sq[h]).astype(BF16)
        for b in range(8):
            me = home & (blk == b)

            @pl.when(me)
            def _():
                orecv[h, line_slot] = obuf[h, b * 32 : (b + 1) * 32]

            @pl.when(jnp.logical_not(me))
            def _():
                out_copy(h, b).start()

    def emit(h):
        for k in range(8):
            @pl.when(jnp.logical_not(home & (line_slot == k)))
            def _():
                waits[h](OUT_ID + k, orecv.at[h, k])

        for k in range(8):
            out = (act_out, grad_out)[k % 2]
            start = (2 * (k // 2) + h) * BLOCK
            out[:, start : start + BLOCK] = orecv[h, k].astype(F32)

    load(act_ref, give, 1).wait()
    z_start()
    load(act_ref, give, 0).wait()
    x_put(0, 0)
    x_put(0, 2)
    x_put(0, 1)
    x_put(0, 3)
    z_rest()
    column_sums()
    sums_start()
    x_take(0, 0)
    x_put(0, 4)
    x_take(0, 2)
    x_put(0, 5)
    x_wait(18, x_block(1, 0, 0))
    x_put(1, 0)
    x_wait(19, x_block(1, 0, 1))
    x_put(1, 2)
    x_put(1, 1)
    x_put(1, 3)
    totals_start()
    x_take(0, 1)
    x_take(0, 3)
    x_take(0, 4)
    x_take(0, 5)
    x_wait(16, xall.at[0, 4])
    gram_first()
    x_take(1, 0)
    x_put(1, 4)
    x_take(1, 2)
    x_put(1, 5)
    x_wait(17, xall.at[1, 4])
    x_take(1, 1)
    x_take(1, 3)
    gram_second(0, 3)
    x_take(1, 4)
    x_take(1, 5)
    gram_second(3, 4)
    reduce_start(0)
    reduce_start(1)
    reduce_middle(0)
    reduce_middle(1)
    totals_finish()
    normalise(0)
    cols[0].start()
    rows[0].start()
    normalise(1)
    rows[1].start()
    cols[0].near()
    cols[0].other()
    cols[1].start()
    rows[0].near()
    rows[1].near()
    cols[0].far()
    cols[1].near()
    cols[1].other()
    rows[0].finish()
    rows[1].finish()
    cols[0].finish()
    sibling_finish(0)
    square(0)
    cols[1].far()
    sq_rows[0].near()
    cols[1].finish()
    sibling_finish(1)
    square(1)
    sq_rows[0].finish()
    sq_rows[1].near()
    sq_rows[1].finish()
    cube(0)
    cube(1)
    emit(0)
    emit(1)

    for copy in sent:
        copy.wait_send()

    def sums_left(j, carry):
        sum_copy(j).wait_send()
        return carry

    lax.fori_loop(1, 16, sums_left, 0)
    for j in range(4):
        total_copy(j).wait_send()
    for h in range(2):
        for k in range(4):
            d_copy(h, k).wait_send()
        for b in range(8):
            @pl.when(jnp.logical_not(home & (blk == b)))
            def _():
                out_copy(h, b).wait_send()


def body(activations, out_grads):
    hbm = pl.BlockSpec(memory_space=pltpu.HBM)
    vmem = pl.BlockSpec(memory_space=pltpu.VMEM)
    out = jax.ShapeDtypeStruct((32, D), F32)
    tile = (HALF, BLOCK)
    part = (QUARTER, BLOCK)
    scratch = [
        pltpu.VMEM((2, 5, BLOCK, BLOCK), BF16),
        pltpu.VMEM((BLOCK, BLOCK), BF16),
        pltpu.VMEM((2, 4, 2, *tile), F32),
        pltpu.VMEM((2, 4, *tile), BF16),
        pltpu.VMEM((2, 4, *tile), BF16),
        pltpu.VMEM((2, 2, *part), BF16),
        pltpu.VMEM((2, 2, *part), BF16),
        pltpu.VMEM((2, 4, *part), BF16),
        pltpu.VMEM((2, 4, *part), BF16),
        pltpu.VMEM((2, *tile), F32),
        pltpu.VMEM((8, *tile), BF16),
        pltpu.VMEM((2, 8, 2, *tile), BF16),
        pltpu.VMEM((8, *tile), BF16),
        pltpu.VMEM((2, *tile), F32),
        pltpu.VMEM((2, *tile), BF16),
        pltpu.VMEM((2, 8, 32, BLOCK), BF16),
        pltpu.VMEM((2, 1, BLOCK), F32),
        pltpu.VMEM((16, 2, 1, BLOCK), F32),
        pltpu.VMEM((5, 2, 1, BLOCK), F32),
        pltpu.SemaphoreType.DMA((NX_ID,)),
        pltpu.SemaphoreType.DMA((NX_ID,)),
        pltpu.SemaphoreType.DMA((2, N_ID)),
        pltpu.SemaphoreType.DMA((2, N_ID)),
        pltpu.SemaphoreType.DMA((16,)),
        pltpu.SemaphoreType.DMA((16,)),
        pltpu.SemaphoreType.DMA((4,)),
        pltpu.SemaphoreType.DMA((4,)),
        pltpu.SemaphoreType.DMA((2,)),
    ]
    return pl.pallas_call(
        kernel,
        out_shape=(out, out),
        in_specs=[hbm, hbm],
        out_specs=(vmem, vmem),
        scratch_shapes=scratch,
        compiler_params=pltpu.CompilerParams(
            collective_id=0, has_side_effects=True, vmem_limit_bytes=62 * 1024 * 1024
        ),
    )(activations, out_grads)


def solution(mesh):
    placed = (P("tok", "blk"), P("tok", "blk"))
    return jax.shard_map(
        body,
        mesh=mesh,
        in_specs=placed,
        out_specs=(P(("tok", "blk"), None), P(("tok", "blk"), None)),
        check_vma=False,
    )
```

```python
import jax
import jax.numpy as jnp
from jax import lax
from jax.experimental import pallas as pl
from jax.experimental.pallas import tpu as pltpu
from jax.sharding import PartitionSpec as P

D = 4096
TOKENS = 8192
BLOCK = 512
HALF = 256
PART = 128

damping = 0.3
epsilon = 1e-06
divisor = 2.0

MESH = pl.DeviceIdType.MESH
F32 = jnp.float32
BF16 = jnp.bfloat16


class Ids:
    def __init__(self):
        self.next = 0

    def take(self, n):
        first = self.next
        self.next += n
        return first


IDS = Ids()
Z_ID = IDS.take(6)
X_ID = [[IDS.take(6) for _ in range(2)] for _ in range(2)]
D_ID = [IDS.take(4) for _ in range(2)]
Y1_ID = [IDS.take(2) for _ in range(2)]
Y2_ID = [IDS.take(4) for _ in range(2)]
ROW_ID = [IDS.take(6) for _ in range(2)]
COL_ID = [IDS.take(23) for _ in range(3)]
SQ_ID = [IDS.take(6) for _ in range(2)]
OUT_ID = [IDS.take(8) for _ in range(2)]
SUM_ID = IDS.take(16)
TOTAL_ID = IDS.take(4)
N_ID = IDS.next


class Line:
    arrivals = [(3, 0), (3, 1), (1, 1), (1, 0), (2, 0), (2, 1)]

    def __init__(self, send, wait, base, ref, plus, minus, arrived=None):
        self.send, self.wait, self.base, self.ref = send, wait, base, ref
        self.plus, self.minus, self.arrived = plus, minus, arrived

    def put(self, k, where, to):
        r = self.ref(*where)
        self.send(self.base + k, r, r, to)

    def take(self, k):
        r = self.ref(*self.arrivals[k])
        self.wait(self.base + k, r)
        if self.arrived is not None:
            self.arrived(k, r)

    def start(self):
        self.put(0, (0, 0), self.plus)
        self.put(2, (0, 1), self.minus)
        self.put(1, (0, 1), self.plus)
        self.put(3, (0, 0), self.minus)

    def near(self):
        self.take(0)
        self.put(4, (3, 0), self.plus)
        self.take(2)
        self.put(5, (1, 1), self.minus)

    def finish(self):
        for k in (1, 3, 4, 5):
            self.take(k)


class Plane(Line):
    arrivals = Line.arrivals + [
        (0, None, 1), (3, None, 1), (1, None, 1), (2, 0, 1), (2, 1, 1)
    ]

    def __init__(self, send, wait, base, ref, plus, minus, across, sibling, mirrored):
        super().__init__(send, wait, base, ref, plus, minus, self.pass_on)
        self.across, self.sibling, self.mirrored = across, sibling, mirrored

    def pass_on(self, k, r):
        self.send(self.base + 12 + k, r, r, self.sibling)

    def start(self):
        super().start()
        self.put(6, (0, None, 0), self.across)
        self.send(self.base + 11, self.ref(0, None, 0), self.ref(0, None, 0), self.sibling)

    def other(self):
        self.take(6)
        self.put(7, (0, None, 1), self.plus)
        self.put(8, (0, None, 1), self.minus)

    def far(self):
        self.take(4)
        self.put(9, (2, 0, 0), self.across)
        self.take(5)
        self.put(10, (2, 1, 0), self.across)

    def finish(self):
        for k in (1, 3, 7, 8, 9, 10):
            self.take(k)
        for k in range(11, 23):
            half = None if k in (11, 18, 19, 20) else 0
            self.wait(self.base + k, self.mirrored(half))


def kernel(
    act_ref, grad_ref, act_out, grad_out,
    xall, give, gram_part, drecv, y1s, y1r, y2s, y2r, scaled,
    rowbuf, colbuf, sqrow, sq, obuf, orecv, csend, crecv, totbuf,
    ssem, rsem, lsem,
):
    tok, blk = lax.axis_index("tok"), lax.axis_index("blk")
    c, y, zl = tok % 2, (tok // 2) % 4, tok // 8
    x, zh = blk // 2, blk % 2

    def tok_of(zl_, y_, c_):
        return zl_ * 8 + y_ * 2 + c_

    def blk_of(x_, zh_):
        return x_ * 2 + zh_

    x_plus = (tok, blk_of((x + 1) % 4, zh))
    x_minus = (tok, blk_of((x + 3) % 4, zh))
    zh_mate = (tok, blk_of(x, 1 - zh))
    y_plus = (tok_of(zl, (y + 1) % 4, c), blk)
    y_minus = (tok_of(zl, (y + 3) % 4, c), blk)
    zl_mate = (tok_of(1 - zl, y, c), blk)
    z_cross = (tok_of(1 - zl, y, c), blk_of(x, 1 - zh))
    sibling = (tok_of(zl, y, 1 - c), blk)

    def place(to):
        return {"tok": to[0], "blk": to[1]}

    out_tok = 4 * y + 2 * zh + c
    home = out_tok == tok
    line_slot = 2 * x + zl
    row_block = 2 * y + zh

    def loads(src, dst, first):
        out = []
        for s in range(2):
            for k in range(2):
                cols = pl.ds(HALF * k + PART * s, PART)
                out.append(
                    pltpu.make_async_copy(
                        src.at[:, cols], dst(s).at[:, pl.ds(PART * k, PART)],
                        lsem.at[first + 2 * s + k],
                    )
                )
        return out

    def own_block(s):
        return xall.at[0, x, s]

    def give_block(s):
        return give.at[s]

    def all_loads(own_ref, give_ref):
        return loads(own_ref, own_block, 0) + loads(give_ref, give_block, 4)

    @pl.when(zl == 0)
    def _():
        for copy in all_loads(act_ref, grad_ref):
            copy.start()

    @pl.when(zl == 1)
    def _():
        for copy in all_loads(grad_ref, act_ref):
            copy.start()

    barrier = pltpu.get_barrier_semaphore()

    def greet(to):
        pl.semaphore_signal(barrier, inc=1, device_id=place(to), device_id_type=MESH)

    def greet_tok(j, carry):
        greet(((tok + j) % 16, blk))
        return carry

    def greet_blk(j, carry):
        greet((tok, (blk + j) % 8))
        return carry

    lax.fori_loop(1, 16, greet_tok, 0)
    lax.fori_loop(1, 8, greet_blk, 0)
    greet(z_cross)

    def greet_source(j, carry):
        to = (tok_of(j % 2, tok // 4, c), blk_of(j // 2, (tok // 2) % 2))

        @pl.when(jnp.logical_not((to[0] == tok) & (to[1] == blk)))
        def _():
            greet(to)

        return carry

    lax.fori_loop(0, 8, greet_source, 0)
    for copy in all_loads(act_ref, grad_ref):
        copy.wait()
    pl.semaphore_wait(barrier, 15 + 7 + 1 + 8 - home.astype(jnp.int32))

    sent = []

    def remote(k, src, dst, to, k_there=None):
        return pltpu.make_async_remote_copy(
            src_ref=src, dst_ref=dst, send_sem=ssem.at[k],
            recv_sem=rsem.at[k if k_there is None else k_there],
            device_id=place(to), device_id_type=MESH,
        )

    def send(k, src, dst, to):
        copy = remote(k, src, dst, to)
        copy.start()
        sent.append(copy)

    def wait(k, dst):
        remote(k, dst, dst, sibling).wait_recv()

    token_half = (pl.ds(0, HALF), pl.ds(HALF, HALF))

    def x_line(s, t):
        def ref(step, half):
            return xall.at[t, (x + step) % 4, s, token_half[half]]

        return Line(send, wait, X_ID[s][t], ref, x_plus, x_minus)

    lines = [[x_line(s, t) for t in range(2)] for s in range(2)]

    def z_first(s):
        send(Z_ID + s, give.at[s], xall.at[1, x, s], zl_mate)

    def z_rest(s):
        send(Z_ID + 2 + s, give.at[s], xall.at[1, 4, s], z_cross)
        send(Z_ID + 4 + s, xall.at[0, x, s], xall.at[0, 4, s], zh_mate)

    def z_first_take(s):
        wait(Z_ID + s, xall.at[1, x, s])

    def z_rest_take(s):
        wait(Z_ID + 2 + s, xall.at[1, 4, s])
        wait(Z_ID + 4 + s, xall.at[0, 4, s])

    def column_sums():
        for which, ref in ((zl, own_block), (1 - zl, give_block)):
            for s in range(2):
                values = ref(s)[...].astype(F32)
                total = jnp.sum(values * values, axis=0, keepdims=True)
                for k in range(2):
                    csend[which, :, HALF * k + PART * s : HALF * k + PART * (s + 1)] = total[
                        :, PART * k : PART * (k + 1)
                    ]

    def sum_copy(j):
        return remote(SUM_ID + j, csend, crecv.at[j], ((tok + j) % 16, blk))

    def sums_start():
        def step(j, carry):
            sum_copy(j).start()
            return carry

        lax.fori_loop(1, 16, step, 0)

    total_to = [(tok, blk_of((x + j) % 4, zh)) for j in (1, 2, 3)] + [zh_mate]

    def total_copy(j):
        return remote(TOTAL_ID + j, totbuf.at[x], totbuf.at[x if j < 3 else 4], total_to[j])

    def totals_start():
        def step(j, carry):
            sum_copy(j).wait_recv()
            return carry

        lax.fori_loop(1, 16, step, 0)
        total = csend[...]
        for j in range(1, 16):
            total = total + crecv[j]
        totbuf[x] = total
        for j in range(4):
            total_copy(j).start()

    def totals_finish():
        for j in range(4):
            total_copy(j).wait_recv()

    col_slot = [jnp.where(zh == h, x, 4) for h in range(2)]

    def gram(s):
        def step(i, carry):
            to = (x + 3 + i) % 4
            for h in range(2):
                for s2 in range(2):
                    value = None
                    for t in range(2):
                        term = lax.dot_general(
                            xall[t, to, s], xall[t, col_slot[h], s2],
                            (((0,), (0,)), ((), ())), preferred_element_type=F32,
                        )
                        value = term if value is None else value + term
                    value = value.astype(BF16)
                    for k in range(2):
                        for k2 in range(2):
                            start = HALF * k2 + PART * s2
                            gram_part[s, to, k, h, :, start : start + PART] = value[
                                PART * k : PART * (k + 1), PART * k2 : PART * (k2 + 1)
                            ]
            d_copy(s, to).start()
            return carry

        lax.fori_loop(0, 4, step, 0)

    def d_copy(s, to):
        return remote(
            D_ID[s] + to, gram_part.at[s, to, 1 - c], drecv.at[s, to], sibling
        )

    def both(s, to, h):
        return gram_part[s, to, c, h].astype(F32) + drecv[s, to, h].astype(F32)

    y_far, y_up, y_down = (y + 2) % 4, (y + 1) % 4, (y + 3) % 4

    def reduce_start(s):
        d_copy(s, y_far).wait_recv()
        y1s[s, 0] = both(s, y_far, 0).astype(BF16)
        send(Y1_ID[s] + 0, y1s.at[s, 0], y1r.at[s, 0], y_plus)
        y1s[s, 1] = both(s, y_far, 1).astype(BF16)
        send(Y1_ID[s] + 1, y1s.at[s, 1], y1r.at[s, 1], y_minus)
        d_copy(s, y_up).wait_recv()
        y2s[s, 0] = both(s, y_up, 1).astype(BF16)
        send(Y2_ID[s] + 0, y2s.at[s, 0], y2r.at[s, 0], y_plus)
        d_copy(s, y_down).wait_recv()
        y2s[s, 2] = both(s, y_down, 0).astype(BF16)
        send(Y2_ID[s] + 2, y2s.at[s, 2], y2r.at[s, 2], y_minus)
        d_copy(s, y).wait_recv()

    def reduce_middle(s):
        wait(Y1_ID[s] + 0, y1r.at[s, 0])
        y2s[s, 1] = (both(s, y_up, 0) + y1r[s, 0].astype(F32)).astype(BF16)
        send(Y2_ID[s] + 1, y2s.at[s, 1], y2r.at[s, 1], y_plus)
        wait(Y1_ID[s] + 1, y1r.at[s, 1])
        y2s[s, 3] = (both(s, y_down, 1) + y1r[s, 1].astype(F32)).astype(BF16)
        send(Y2_ID[s] + 3, y2s.at[s, 3], y2r.at[s, 3], y_minus)

    def eye(s, h):
        shape = (PART, BLOCK)
        r = lax.broadcasted_iota(jnp.int32, shape, 0) + BLOCK * row_block + HALF * c + PART * s
        k = lax.broadcasted_iota(jnp.int32, shape, 1) + BLOCK * (2 * x + h)
        return (r == k).astype(F32)

    def inverse(sums):
        return lax.rsqrt(sums / TOKENS + epsilon)

    def lane_block(block):
        return pl.ds(pl.multiple_of(block * BLOCK, BLOCK), BLOCK)

    def normalise(s):
        for k in range(4):
            wait(Y2_ID[s] + k, y2r.at[s, k])
        rows = pl.ds(pl.multiple_of(HALF * c + PART * s, PART), PART)
        inv_row = jnp.broadcast_to(inverse(totbuf[y, zl, :, rows]), (PART, PART))
        inv_row = jnp.concatenate([jnp.transpose(inv_row)] * 4, axis=1)
        for h in range(2):
            inv_col = inverse(totbuf[col_slot[h], zl])
            first, second = ((1, 2), (0, 3))[h]
            g = both(s, y, h) + y2r[s, first].astype(F32) + y2r[s, second].astype(F32)
            damped = g / TOKENS * inv_row * inv_col + damping * eye(s, h)
            value = damped / divisor
            scaled[h, s] = value
            half = value.astype(BF16)
            rowbuf[s, :, lane_block(2 * x + h)] = half
            colbuf[h, row_block, c, s] = half

    def row_line(s):
        def ref(step, half):
            return rowbuf.at[s, :, lane_block(((x + step) % 4) * 2 + half)]

        return Line(send, wait, ROW_ID[s], ref, x_plus, x_minus)

    def col_plane(k, s, h=None):
        def piece(block, core, half):
            if h is None:
                r = colbuf.at[:, block, core, s]
                return r if half is None else r.at[half]
            r = colbuf.at[h, block, core, s]
            return r if half is None else r.at[pl.ds(half * (PART // 2), PART // 2)]

        def ref(step, half, other=0):
            return piece(((y + step) % 4) * 2 + (1 - zh if other else zh), c, half)

        def mirrored(half):
            return piece(0, 1 - c, half)

        return Plane(
            send, wait, COL_ID[k], ref, y_plus, y_minus, zh_mate, sibling, mirrored
        )

    def sq_line(h):
        def ref(step, half):
            return sqrow.at[pl.ds(PART * half, PART), lane_block(((x + step) % 4) * 2 + h)]

        return Line(send, wait, SQ_ID[h], ref, x_plus, x_minus)

    rows = [row_line(s) for s in range(2)]
    cols = [col_plane(0, 0), col_plane(1, 1, 0), col_plane(2, 1, 1)]
    sq_rows = [sq_line(h) for h in range(2)]

    def product(h, left):
        def step(k, carry):
            lanes = pl.ds(pl.multiple_of(k * HALF, HALF), HALF)
            sq[h, :, lanes] = jnp.dot(
                left[...].reshape(HALF, D), colbuf[h, :, :, :, :, lanes].reshape(D, HALF),
                preferred_element_type=F32,
            )
            return carry

        lax.fori_loop(0, 2, step, 0)

    def square(h):
        product(h, rowbuf)
        sqrow[:, lane_block(2 * x + h)] = sq[h].astype(BF16)
        sq_rows[h].start()
        for s in range(2):
            scaled[h, s] = (
                4.0 * eye(s, h) - 6.0 * scaled[h, s] + 4.0 * sq[h, PART * s : PART * (s + 1)]
            )

    def out_copy(h, b):
        return remote(
            OUT_ID[h] + b, obuf.at[h, pl.ds(b * 32, 32)], orecv.at[h, line_slot], (out_tok, b),
            OUT_ID[h] + line_slot,
        )

    def cube(h):
        product(h, sqrow)
        obuf[h] = (scaled[h].reshape(HALF, BLOCK) - sq[h]).astype(BF16)
        for b in range(8):
            me = home & (blk == b)

            @pl.when(me)
            def _():
                orecv[h, line_slot] = obuf[h, b * 32 : (b + 1) * 32]

            @pl.when(jnp.logical_not(me))
            def _():
                out_copy(h, b).start()

    def emit(h):
        for k in range(8):
            @pl.when(jnp.logical_not(home & (line_slot == k)))
            def _():
                wait(OUT_ID[h] + k, orecv.at[h, k])

        for k in range(8):
            out = (act_out, grad_out)[k % 2]
            start = (2 * (k // 2) + h) * BLOCK
            out[:, start : start + BLOCK] = orecv[h, k].astype(F32)

    z_first(0)
    lines[0][0].start()
    column_sums()
    sums_start()
    z_rest(0)
    z_first(1)
    z_rest(1)
    lines[0][0].near()
    z_first_take(0)
    lines[0][1].start()
    totals_start()
    lines[0][1].near()
    lines[1][0].start()
    z_first_take(1)
    lines[1][1].start()
    lines[0][0].finish()
    lines[0][1].finish()
    z_rest_take(0)
    z_rest_take(1)
    gram(0)
    lines[1][0].near()
    reduce_start(0)
    lines[1][1].near()
    reduce_middle(0)
    lines[1][0].finish()
    lines[1][1].finish()
    gram(1)
    totals_finish()
    normalise(0)
    cols[0].start()
    rows[0].start()
    reduce_start(1)
    cols[0].near()
    reduce_middle(1)
    cols[0].other()
    rows[0].near()
    cols[0].far()
    normalise(1)
    cols[1].start()
    rows[1].start()
    cols[0].finish()
    cols[1].near()
    cols[1].other()
    cols[2].start()
    rows[1].near()
    rows[0].finish()
    cols[1].far()
    cols[2].near()
    cols[2].other()
    rows[1].finish()
    cols[1].finish()
    square(0)
    cols[2].far()
    sq_rows[0].near()
    cols[2].finish()
    square(1)
    sq_rows[0].finish()
    sq_rows[1].near()
    sq_rows[1].finish()
    cube(0)
    cube(1)
    emit(0)
    emit(1)

    for copy in sent:
        copy.wait_send()

    def sums_left(j, carry):
        sum_copy(j).wait_send()
        return carry

    lax.fori_loop(1, 16, sums_left, 0)
    for j in range(4):
        total_copy(j).wait_send()
    for h in range(2):
        for k in range(4):
            d_copy(h, k).wait_send()
        for b in range(8):
            @pl.when(jnp.logical_not(home & (blk == b)))
            def _():
                out_copy(h, b).wait_send()


def body(activations, out_grads):
    hbm = pl.BlockSpec(memory_space=pltpu.HBM)
    vmem = pl.BlockSpec(memory_space=pltpu.VMEM)
    out = jax.ShapeDtypeStruct((32, D), F32)
    part = (PART, BLOCK)
    scratch = [
        pltpu.VMEM((2, 5, 2, BLOCK, HALF), BF16),
        pltpu.VMEM((2, BLOCK, HALF), BF16),
        pltpu.VMEM((2, 4, 2, 2, *part), BF16),
        pltpu.VMEM((2, 4, 2, *part), BF16),
        pltpu.VMEM((2, 2, *part), BF16),
        pltpu.VMEM((2, 2, *part), BF16),
        pltpu.VMEM((2, 4, *part), BF16),
        pltpu.VMEM((2, 4, *part), BF16),
        pltpu.VMEM((2, 2, *part), F32),
        pltpu.VMEM((2, PART, D), BF16),
        pltpu.VMEM((2, 8, 2, 2, *part), BF16),
        pltpu.VMEM((HALF, D), BF16),
        pltpu.VMEM((2, HALF, BLOCK), F32),
        pltpu.VMEM((2, HALF, BLOCK), BF16),
        pltpu.VMEM((2, 8, 32, BLOCK), BF16),
        pltpu.VMEM((2, 1, BLOCK), F32),
        pltpu.VMEM((16, 2, 1, BLOCK), F32),
        pltpu.VMEM((5, 2, 1, BLOCK), F32),
        pltpu.SemaphoreType.DMA((N_ID,)),
        pltpu.SemaphoreType.DMA((N_ID,)),
        pltpu.SemaphoreType.DMA((8,)),
    ]
    return pl.pallas_call(
        kernel,
        out_shape=(out, out),
        in_specs=[hbm, hbm],
        out_specs=(vmem, vmem),
        scratch_shapes=scratch,
        compiler_params=pltpu.CompilerParams(
            collective_id=0, has_side_effects=True, vmem_limit_bytes=62 * 1024 * 1024
        ),
    )(activations, out_grads)


def solution(mesh):
    placed = (P("tok", "blk"), P("tok", "blk"))
    return jax.shard_map(
        body,
        mesh=mesh,
        in_specs=placed,
        out_specs=(P(("tok", "blk"), None), P(("tok", "blk"), None)),
        check_vma=False,
    )
```

```python
import jax
import jax.numpy as jnp
from jax import lax
from jax.experimental import pallas as pl
from jax.experimental.pallas import tpu as pltpu
from jax.sharding import PartitionSpec as P

D = 4096
TOKENS = 8192
BLOCK = 512
HALF = 256
PART = 128

damping = 0.3
epsilon = 1e-06
divisor = 2.0

MESH = pl.DeviceIdType.MESH
F32 = jnp.float32
BF16 = jnp.bfloat16


class Ids:
    def __init__(self):
        self.next = 0

    def take(self, n):
        first = self.next
        self.next += n
        return first


IDS = Ids()
Z_ID = IDS.take(6)
X_ID = [[IDS.take(6) for _ in range(2)] for _ in range(2)]
D_ID = [[IDS.take(4) for _ in range(2)] for _ in range(2)]
Y1_ID = [[IDS.take(2) for _ in range(2)] for _ in range(2)]
Y2_ID = [[IDS.take(4) for _ in range(2)] for _ in range(2)]
ROW_ID = [IDS.take(6) for _ in range(2)]
COL_ID = [IDS.take(23) for _ in range(3)]
SQ_ID = [IDS.take(6) for _ in range(2)]
OUT_ID = [IDS.take(8) for _ in range(2)]
SUM_ID = IDS.take(16)
TOTAL_ID = IDS.take(4)
N_ID = IDS.next


class Line:
    arrivals = [(3, 0), (3, 1), (1, 1), (1, 0), (2, 0), (2, 1)]

    def __init__(self, send, wait, base, ref, plus, minus, arrived=None):
        self.send, self.wait, self.base, self.ref = send, wait, base, ref
        self.plus, self.minus, self.arrived = plus, minus, arrived

    def put(self, k, where, to):
        r = self.ref(*where)
        self.send(self.base + k, r, r, to)

    def take(self, k):
        r = self.ref(*self.arrivals[k])
        self.wait(self.base + k, r)
        if self.arrived is not None:
            self.arrived(k, r)

    def start(self):
        self.put(0, (0, 0), self.plus)
        self.put(2, (0, 1), self.minus)
        self.put(1, (0, 1), self.plus)
        self.put(3, (0, 0), self.minus)

    def near(self):
        self.take(0)
        self.put(4, (3, 0), self.plus)
        self.take(2)
        self.put(5, (1, 1), self.minus)

    def finish(self):
        for k in (1, 3, 4, 5):
            self.take(k)


class Plane(Line):
    arrivals = Line.arrivals + [
        (0, None, 1), (3, None, 1), (1, None, 1), (2, 0, 1), (2, 1, 1)
    ]

    def __init__(self, send, wait, base, ref, plus, minus, across, sibling, mirrored):
        super().__init__(send, wait, base, ref, plus, minus, self.pass_on)
        self.across, self.sibling, self.mirrored = across, sibling, mirrored

    def pass_on(self, k, r):
        self.send(self.base + 12 + k, r, r, self.sibling)

    def start(self):
        super().start()
        self.put(6, (0, None, 0), self.across)
        self.send(self.base + 11, self.ref(0, None, 0), self.ref(0, None, 0), self.sibling)

    def other(self):
        self.take(6)
        self.put(7, (0, None, 1), self.plus)
        self.put(8, (0, None, 1), self.minus)
        self.take(1)
        self.take(3)

    def far(self):
        self.take(4)
        self.put(9, (2, 0, 0), self.across)
        self.take(5)
        self.put(10, (2, 1, 0), self.across)

    def finish(self):
        for k in (7, 8, 9, 10):
            self.take(k)
        for k in range(11, 23):
            half = None if k in (11, 18, 19, 20) else 0
            self.wait(self.base + k, self.mirrored(half))


def kernel(
    act_ref, grad_ref, out_ref,
    xall, give, gram_part, drecv, y1s, y1r, y2s, y2r, scaled,
    rowbuf, colbuf, sqrow, sq, obuf, csend, crecv, totbuf,
    ssem, rsem, lsem,
):
    tok, blk = lax.axis_index("tok"), lax.axis_index("blk")
    c, y, zl = tok % 2, (tok // 2) % 4, tok // 8
    x, zh = blk // 2, blk % 2

    def tok_of(zl_, y_, c_):
        return zl_ * 8 + y_ * 2 + c_

    def blk_of(x_, zh_):
        return x_ * 2 + zh_

    x_plus = (tok, blk_of((x + 1) % 4, zh))
    x_minus = (tok, blk_of((x + 3) % 4, zh))
    zh_mate = (tok, blk_of(x, 1 - zh))
    y_plus = (tok_of(zl, (y + 1) % 4, c), blk)
    y_minus = (tok_of(zl, (y + 3) % 4, c), blk)
    zl_mate = (tok_of(1 - zl, y, c), blk)
    z_cross = (tok_of(1 - zl, y, c), blk_of(x, 1 - zh))
    sibling = (tok_of(zl, y, 1 - c), blk)

    def place(to):
        return {"tok": to[0], "blk": to[1]}

    def row_of(s, zh_, y_):
        if s == 0:
            return (y_ % 2) * 2 + y_ // 2
        return (y_ // 2) * 2 + (y_ % 2 + y_ // 2 + zh_) % 2

    def line_of(zh_, x_):
        return (
            (x_ % 2) * 2 + x_ // 2,
            (x_ // 2) * 2 + (x_ % 2 + x_ // 2 + zh_) % 2,
        )

    row_block = [2 * row_of(s, zh, y) + zh for s in range(2)]
    out_tok = [2 * row_block[s] + c for s in range(2)]
    my_set = blk // 4
    home = jnp.where(my_set == 0, out_tok[0], out_tok[1]) == tok
    line_slot = 2 * x + zl

    def loads(src, dst, first):
        out = []
        for s in range(2):
            for k in range(2):
                cols = pl.ds(HALF * k + PART * s, PART)
                out.append(
                    pltpu.make_async_copy(
                        src.at[:, cols], dst(s).at[:, pl.ds(PART * k, PART)],
                        lsem.at[first + 2 * s + k],
                    )
                )
        return out

    def own_block(s):
        return xall.at[0, x, s]

    def give_block(s):
        return give.at[s]

    def all_loads(own_ref, give_ref):
        return loads(own_ref, own_block, 0) + loads(give_ref, give_block, 4)

    @pl.when(zl == 0)
    def _():
        for copy in all_loads(act_ref, grad_ref):
            copy.start()

    @pl.when(zl == 1)
    def _():
        for copy in all_loads(grad_ref, act_ref):
            copy.start()

    barrier = pltpu.get_barrier_semaphore()

    def greet(to):
        pl.semaphore_signal(barrier, inc=1, device_id=place(to), device_id_type=MESH)

    def greet_tok(j, carry):
        greet(((tok + j) % 16, blk))
        return carry

    def greet_blk(j, carry):
        greet((tok, (blk + j) % 8))
        return carry

    lax.fori_loop(1, 16, greet_tok, 0)
    lax.fori_loop(1, 8, greet_blk, 0)
    greet(z_cross)

    def greet_source(j, carry):
        zh_ = (tok // 2) % 2
        y_of = line_of(zh_, tok // 4)
        to = (tok_of(j % 2, jnp.where(my_set == 0, y_of[0], y_of[1]), c), blk_of(j // 2, zh_))

        @pl.when(jnp.logical_not((to[0] == tok) & (to[1] == blk)))
        def _():
            greet(to)

        return carry

    lax.fori_loop(0, 8, greet_source, 0)
    for copy in all_loads(act_ref, grad_ref):
        copy.wait()
    pl.semaphore_wait(barrier, 15 + 7 + 1 + 8 - home.astype(jnp.int32))

    sent = []

    def remote(k, src, dst, to, k_there=None):
        return pltpu.make_async_remote_copy(
            src_ref=src, dst_ref=dst, send_sem=ssem.at[k],
            recv_sem=rsem.at[k if k_there is None else k_there],
            device_id=place(to), device_id_type=MESH,
        )

    def send(k, src, dst, to):
        copy = remote(k, src, dst, to)
        copy.start()
        sent.append(copy)

    def wait(k, dst):
        remote(k, dst, dst, sibling).wait_recv()

    token_half = (pl.ds(0, HALF), pl.ds(HALF, HALF))

    def x_line(s, t):
        def ref(step, half):
            return xall.at[t, (x + step) % 4, s, token_half[half]]

        return Line(send, wait, X_ID[s][t], ref, x_plus, x_minus)

    lines = [[x_line(s, t) for t in range(2)] for s in range(2)]

    def z_first(s):
        send(Z_ID + s, give.at[s], xall.at[1, x, s], zl_mate)

    def z_rest(s):
        send(Z_ID + 2 + s, give.at[s], xall.at[1, 4, s], z_cross)
        send(Z_ID + 4 + s, xall.at[0, x, s], xall.at[0, 4, s], zh_mate)

    def z_first_take(s):
        wait(Z_ID + s, xall.at[1, x, s])

    def z_rest_take(s):
        wait(Z_ID + 2 + s, xall.at[1, 4, s])
        wait(Z_ID + 4 + s, xall.at[0, 4, s])

    def column_sums():
        for which, ref in ((zl, own_block), (1 - zl, give_block)):
            for s in range(2):
                values = ref(s)[...].astype(F32)
                total = jnp.sum(values * values, axis=0, keepdims=True)
                for k in range(2):
                    csend[which, :, HALF * k + PART * s : HALF * k + PART * (s + 1)] = total[
                        :, PART * k : PART * (k + 1)
                    ]

    def sum_copy(j):
        return remote(SUM_ID + j, csend, crecv.at[j], ((tok + j) % 16, blk))

    def sums_start():
        def step(j, carry):
            sum_copy(j).start()
            return carry

        lax.fori_loop(1, 16, step, 0)

    total_to = [(tok, blk_of((x + j) % 4, zh)) for j in (1, 2, 3)] + [zh_mate]

    def total_copy(j):
        return remote(TOTAL_ID + j, totbuf.at[x], totbuf.at[x if j < 3 else 4], total_to[j])

    def totals_start():
        def step(j, carry):
            sum_copy(j).wait_recv()
            return carry

        lax.fori_loop(1, 16, step, 0)
        total = csend[...]
        for j in range(1, 16):
            total = total + crecv[j]
        totbuf[x] = total
        for j in range(4):
            total_copy(j).start()

    def totals_finish():
        for j in range(4):
            total_copy(j).wait_recv()

    def gram(s, g):
        cols = (x, 4)[g]

        def step(i, carry):
            to = (x + 3 + i) % 4
            for s2 in range(2):
                value = None
                for t in range(2):
                    term = lax.dot_general(
                        xall[t, to, s], xall[t, cols, s2],
                        (((0,), (0,)), ((), ())), preferred_element_type=F32,
                    )
                    value = term if value is None else value + term
                value = value.astype(BF16)
                for k in range(2):
                    for k2 in range(2):
                        start = HALF * k2 + PART * s2
                        gram_part[s, g, to, k, :, start : start + PART] = value[
                            PART * k : PART * (k + 1), PART * k2 : PART * (k2 + 1)
                        ]
            d_copy(s, g, to).start()
            return carry

        lax.fori_loop(0, 4, step, 0)

    def d_copy(s, g, to):
        return remote(
            D_ID[s][g] + to, gram_part.at[s, g, to, 1 - c], drecv.at[s, g, to], sibling
        )

    halves = (pl.ds(0, PART // 2), pl.ds(PART // 2, PART // 2))

    def both(s, g, to, half):
        mine = gram_part[s, g, to, c, halves[half]].astype(F32)
        return mine + drecv[s, g, to, halves[half]].astype(F32)

    def keep(s, step):
        return row_of(s, zh, (y + step) % 4)

    def reduce_start(s, g):
        y1, y2, far, up, down = Y1_ID[s][g], Y2_ID[s][g], keep(s, 2), keep(s, 1), keep(s, 3)
        d_copy(s, g, far).wait_recv()
        y1s[s, g, 0] = both(s, g, far, 0).astype(BF16)
        send(y1, y1s.at[s, g, 0], y1r.at[s, g, 0], y_plus)
        y1s[s, g, 1] = both(s, g, far, 1).astype(BF16)
        send(y1 + 1, y1s.at[s, g, 1], y1r.at[s, g, 1], y_minus)
        d_copy(s, g, up).wait_recv()
        y2s[s, g, 0] = both(s, g, up, 1).astype(BF16)
        send(y2, y2s.at[s, g, 0], y2r.at[s, g, 0], y_plus)
        d_copy(s, g, down).wait_recv()
        y2s[s, g, 2] = both(s, g, down, 0).astype(BF16)
        send(y2 + 2, y2s.at[s, g, 2], y2r.at[s, g, 2], y_minus)
        d_copy(s, g, keep(s, 0)).wait_recv()

    def reduce_middle(s, g):
        y1, y2, up, down = Y1_ID[s][g], Y2_ID[s][g], keep(s, 1), keep(s, 3)
        wait(y1, y1r.at[s, g, 0])
        y2s[s, g, 1] = (both(s, g, up, 0) + y1r[s, g, 0].astype(F32)).astype(BF16)
        send(y2 + 1, y2s.at[s, g, 1], y2r.at[s, g, 1], y_plus)
        wait(y1 + 1, y1r.at[s, g, 1])
        y2s[s, g, 3] = (both(s, g, down, 1) + y1r[s, g, 1].astype(F32)).astype(BF16)
        send(y2 + 3, y2s.at[s, g, 3], y2r.at[s, g, 3], y_minus)

    def eye(s, h):
        shape = (PART, BLOCK)
        r = lax.broadcasted_iota(jnp.int32, shape, 0) + BLOCK * row_block[s] + HALF * c + PART * s
        k = lax.broadcasted_iota(jnp.int32, shape, 1) + BLOCK * (2 * x + h)
        return (r == k).astype(F32)

    def inverse(sums):
        return lax.rsqrt(sums / TOKENS + epsilon)

    def lane_block(block):
        return pl.ds(pl.multiple_of(block * BLOCK, BLOCK), BLOCK)

    def normalise(s):
        rows = pl.ds(pl.multiple_of(HALF * c + PART * s, PART), PART)
        inv_row = jnp.broadcast_to(inverse(totbuf[keep(s, 0), zl, :, rows]), (PART, PART))
        inv_row = jnp.concatenate([jnp.transpose(inv_row)] * 4, axis=1)
        for g in range(2):
            for k in range(4):
                wait(Y2_ID[s][g] + k, y2r.at[s, g, k])
            h = zh if g == 0 else 1 - zh
            inv_col = inverse(totbuf[(x, 4)[g], zl])
            low = both(s, g, keep(s, 0), 0) + y2r[s, g, 1].astype(F32) + y2r[s, g, 2].astype(F32)
            high = both(s, g, keep(s, 0), 1) + y2r[s, g, 0].astype(F32) + y2r[s, g, 3].astype(F32)
            total = jnp.concatenate([low, high], axis=0)
            damped = total / TOKENS * inv_row * inv_col + damping * eye(s, h)
            value = damped / divisor
            scaled[h, s] = value
            half = value.astype(BF16)
            rowbuf[s, :, lane_block(2 * x + h)] = half
            colbuf[h, row_block[s], c, s] = half

    def row_line(s):
        def ref(step, half):
            return rowbuf.at[s, :, lane_block(((x + step) % 4) * 2 + half)]

        return Line(send, wait, ROW_ID[s], ref, x_plus, x_minus)

    def col_plane(k, s, h=None):
        def piece(block, core, half):
            if h is None:
                r = colbuf.at[:, block, core, s]
                return r if half is None else r.at[half]
            r = colbuf.at[h, block, core, s]
            return r if half is None else r.at[halves[half]]

        def ref(step, half, other=0):
            zh_ = 1 - zh if other else zh
            return piece(2 * row_of(s, zh_, (y + step) % 4) + zh_, c, half)

        def mirrored(half):
            return piece(0, 1 - c, half)

        return Plane(
            send, wait, COL_ID[k], ref, y_plus, y_minus, zh_mate, sibling, mirrored
        )

    def sq_line(h):
        def ref(step, half):
            return sqrow.at[pl.ds(PART * half, PART), lane_block(((x + step) % 4) * 2 + h)]

        return Line(send, wait, SQ_ID[h], ref, x_plus, x_minus)

    rows = [row_line(s) for s in range(2)]
    cols = [col_plane(0, 0), col_plane(1, 1, 0), col_plane(2, 1, 1)]
    sq_rows = [sq_line(h) for h in range(2)]

    def product(h, left):
        def step(k, carry):
            lanes = pl.ds(pl.multiple_of(k * HALF, HALF), HALF)
            sq[h, :, lanes] = jnp.dot(
                left[...].reshape(HALF, D), colbuf[h, :, :, :, :, lanes].reshape(D, HALF),
                preferred_element_type=F32,
            )
            return carry

        lax.fori_loop(0, 2, step, 0)

    def square(h):
        product(h, rowbuf)
        sqrow[:, lane_block(2 * x + h)] = sq[h].astype(BF16)
        sq_rows[h].start()
        for s in range(2):
            scaled[h, s] = (
                4.0 * eye(s, h) - 6.0 * scaled[h, s] + 4.0 * sq[h, PART * s : PART * (s + 1)]
            )

    def out_copy(h, b):
        return remote(
            OUT_ID[h] + b, obuf.at[h, pl.ds(b * 32, 32)],
            out_ref.at[zl, :, lane_block(2 * x + h)], (out_tok[b // 4], b),
            OUT_ID[h] + line_slot,
        )

    def cube(h):
        product(h, sqrow)
        obuf[h] = (scaled[h].reshape(HALF, BLOCK) - sq[h]).astype(BF16)
        for b in range(8):
            me = home & (blk == b)

            @pl.when(me)
            def _():
                out_ref[zl, :, lane_block(2 * x + h)] = obuf[h, b * 32 : (b + 1) * 32]

            @pl.when(jnp.logical_not(me))
            def _():
                out_copy(h, b).start()

    def emit(h):
        for k in range(8):
            @pl.when(jnp.logical_not(home & (line_slot == k)))
            def _():
                wait(OUT_ID[h] + k, out_ref.at[k % 2, :, pl.ds((2 * (k // 2) + h) * BLOCK, BLOCK)])

    z_first(0)
    lines[0][0].start()
    column_sums()
    sums_start()
    z_first(1)
    z_rest(0)
    z_rest(1)
    lines[0][0].near()
    z_first_take(0)
    lines[0][1].start()
    totals_start()
    lines[0][1].near()
    lines[1][0].start()
    z_first_take(1)
    lines[1][1].start()
    lines[0][0].finish()
    lines[0][1].finish()
    gram(0, 0)
    reduce_start(0, 0)
    lines[1][0].near()
    z_rest_take(0)
    z_rest_take(1)
    gram(0, 1)
    reduce_middle(0, 0)
    reduce_start(0, 1)
    lines[1][1].near()
    reduce_middle(0, 1)
    totals_finish()
    normalise(0)
    cols[0].start()
    rows[0].start()
    lines[1][0].finish()
    lines[1][1].finish()
    gram(1, 0)
    gram(1, 1)
    reduce_start(1, 0)
    reduce_start(1, 1)
    cols[0].near()
    reduce_middle(1, 0)
    reduce_middle(1, 1)
    cols[0].other()
    rows[0].near()
    cols[0].far()
    normalise(1)
    cols[1].start()
    rows[1].start()
    cols[1].near()
    cols[2].start()
    cols[1].other()
    rows[1].near()
    cols[1].far()
    cols[2].near()
    cols[2].other()
    cols[0].finish()
    rows[0].finish()
    rows[1].finish()
    cols[1].finish()
    square(0)
    cols[2].far()
    sq_rows[0].near()
    cols[2].finish()
    square(1)
    sq_rows[0].finish()
    sq_rows[1].near()
    sq_rows[1].finish()
    cube(0)
    cube(1)
    emit(0)
    emit(1)

    for copy in sent:
        copy.wait_send()

    def sums_left(j, carry):
        sum_copy(j).wait_send()
        return carry

    lax.fori_loop(1, 16, sums_left, 0)
    for j in range(4):
        total_copy(j).wait_send()
    for h in range(2):
        for k in range(8):
            d_copy(h, k // 4, k % 4).wait_send()
        for b in range(8):
            @pl.when(jnp.logical_not(home & (blk == b)))
            def _():
                out_copy(h, b).wait_send()


def body(activations, out_grads):
    hbm = pl.BlockSpec(memory_space=pltpu.HBM)
    vmem = pl.BlockSpec(memory_space=pltpu.VMEM)
    part = (PART, BLOCK)
    half_part = (PART // 2, BLOCK)
    scratch = [
        pltpu.VMEM((2, 5, 2, BLOCK, HALF), BF16),
        pltpu.VMEM((2, BLOCK, HALF), BF16),
        pltpu.VMEM((2, 2, 4, 2, *part), BF16),
        pltpu.VMEM((2, 2, 4, *part), BF16),
        pltpu.VMEM((2, 2, 2, *half_part), BF16),
        pltpu.VMEM((2, 2, 2, *half_part), BF16),
        pltpu.VMEM((2, 2, 4, *half_part), BF16),
        pltpu.VMEM((2, 2, 4, *half_part), BF16),
        pltpu.VMEM((2, 2, *part), F32),
        pltpu.VMEM((2, PART, D), BF16),
        pltpu.VMEM((2, 8, 2, 2, *part), BF16),
        pltpu.VMEM((HALF, D), BF16),
        pltpu.VMEM((2, HALF, BLOCK), F32),
        pltpu.VMEM((2, HALF, BLOCK), BF16),
        pltpu.VMEM((2, 1, BLOCK), F32),
        pltpu.VMEM((16, 2, 1, BLOCK), F32),
        pltpu.VMEM((5, 2, 1, BLOCK), F32),
        pltpu.SemaphoreType.DMA((N_ID,)),
        pltpu.SemaphoreType.DMA((N_ID,)),
        pltpu.SemaphoreType.DMA((8,)),
    ]
    out = pl.pallas_call(
        kernel,
        out_shape=jax.ShapeDtypeStruct((2, 32, D), BF16),
        in_specs=[hbm, hbm],
        out_specs=vmem,
        scratch_shapes=scratch,
        compiler_params=pltpu.CompilerParams(
            collective_id=0, has_side_effects=True, vmem_limit_bytes=60 * 1024 * 1024
        ),
    )(activations, out_grads)
    return out[0].astype(F32), out[1].astype(F32)


def solution(mesh):
    placed = (P("tok", "blk"), P("tok", "blk"))
    return jax.shard_map(
        body,
        mesh=mesh,
        in_specs=placed,
        out_specs=(P(("tok", "blk"), None), P(("tok", "blk"), None)),
        check_vma=False,
    )
```

```python
import jax
import jax.numpy as jnp
from jax import lax
from jax.experimental import pallas as pl
from jax.experimental.pallas import tpu as pltpu
from jax.sharding import PartitionSpec as P

D = 4096
TOKENS = 8192
BLOCK = 512
HALF = 256
PART = 128

damping = 0.3
epsilon = 1e-06
divisor = 2.0

MESH = pl.DeviceIdType.MESH
F32 = jnp.float32
BF16 = jnp.bfloat16


class Ids:
    def __init__(self):
        self.next = 0

    def take(self, n):
        first = self.next
        self.next += n
        return first


IDS = Ids()
Z_ID = IDS.take(6)
X_ID = [[IDS.take(6) for _ in range(2)] for _ in range(2)]
D_ID = [[IDS.take(4) for _ in range(2)] for _ in range(2)]
Y1_ID = [[IDS.take(2) for _ in range(2)] for _ in range(2)]
Y2_ID = [[IDS.take(4) for _ in range(2)] for _ in range(2)]
ROW_ID = [IDS.take(6) for _ in range(2)]
COL_ID = [IDS.take(23) for _ in range(3)]
SQ_ID = [IDS.take(6) for _ in range(3)]
OUT_ID = IDS.take(8)
SUM_ID = IDS.take(16)
TOTAL_ID = IDS.take(4)
N_ID = IDS.next


class Line:
    arrivals = [(3, 0), (3, 1), (1, 1), (1, 0), (2, 0), (2, 1)]

    def __init__(self, send, wait, base, ref, plus, minus, arrived=None):
        self.send, self.wait, self.base, self.ref = send, wait, base, ref
        self.plus, self.minus, self.arrived = plus, minus, arrived

    def put(self, k, where, to):
        r = self.ref(*where)
        self.send(self.base + k, r, r, to)

    def take(self, k):
        r = self.ref(*self.arrivals[k])
        self.wait(self.base + k, r)
        if self.arrived is not None:
            self.arrived(k, r)

    def start(self):
        self.put(0, (0, 0), self.plus)
        self.put(2, (0, 1), self.minus)
        self.put(1, (0, 1), self.plus)
        self.put(3, (0, 0), self.minus)

    def near(self):
        self.take(0)
        self.put(4, (3, 0), self.plus)
        self.take(2)
        self.put(5, (1, 1), self.minus)

    def finish(self):
        for k in (1, 3, 4, 5):
            self.take(k)


class Plane(Line):
    arrivals = Line.arrivals + [
        (0, None, 1), (3, None, 1), (1, None, 1), (2, 0, 1), (2, 1, 1)
    ]

    def __init__(self, send, wait, base, ref, plus, minus, across, sibling, mirrored):
        super().__init__(send, wait, base, ref, plus, minus, self.pass_on)
        self.across, self.sibling, self.mirrored = across, sibling, mirrored

    def pass_on(self, k, r):
        self.send(self.base + 12 + k, r, r, self.sibling)

    def start(self):
        super().start()
        self.put(6, (0, None, 0), self.across)
        self.send(self.base + 11, self.ref(0, None, 0), self.ref(0, None, 0), self.sibling)

    def other(self):
        self.take(6)
        self.put(7, (0, None, 1), self.plus)
        self.put(8, (0, None, 1), self.minus)

    def rest(self):
        self.take(1)
        self.take(3)

    def far(self):
        self.take(4)
        self.put(9, (2, 0, 0), self.across)
        self.take(5)
        self.put(10, (2, 1, 0), self.across)

    def last(self):
        for k in (7, 8, 9, 10):
            self.take(k)

    def passed(self):
        for k in range(11, 23):
            half = None if k in (11, 18, 19, 20) else 0
            self.wait(self.base + k, self.mirrored(half))


def kernel(
    act_ref, grad_ref, out_ref,
    xall, give, gram_part, drecv, y1s, y1r, y2s, y2r, scaled,
    rowbuf, colbuf, sqrow, sq, obuf, csend, crecv, totbuf,
    ssem, rsem, lsem,
):
    tok, blk = lax.axis_index("tok"), lax.axis_index("blk")
    c, y, zl = tok % 2, (tok // 2) % 4, tok // 8
    x, zh = blk // 2, blk % 2

    def tok_of(zl_, y_, c_):
        return zl_ * 8 + y_ * 2 + c_

    def blk_of(x_, zh_):
        return x_ * 2 + zh_

    x_plus = (tok, blk_of((x + 1) % 4, zh))
    x_minus = (tok, blk_of((x + 3) % 4, zh))
    zh_mate = (tok, blk_of(x, 1 - zh))
    y_plus = (tok_of(zl, (y + 1) % 4, c), blk)
    y_minus = (tok_of(zl, (y + 3) % 4, c), blk)
    zl_mate = (tok_of(1 - zl, y, c), blk)
    z_cross = (tok_of(1 - zl, y, c), blk_of(x, 1 - zh))
    sibling = (tok_of(zl, y, 1 - c), blk)

    def place(to):
        return {"tok": to[0], "blk": to[1]}

    def row_of(s, zh_, y_):
        if s == 0:
            return (y_ % 2) * 2 + y_ // 2
        return (y_ // 2) * 2 + (y_ % 2 + y_ // 2 + zh_) % 2

    def line_of(zh_, x_):
        return (
            (x_ % 2) * 2 + x_ // 2,
            (x_ // 2) * 2 + (x_ % 2 + x_ // 2 + zh_) % 2,
        )

    row_block = [2 * row_of(s, zh, y) + zh for s in range(2)]
    out_tok = [2 * row_block[s] + c for s in range(2)]
    my_set = blk // 4
    home = jnp.where(my_set == 0, out_tok[0], out_tok[1]) == tok
    line_slot = 2 * x + zl

    def loads(src, dst, first):
        out = []
        for s in range(2):
            for k in range(2):
                cols = pl.ds(HALF * k + PART * s, PART)
                out.append(
                    pltpu.make_async_copy(
                        src.at[:, cols], dst(s).at[:, pl.ds(PART * k, PART)],
                        lsem.at[first + 2 * s + k],
                    )
                )
        return out

    def own_block(s):
        return xall.at[0, x, s]

    def give_block(s):
        return give.at[s]

    def all_loads(own_ref, give_ref):
        return loads(own_ref, own_block, 0) + loads(give_ref, give_block, 4)

    @pl.when(zl == 0)
    def _():
        for copy in all_loads(act_ref, grad_ref):
            copy.start()

    @pl.when(zl == 1)
    def _():
        for copy in all_loads(grad_ref, act_ref):
            copy.start()

    barrier = pltpu.get_barrier_semaphore()

    def greet(to):
        pl.semaphore_signal(barrier, inc=1, device_id=place(to), device_id_type=MESH)

    def greet_tok(j, carry):
        greet(((tok + j) % 16, blk))
        return carry

    def greet_blk(j, carry):
        greet((tok, (blk + j) % 8))
        return carry

    lax.fori_loop(1, 16, greet_tok, 0)
    lax.fori_loop(1, 8, greet_blk, 0)
    greet(z_cross)

    def greet_source(j, carry):
        zh_ = (tok // 2) % 2
        y_of = line_of(zh_, tok // 4)
        to = (tok_of(j % 2, jnp.where(my_set == 0, y_of[0], y_of[1]), c), blk_of(j // 2, zh_))

        @pl.when(jnp.logical_not((to[0] == tok) & (to[1] == blk)))
        def _():
            greet(to)

        return carry

    lax.fori_loop(0, 8, greet_source, 0)
    for copy in all_loads(act_ref, grad_ref):
        copy.wait()
    pl.semaphore_wait(barrier, 15 + 7 + 1 + 8 - home.astype(jnp.int32))

    sent = []

    def remote(k, src, dst, to, k_there=None):
        return pltpu.make_async_remote_copy(
            src_ref=src, dst_ref=dst, send_sem=ssem.at[k],
            recv_sem=rsem.at[k if k_there is None else k_there],
            device_id=place(to), device_id_type=MESH,
        )

    def send(k, src, dst, to):
        copy = remote(k, src, dst, to)
        copy.start()
        sent.append(copy)

    def wait(k, dst):
        remote(k, dst, dst, sibling).wait_recv()

    token_half = (pl.ds(0, HALF), pl.ds(HALF, HALF))

    def x_line(s, t):
        def ref(step, half):
            return xall.at[t, (x + step) % 4, s, token_half[half]]

        return Line(send, wait, X_ID[s][t], ref, x_plus, x_minus)

    lines = [[x_line(s, t) for t in range(2)] for s in range(2)]

    def z_first(s):
        send(Z_ID + s, give.at[s], xall.at[1, x, s], zl_mate)

    def z_rest(s):
        send(Z_ID + 2 + s, give.at[s], xall.at[1, 4, s], z_cross)
        send(Z_ID + 4 + s, xall.at[0, x, s], xall.at[0, 4, s], zh_mate)

    def z_first_take(s):
        wait(Z_ID + s, xall.at[1, x, s])

    def z_rest_take(s):
        wait(Z_ID + 2 + s, xall.at[1, 4, s])
        wait(Z_ID + 4 + s, xall.at[0, 4, s])

    def column_sums():
        for which, ref in ((zl, own_block), (1 - zl, give_block)):
            for s in range(2):
                values = ref(s)[...].astype(F32)
                total = jnp.sum(values * values, axis=0, keepdims=True)
                for k in range(2):
                    csend[which, :, HALF * k + PART * s : HALF * k + PART * (s + 1)] = total[
                        :, PART * k : PART * (k + 1)
                    ]

    def sum_copy(j):
        return remote(SUM_ID + j, csend, crecv.at[j], ((tok + j) % 16, blk))

    def sums_start():
        def step(j, carry):
            sum_copy(j).start()
            return carry

        lax.fori_loop(1, 16, step, 0)

    total_to = [(tok, blk_of((x + j) % 4, zh)) for j in (1, 2, 3)] + [zh_mate]

    def total_copy(j):
        return remote(TOTAL_ID + j, totbuf.at[x], totbuf.at[x if j < 3 else 4], total_to[j])

    def totals_start():
        def step(j, carry):
            sum_copy(j).wait_recv()
            return carry

        lax.fori_loop(1, 16, step, 0)
        total = csend[...]
        for j in range(1, 16):
            total = total + crecv[j]
        totbuf[x] = total
        for j in range(4):
            total_copy(j).start()

    def totals_finish():
        for j in range(4):
            total_copy(j).wait_recv()

    def gram(s, g):
        cols = (x, 4)[g]

        def step(i, carry):
            to = (x + 3 + i) % 4
            for s2 in range(2):
                value = None
                for t in range(2):
                    term = lax.dot_general(
                        xall[t, to, s], xall[t, cols, s2],
                        (((0,), (0,)), ((), ())), preferred_element_type=F32,
                    )
                    value = term if value is None else value + term
                value = value.astype(BF16)
                for k in range(2):
                    for k2 in range(2):
                        start = HALF * k2 + PART * s2
                        gram_part[s, g, to, k, :, start : start + PART] = value[
                            PART * k : PART * (k + 1), PART * k2 : PART * (k2 + 1)
                        ]
            d_copy(s, g, to).start()
            return carry

        lax.fori_loop(0, 4, step, 0)

    def d_copy(s, g, to):
        return remote(
            D_ID[s][g] + to, gram_part.at[s, g, to, 1 - c], drecv.at[s, g, to], sibling
        )

    halves = (pl.ds(0, PART // 2), pl.ds(PART // 2, PART // 2))

    def both(s, g, to, half):
        mine = gram_part[s, g, to, c, halves[half]].astype(F32)
        return mine + drecv[s, g, to, halves[half]].astype(F32)

    def keep(s, step):
        return row_of(s, zh, (y + step) % 4)

    def reduce_start(s, g):
        y1, y2, far, up, down = Y1_ID[s][g], Y2_ID[s][g], keep(s, 2), keep(s, 1), keep(s, 3)
        d_copy(s, g, far).wait_recv()
        y1s[s, g, 0] = both(s, g, far, 0).astype(BF16)
        send(y1, y1s.at[s, g, 0], y1r.at[s, g, 0], y_plus)
        y1s[s, g, 1] = both(s, g, far, 1).astype(BF16)
        send(y1 + 1, y1s.at[s, g, 1], y1r.at[s, g, 1], y_minus)
        d_copy(s, g, up).wait_recv()
        y2s[s, g, 0] = both(s, g, up, 1).astype(BF16)
        send(y2, y2s.at[s, g, 0], y2r.at[s, g, 0], y_plus)
        d_copy(s, g, down).wait_recv()
        y2s[s, g, 2] = both(s, g, down, 0).astype(BF16)
        send(y2 + 2, y2s.at[s, g, 2], y2r.at[s, g, 2], y_minus)
        d_copy(s, g, keep(s, 0)).wait_recv()

    def reduce_middle(s, g):
        y1, y2, up, down = Y1_ID[s][g], Y2_ID[s][g], keep(s, 1), keep(s, 3)
        wait(y1, y1r.at[s, g, 0])
        y2s[s, g, 1] = (both(s, g, up, 0) + y1r[s, g, 0].astype(F32)).astype(BF16)
        send(y2 + 1, y2s.at[s, g, 1], y2r.at[s, g, 1], y_plus)
        wait(y1 + 1, y1r.at[s, g, 1])
        y2s[s, g, 3] = (both(s, g, down, 1) + y1r[s, g, 1].astype(F32)).astype(BF16)
        send(y2 + 3, y2s.at[s, g, 3], y2r.at[s, g, 3], y_minus)

    def eye(s, h):
        shape = (PART, BLOCK)
        r = lax.broadcasted_iota(jnp.int32, shape, 0) + BLOCK * row_block[s] + HALF * c + PART * s
        k = lax.broadcasted_iota(jnp.int32, shape, 1) + BLOCK * (2 * x + h)
        return (r == k).astype(F32)

    def inverse(sums):
        return lax.rsqrt(sums / TOKENS + epsilon)

    def lane_block(block):
        return pl.ds(pl.multiple_of(block * BLOCK, BLOCK), BLOCK)

    def normalise(s):
        rows = pl.ds(pl.multiple_of(HALF * c + PART * s, PART), PART)
        inv_row = jnp.broadcast_to(inverse(totbuf[keep(s, 0), zl, :, rows]), (PART, PART))
        inv_row = jnp.concatenate([jnp.transpose(inv_row)] * 4, axis=1)
        for g in range(2):
            for k in range(4):
                wait(Y2_ID[s][g] + k, y2r.at[s, g, k])
            h = zh if g == 0 else 1 - zh
            inv_col = inverse(totbuf[(x, 4)[g], zl])
            low = both(s, g, keep(s, 0), 0) + y2r[s, g, 1].astype(F32) + y2r[s, g, 2].astype(F32)
            high = both(s, g, keep(s, 0), 1) + y2r[s, g, 0].astype(F32) + y2r[s, g, 3].astype(F32)
            total = jnp.concatenate([low, high], axis=0)
            damped = total / TOKENS * inv_row * inv_col + damping * eye(s, h)
            value = damped / divisor
            scaled[h, s] = value
            half = value.astype(BF16)
            rowbuf[s, :, lane_block(2 * x + h)] = half
            colbuf[h, keep(s, 0), zh, c, s] = half

    def row_line(s):
        def ref(step, half):
            return rowbuf.at[s, :, lane_block(((x + step) % 4) * 2 + half)]

        return Line(send, wait, ROW_ID[s], ref, x_plus, x_minus)

    def col_plane(k, s, h=None):
        def piece(block, zh_, core, half):
            if h is None:
                r = colbuf.at[:, block, zh_, core, s]
                return r if half is None else r.at[half]
            r = colbuf.at[h, block, zh_, core, s]
            return r if half is None else r.at[halves[half]]

        def ref(step, half, other=0):
            zh_ = 1 - zh if other else zh
            return piece(row_of(s, zh_, (y + step) % 4), zh_, c, half)

        def mirrored(half):
            return piece(0, 0, 1 - c, half)

        return Plane(
            send, wait, COL_ID[k], ref, y_plus, y_minus, zh_mate, sibling, mirrored
        )

    def sq_line(k, h, s=None):
        def ref(step, half):
            if s is None:
                part = pl.ds(PART * half, PART)
            else:
                part = pl.ds(PART * s + PART // 2 * half, PART // 2)
            return sqrow.at[h, part, lane_block((x + step) % 4)]

        return Line(send, wait, SQ_ID[k], ref, x_plus, x_minus)

    rows = [row_line(s) for s in range(2)]
    cols = [col_plane(0, 0), col_plane(1, 1, 0), col_plane(2, 1, 1)]
    sq_rows = [sq_line(0, 0), sq_line(1, 1, 0), sq_line(2, 1, 1)]

    def square(h):
        def step(k, carry):
            lanes = pl.ds(pl.multiple_of(k * HALF, HALF), HALF)
            sq[h, :, lanes] = jnp.dot(
                rowbuf[...].reshape(HALF, D),
                colbuf[h, :, :, :, :, :, lanes].reshape(D, HALF),
                preferred_element_type=F32,
            )
            return carry

        lax.fori_loop(0, 2, step, 0)
        sqrow[h, :, lane_block(x)] = sq[h].astype(BF16)

    def combine(h):
        for s in range(2):
            scaled[h, s] = (
                4.0 * eye(s, h) - 6.0 * scaled[h, s] + 4.0 * sq[h, PART * s : PART * (s + 1)]
            )

    def cube_even():
        for h in range(2):
            def step(k, carry):
                lanes = pl.ds(pl.multiple_of(k * HALF, HALF), HALF)
                sq[h, :, lanes] = jnp.dot(
                    sqrow[0], colbuf[h, :, 0, :, :, :, lanes].reshape(D // 2, HALF),
                    preferred_element_type=F32,
                )
                return carry

            lax.fori_loop(0, 2, step, 0)

    def cube_odd(s):
        part = slice(PART * s, PART * (s + 1))
        for h in range(2):
            def step(k, carry):
                lanes = pl.ds(pl.multiple_of(k * HALF, HALF), HALF)
                value = jnp.dot(
                    sqrow[1, part], colbuf[h, :, 1, :, :, :, lanes].reshape(D // 2, HALF),
                    preferred_element_type=F32,
                )
                value = scaled[h, s, :, lanes] - sq[h, part, lanes] - value
                start = pl.multiple_of(BLOCK * h + k * HALF, HALF)
                obuf[part, pl.ds(start, HALF)] = value.astype(BF16)
                return carry

            lax.fori_loop(0, 2, step, 0)
        for b in range(4 * s, 4 * s + 4):
            me = home & (blk == b)

            @pl.when(me)
            def _():
                out_ref[zl, :, wide_block(x)] = obuf[b * 32 : (b + 1) * 32]

            @pl.when(jnp.logical_not(me))
            def _():
                out_copy(b).start()

    def wide_block(block):
        return pl.ds(pl.multiple_of(block * 2 * BLOCK, 2 * BLOCK), 2 * BLOCK)

    def out_copy(b):
        return remote(
            OUT_ID + b, obuf.at[pl.ds(b * 32, 32)], out_ref.at[zl, :, wide_block(x)],
            (out_tok[b // 4], b), OUT_ID + line_slot,
        )

    def emit():
        for k in range(8):
            @pl.when(jnp.logical_not(home & (line_slot == k)))
            def _():
                wait(OUT_ID + k, out_ref.at[k % 2, :, wide_block(k // 2)])

    def drain(n):
        for copy in sent[:n]:
            copy.wait_send()
        del sent[:n]

    def drain_small():
        def step(j, carry):
            sum_copy(j).wait_send()
            return carry

        lax.fori_loop(1, 16, step, 0)
        for j in range(4):
            total_copy(j).wait_send()

        def step_d(j, carry):
            for s in range(2):
                for g in range(2):
                    d_copy(s, g, j).wait_send()
            return carry

        lax.fori_loop(0, 4, step_d, 0)

    z_first(0)
    lines[0][0].start()
    column_sums()
    sums_start()
    z_first(1)
    z_rest(0)
    z_rest(1)
    lines[0][0].near()
    z_first_take(0)
    lines[0][1].start()
    totals_start()
    lines[0][1].near()
    lines[1][0].start()
    z_first_take(1)
    lines[1][1].start()
    lines[0][0].finish()
    lines[0][1].finish()
    gram(0, 0)
    reduce_start(0, 0)
    lines[1][0].near()
    z_rest_take(0)
    z_rest_take(1)
    gram(0, 1)
    reduce_middle(0, 0)
    reduce_start(0, 1)
    lines[1][1].near()
    reduce_middle(0, 1)
    totals_finish()
    normalise(0)
    cols[0].start()
    rows[0].start()
    lines[1][0].finish()
    lines[1][1].finish()
    gram(1, 0)
    reduce_start(1, 0)
    gram(1, 1)
    cols[0].near()
    reduce_start(1, 1)
    reduce_middle(1, 0)
    cols[0].rest()
    rows[0].near()
    reduce_middle(1, 1)
    cols[0].other()
    normalise(1)
    cols[1].start()
    rows[1].start()
    cols[0].far()
    drain(30)
    cols[1].near()
    cols[2].start()
    cols[1].rest()
    rows[1].near()
    cols[1].other()
    cols[2].near()
    cols[1].far()
    cols[2].rest()
    cols[2].other()
    cols[0].last()
    cols[2].far()
    cols[1].last()
    cols[0].passed()
    rows[0].finish()
    rows[1].finish()
    cols[1].passed()
    square(0)
    sq_rows[0].start()
    combine(0)
    cols[2].last()
    sq_rows[0].near()
    drain_small()
    cols[2].passed()
    square(1)
    sq_rows[1].start()
    sq_rows[2].start()
    sq_rows[0].finish()
    combine(1)
    sq_rows[1].near()
    sq_rows[2].near()
    cube_even()
    drain(80)
    sq_rows[1].finish()
    cube_odd(0)
    sq_rows[2].finish()
    cube_odd(1)
    drain(len(sent))
    emit()
    for b in range(8):
        @pl.when(jnp.logical_not(home & (blk == b)))
        def _():
            out_copy(b).wait_send()


def body(activations, out_grads):
    hbm = pl.BlockSpec(memory_space=pltpu.HBM)
    vmem = pl.BlockSpec(memory_space=pltpu.VMEM)
    part = (PART, BLOCK)
    half_part = (PART // 2, BLOCK)
    scratch = [
        pltpu.VMEM((2, 5, 2, BLOCK, HALF), BF16),
        pltpu.VMEM((2, BLOCK, HALF), BF16),
        pltpu.VMEM((2, 2, 4, 2, *part), BF16),
        pltpu.VMEM((2, 2, 4, *part), BF16),
        pltpu.VMEM((2, 2, 2, *half_part), BF16),
        pltpu.VMEM((2, 2, 2, *half_part), BF16),
        pltpu.VMEM((2, 2, 4, *half_part), BF16),
        pltpu.VMEM((2, 2, 4, *half_part), BF16),
        pltpu.VMEM((2, 2, *part), F32),
        pltpu.VMEM((2, PART, D), BF16),
        pltpu.VMEM((2, 4, 2, 2, 2, *part), BF16),
        pltpu.VMEM((2, HALF, D // 2), BF16),
        pltpu.VMEM((2, HALF, BLOCK), F32),
        pltpu.VMEM((HALF, 2 * BLOCK), BF16),
        pltpu.VMEM((2, 1, BLOCK), F32),
        pltpu.VMEM((16, 2, 1, BLOCK), F32),
        pltpu.VMEM((5, 2, 1, BLOCK), F32),
        pltpu.SemaphoreType.DMA((N_ID,)),
        pltpu.SemaphoreType.DMA((N_ID,)),
        pltpu.SemaphoreType.DMA((8,)),
    ]
    out = pl.pallas_call(
        kernel,
        out_shape=jax.ShapeDtypeStruct((2, 32, D), BF16),
        in_specs=[hbm, hbm],
        out_specs=vmem,
        scratch_shapes=scratch,
        compiler_params=pltpu.CompilerParams(
            collective_id=0, has_side_effects=True, vmem_limit_bytes=60 * 1024 * 1024
        ),
    )(activations, out_grads)
    return out[0].astype(F32), out[1].astype(F32)


def solution(mesh):
    placed = (P("tok", "blk"), P("tok", "blk"))
    return jax.shard_map(
        body,
        mesh=mesh,
        in_specs=placed,
        out_specs=(P(("tok", "blk"), None), P(("tok", "blk"), None)),
        check_vma=False,
    )
```

```python
import jax
import jax.numpy as jnp
from jax import lax
from jax.experimental import pallas as pl
from jax.experimental.pallas import tpu as pltpu
from jax.sharding import PartitionSpec as P

D = 4096
TOKENS = 8192
BLOCK = 512
HALF = 256
PART = 128

damping = 0.3
epsilon = 1e-06
divisor = 2.0

MESH = pl.DeviceIdType.MESH
F32 = jnp.float32
BF16 = jnp.bfloat16


class Ids:
    def __init__(self):
        self.next = 0

    def take(self, n):
        first = self.next
        self.next += n
        return first


IDS = Ids()
Z_ID = IDS.take(6)
X_ID = [[IDS.take(3) for _ in range(2)] for _ in range(2)]
D_ID = [[IDS.take(1) for _ in range(2)] for _ in range(2)]
Y1_ID = [[IDS.take(2) for _ in range(2)] for _ in range(2)]
Y2_ID = [[IDS.take(1) for _ in range(2)] for _ in range(2)]
ROW_ID = [IDS.take(3) for _ in range(2)]
COL_ID = [IDS.take(8) for _ in range(3)]
SQ_ID = [IDS.take(3) for _ in range(3)]
OUT_ID = IDS.take(1)
SUM_ID = IDS.take(1)
TOTAL_ID = IDS.take(1)
N_ID = IDS.next

(TO_X, TO_Z, TO_SIBLING, TO_Y1, TO_Y2, TO_ROWS, TO_PASS, TO_COLS, TO_SQ, TO_OUT, TO_SUM,
 TO_TOTAL, N_TO) = range(13)


class Line:
    arrivals = [(3, 0), (3, 1), (1, 1), (1, 0), (2, 0), (2, 1)]
    number = [0, 2, 1, 2, 2, 2]

    def __init__(self, send, wait, base, kind, ref, plus, minus, late):
        self.send, self.wait, self.base, self.kind, self.ref = send, wait, base, kind, ref
        self.plus, self.minus, self.late = plus, minus, late

    def put(self, k, where, to):
        r = self.ref(*where)
        self.send(self.base + self.number[k], r, r, to, self.kind)

    def arrived(self, k):
        pass

    def take(self, k):
        self.wait(self.base + self.number[k], self.ref(*self.arrivals[k]))
        self.arrived(k)

    def start(self):
        self.put(0, (0, 0), self.plus)
        self.put(2, (0, 1), self.minus)
        self.put(1, (0, 1), self.plus)
        self.put(3, (0, 0), self.minus)

    def near(self):
        self.take(0)
        self.put(4, (3, 0), self.plus)
        self.take(2)
        self.put(5, (1, 1), self.minus)

    def finish(self):
        self.wait(self.base + 2, self.late)


class Plane(Line):
    arrivals = Line.arrivals + [
        (0, None, 1), (3, None, 1), (1, None, 1), (2, 0, 1), (2, 1, 1)
    ]
    number = [0, 2, 1, 2, 3, 4, 5, 6, 6, 6, 6]

    def __init__(self, send, wait, base, ref, plus, minus, late, across, sibling, mirrored):
        super().__init__(send, wait, base, TO_COLS, ref, plus, minus, late)
        self.across, self.sibling, self.mirrored = across, sibling, mirrored

    def arrived(self, k):
        self.pass_on(self.arrivals[k])

    def pass_on(self, where):
        r = self.ref(*where)
        self.send(self.base + 7, r, r, self.sibling, TO_PASS)

    def start(self):
        super().start()
        self.put(6, (0, None, 0), self.across)
        self.pass_on((0, None, 0))

    def other(self):
        self.take(6)
        self.put(7, (0, None, 1), self.plus)
        self.put(8, (0, None, 1), self.minus)

    def rest(self):
        self.wait(self.base + 2, self.ref(3, None))
        self.arrived(1)
        self.arrived(3)

    def far(self):
        self.take(4)
        self.put(9, (2, 0, 0), self.across)
        self.take(5)
        self.put(10, (2, 1, 0), self.across)

    def last(self):
        self.wait(self.base + 6, self.late)
        for k in (7, 8, 9, 10):
            self.arrived(k)

    def passed(self):
        self.wait(self.base + 7, self.mirrored)


def kernel(
    act_ref, grad_ref, out_ref,
    xall, give, gram_part, drecv, y1s, y1r, y2s, y2r, scaled,
    rowbuf, colbuf, sqrow, sq, obuf, csend, crecv, totbuf,
    ssem, rsem, lsem,
):
    tok, blk = lax.axis_index("tok"), lax.axis_index("blk")
    c, y, zl = tok % 2, (tok // 2) % 4, tok // 8
    x, zh = blk // 2, blk % 2

    def tok_of(zl_, y_, c_):
        return zl_ * 8 + y_ * 2 + c_

    def blk_of(x_, zh_):
        return x_ * 2 + zh_

    x_plus = (tok, blk_of((x + 1) % 4, zh))
    x_minus = (tok, blk_of((x + 3) % 4, zh))
    zh_mate = (tok, blk_of(x, 1 - zh))
    y_plus = (tok_of(zl, (y + 1) % 4, c), blk)
    y_minus = (tok_of(zl, (y + 3) % 4, c), blk)
    zl_mate = (tok_of(1 - zl, y, c), blk)
    z_cross = (tok_of(1 - zl, y, c), blk_of(x, 1 - zh))
    sibling = (tok_of(zl, y, 1 - c), blk)

    def place(to):
        return {"tok": to[0], "blk": to[1]}

    def row_of(s, zh_, y_):
        if s == 0:
            return (y_ % 2) * 2 + y_ // 2
        return (y_ // 2) * 2 + (y_ % 2 + y_ // 2 + zh_) % 2

    def line_of(zh_, x_):
        return (
            (x_ % 2) * 2 + x_ // 2,
            (x_ // 2) * 2 + (x_ % 2 + x_ // 2 + zh_) % 2,
        )

    row_block = [2 * row_of(s, zh, y) + zh for s in range(2)]
    out_tok = [2 * row_block[s] + c for s in range(2)]
    my_set = blk // 4
    home = jnp.where(my_set == 0, out_tok[0], out_tok[1]) == tok
    line_slot = 2 * x + zl

    def loads(src, dst, first):
        out = []
        for s in range(2):
            for k in range(2):
                cols = pl.ds(HALF * k + PART * s, PART)
                out.append(
                    pltpu.make_async_copy(
                        src.at[:, cols], dst(s).at[:, pl.ds(PART * k, PART)],
                        lsem.at[first + 2 * s + k],
                    )
                )
        return out

    def own_block(s):
        return xall.at[0, x, s]

    def give_block(s):
        return give.at[s]

    def all_loads(own_ref, give_ref):
        return loads(own_ref, own_block, 0) + loads(give_ref, give_block, 4)

    @pl.when(zl == 0)
    def _():
        for copy in all_loads(act_ref, grad_ref):
            copy.start()

    @pl.when(zl == 1)
    def _():
        for copy in all_loads(grad_ref, act_ref):
            copy.start()

    barrier = pltpu.get_barrier_semaphore()

    def greet(to):
        pl.semaphore_signal(barrier, inc=1, device_id=place(to), device_id_type=MESH)

    def greet_tok(j, carry):
        greet(((tok + j) % 16, blk))
        return carry

    def greet_blk(j, carry):
        greet((tok, (blk + j) % 8))
        return carry

    lax.fori_loop(1, 16, greet_tok, 0)
    lax.fori_loop(1, 8, greet_blk, 0)
    greet(z_cross)

    def greet_source(j, carry):
        zh_ = (tok // 2) % 2
        y_of = line_of(zh_, tok // 4)
        to = (tok_of(j % 2, jnp.where(my_set == 0, y_of[0], y_of[1]), c), blk_of(j // 2, zh_))

        @pl.when(jnp.logical_not((to[0] == tok) & (to[1] == blk)))
        def _():
            greet(to)

        return carry

    lax.fori_loop(0, 8, greet_source, 0)
    for copy in all_loads(act_ref, grad_ref):
        copy.wait()
    pl.semaphore_wait(barrier, 15 + 7 + 1 + 8 - home.astype(jnp.int32))

    def remote(k, src, dst, to, kind):
        return pltpu.make_async_remote_copy(
            src_ref=src, dst_ref=dst, send_sem=ssem.at[kind], recv_sem=rsem.at[k],
            device_id=place(to), device_id_type=MESH,
        )

    def send(k, src, dst, to, kind):
        remote(k, src, dst, to, kind).start()

    def wait(k, dst):
        remote(k, dst, dst, sibling, 0).wait_recv()

    def left(kind, src):
        remote(0, src, src, sibling, kind).wait_send()

    token_half = (pl.ds(0, HALF), pl.ds(HALF, HALF))

    def x_line(s, t):
        def ref(step, half):
            return xall.at[t, (x + step) % 4, s, token_half[half]]

        return Line(
            send, wait, X_ID[s][t], TO_X, ref, x_plus, x_minus, xall.at[t, (x + 2) % 4]
        )

    lines = [[x_line(s, t) for t in range(2)] for s in range(2)]

    def z_first(s):
        send(Z_ID + s, give.at[s], xall.at[1, x, s], zl_mate, TO_Z)

    def z_rest(s):
        send(Z_ID + 2 + s, give.at[s], xall.at[1, 4, s], z_cross, TO_Z)
        send(Z_ID + 4 + s, xall.at[0, x, s], xall.at[0, 4, s], zh_mate, TO_Z)

    def z_first_take(s):
        wait(Z_ID + s, xall.at[1, x, s])

    def z_rest_take(s):
        wait(Z_ID + 2 + s, xall.at[1, 4, s])
        wait(Z_ID + 4 + s, xall.at[0, 4, s])

    def column_sums():
        for which, ref in ((zl, own_block), (1 - zl, give_block)):
            for s in range(2):
                values = ref(s)[...].astype(F32)
                total = jnp.sum(values * values, axis=0, keepdims=True)
                for k in range(2):
                    csend[which, :, HALF * k + PART * s : HALF * k + PART * (s + 1)] = total[
                        :, PART * k : PART * (k + 1)
                    ]

    def sum_copy(j):
        return remote(SUM_ID, csend, crecv.at[j], ((tok + j) % 16, blk), TO_SUM)

    def sums_start():
        def step(j, carry):
            sum_copy(j).start()
            return carry

        lax.fori_loop(1, 16, step, 0)

    total_to = [(tok, blk_of((x + j) % 4, zh)) for j in (1, 2, 3)] + [zh_mate]

    def total_copy(j):
        slot = x if j < 3 else 4
        return remote(TOTAL_ID, totbuf.at[x], totbuf.at[slot], total_to[j], TO_TOTAL)

    def totals_start():
        wait(SUM_ID, crecv.at[pl.ds(1, 15)])
        total = csend[...]
        for j in range(1, 16):
            total = total + crecv[j]
        totbuf[x] = total
        for j in range(4):
            total_copy(j).start()

    def totals_finish():
        wait(TOTAL_ID, totbuf.at[pl.ds(0, 4)])

    def gram(s, g):
        cols = (x, 4)[g]

        def step(i, carry):
            to = (x + 3 + i) % 4
            for s2 in range(2):
                value = None
                for t in range(2):
                    term = lax.dot_general(
                        xall[t, to, s], xall[t, cols, s2],
                        (((0,), (0,)), ((), ())), preferred_element_type=F32,
                    )
                    value = term if value is None else value + term
                value = value.astype(BF16)
                for k in range(2):
                    for k2 in range(2):
                        start = HALF * k2 + PART * s2
                        gram_part[s, g, to, k, :, start : start + PART] = value[
                            PART * k : PART * (k + 1), PART * k2 : PART * (k2 + 1)
                        ]
            d_copy(s, g, to).start()
            return carry

        lax.fori_loop(0, 4, step, 0)

    def d_copy(s, g, to):
        return remote(
            D_ID[s][g], gram_part.at[s, g, to, 1 - c], drecv.at[s, g, to], sibling, TO_SIBLING
        )

    halves = (pl.ds(0, PART // 2), pl.ds(PART // 2, PART // 2))

    def both(s, g, to, half):
        mine = gram_part[s, g, to, c, halves[half]].astype(F32)
        return mine + drecv[s, g, to, halves[half]].astype(F32)

    def keep(s, step):
        return row_of(s, zh, (y + step) % 4)

    def reduce_start(s, g):
        y1, y2, far, up, down = Y1_ID[s][g], Y2_ID[s][g], keep(s, 2), keep(s, 1), keep(s, 3)
        wait(D_ID[s][g], drecv.at[s, g])
        y1s[s, g, 0] = both(s, g, far, 0).astype(BF16)
        send(y1, y1s.at[s, g, 0], y1r.at[s, g, 0], y_plus, TO_Y1)
        y1s[s, g, 1] = both(s, g, far, 1).astype(BF16)
        send(y1 + 1, y1s.at[s, g, 1], y1r.at[s, g, 1], y_minus, TO_Y1)
        y2s[s, g, 0] = both(s, g, up, 1).astype(BF16)
        send(y2, y2s.at[s, g, 0], y2r.at[s, g, 0], y_plus, TO_Y2)
        y2s[s, g, 2] = both(s, g, down, 0).astype(BF16)
        send(y2, y2s.at[s, g, 2], y2r.at[s, g, 2], y_minus, TO_Y2)

    def reduce_middle(s, g):
        y1, y2, up, down = Y1_ID[s][g], Y2_ID[s][g], keep(s, 1), keep(s, 3)
        wait(y1, y1r.at[s, g, 0])
        y2s[s, g, 1] = (both(s, g, up, 0) + y1r[s, g, 0].astype(F32)).astype(BF16)
        send(y2, y2s.at[s, g, 1], y2r.at[s, g, 1], y_plus, TO_Y2)
        wait(y1 + 1, y1r.at[s, g, 1])
        y2s[s, g, 3] = (both(s, g, down, 1) + y1r[s, g, 1].astype(F32)).astype(BF16)
        send(y2, y2s.at[s, g, 3], y2r.at[s, g, 3], y_minus, TO_Y2)

    def eye(s, h):
        shape = (PART, BLOCK)
        r = lax.broadcasted_iota(jnp.int32, shape, 0) + BLOCK * row_block[s] + HALF * c + PART * s
        k = lax.broadcasted_iota(jnp.int32, shape, 1) + BLOCK * (2 * x + h)
        return (r == k).astype(F32)

    def inverse(sums):
        return lax.rsqrt(sums / TOKENS + epsilon)

    def lane_block(block):
        return pl.ds(pl.multiple_of(block * BLOCK, BLOCK), BLOCK)

    def normalise(s):
        rows = pl.ds(pl.multiple_of(HALF * c + PART * s, PART), PART)
        inv_row = jnp.broadcast_to(inverse(totbuf[keep(s, 0), zl, :, rows]), (PART, PART))
        inv_row = jnp.concatenate([jnp.transpose(inv_row)] * 4, axis=1)
        for g in range(2):
            wait(Y2_ID[s][g], y2r.at[s, g])
            h = zh if g == 0 else 1 - zh
            inv_col = inverse(totbuf[(x, 4)[g], zl])
            low = both(s, g, keep(s, 0), 0) + y2r[s, g, 1].astype(F32) + y2r[s, g, 2].astype(F32)
            high = both(s, g, keep(s, 0), 1) + y2r[s, g, 0].astype(F32) + y2r[s, g, 3].astype(F32)
            total = jnp.concatenate([low, high], axis=0)
            damped = total / TOKENS * inv_row * inv_col + damping * eye(s, h)
            value = damped / divisor
            scaled[h, s] = value
            half = value.astype(BF16)
            rowbuf[s, :, lane_block(2 * x + h)] = half
            colbuf[h, keep(s, 0), zh, c, s] = half

    def row_line(s):
        def ref(step, half):
            return rowbuf.at[s, :, lane_block(((x + step) % 4) * 2 + half)]

        late = rowbuf.at[s, :, pl.ds(0, 4 * BLOCK)]
        return Line(send, wait, ROW_ID[s], TO_ROWS, ref, x_plus, x_minus, late)

    def col_plane(k, s, h=None):
        def piece(block, zh_, core, half):
            if h is None:
                r = colbuf.at[:, block, zh_, core, s]
                return r if half is None else r.at[half]
            r = colbuf.at[h, block, zh_, core, s]
            return r if half is None else r.at[halves[half]]

        def ref(step, half, other=0):
            zh_ = 1 - zh if other else zh
            return piece(row_of(s, zh_, (y + step) % 4), zh_, c, half)

        if h is None:
            late, mirrored = colbuf.at[:, pl.ds(0, 3), 0, c, s], colbuf.at[:, :, :, 1 - c, s]
        else:
            late, mirrored = colbuf.at[h, pl.ds(0, 3), 0, c, s], colbuf.at[h, :, :, 1 - c, s]
        return Plane(
            send, wait, COL_ID[k], ref, y_plus, y_minus, late, zh_mate, sibling, mirrored
        )

    def sq_line(k, h, s=None):
        def ref(step, half):
            if s is None:
                part = pl.ds(PART * half, PART)
            else:
                part = pl.ds(PART * s + PART // 2 * half, PART // 2)
            return sqrow.at[h, part, lane_block((x + step) % 4)]

        late = sqrow.at[h, pl.ds(PART * (s or 0), PART if s is None else PART // 2)]
        return Line(send, wait, SQ_ID[k], TO_SQ, ref, x_plus, x_minus, late)

    rows = [row_line(s) for s in range(2)]
    cols = [col_plane(0, 0), col_plane(1, 1, 0), col_plane(2, 1, 1)]
    sq_rows = [sq_line(0, 0), sq_line(1, 1, 0), sq_line(2, 1, 1)]

    def square(h):
        def step(k, carry):
            lanes = pl.ds(pl.multiple_of(k * HALF, HALF), HALF)
            sq[h, :, lanes] = jnp.dot(
                rowbuf[...].reshape(HALF, D),
                colbuf[h, :, :, :, :, :, lanes].reshape(D, HALF),
                preferred_element_type=F32,
            )
            return carry

        lax.fori_loop(0, 2, step, 0)
        sqrow[h, :, lane_block(x)] = sq[h].astype(BF16)

    def combine(h):
        for s in range(2):
            scaled[h, s] = (
                4.0 * eye(s, h) - 6.0 * scaled[h, s] + 4.0 * sq[h, PART * s : PART * (s + 1)]
            )

    def cube_even():
        for h in range(2):
            def step(k, carry):
                lanes = pl.ds(pl.multiple_of(k * HALF, HALF), HALF)
                sq[h, :, lanes] = jnp.dot(
                    sqrow[0], colbuf[h, :, 0, :, :, :, lanes].reshape(D // 2, HALF),
                    preferred_element_type=F32,
                )
                return carry

            lax.fori_loop(0, 2, step, 0)

    def cube_odd(s):
        part = slice(PART * s, PART * (s + 1))
        for h in range(2):
            def step(k, carry):
                lanes = pl.ds(pl.multiple_of(k * HALF, HALF), HALF)
                value = jnp.dot(
                    sqrow[1, part], colbuf[h, :, 1, :, :, :, lanes].reshape(D // 2, HALF),
                    preferred_element_type=F32,
                )
                value = scaled[h, s, :, lanes] - sq[h, part, lanes] - value
                start = pl.multiple_of(BLOCK * h + k * HALF, HALF)
                obuf[part, pl.ds(start, HALF)] = value.astype(BF16)
                return carry

            lax.fori_loop(0, 2, step, 0)
        for b in range(4 * s, 4 * s + 4):
            me = home & (blk == b)

            @pl.when(me)
            def _():
                out_ref[zl, :, wide_block(x)] = obuf[b * 32 : (b + 1) * 32]

            @pl.when(jnp.logical_not(me))
            def _():
                out_copy(b).start()

    def wide_block(block):
        return pl.ds(pl.multiple_of(block * 2 * BLOCK, 2 * BLOCK), 2 * BLOCK)

    def out_copy(b):
        return remote(
            OUT_ID, obuf.at[pl.ds(b * 32, 32)], out_ref.at[zl, :, wide_block(x)],
            (out_tok[b // 4], b), TO_OUT,
        )

    def emit():
        @pl.when(home)
        def _():
            wait(OUT_ID, out_ref.at[:, :, pl.ds(0, 7 * BLOCK)])
            left(TO_OUT, obuf.at[pl.ds(0, 7 * 32)])

        @pl.when(jnp.logical_not(home))
        def _():
            wait(OUT_ID, out_ref)
            left(TO_OUT, obuf)

    def all_left():
        left(TO_X, xall.at[:, pl.ds(0, 3)])
        left(TO_Z, xall.at[0, pl.ds(0, 3)])
        left(TO_SIBLING, gram_part.at[0])
        left(TO_Y1, y1s)
        left(TO_Y2, y2s)
        left(TO_ROWS, rowbuf.at[:, pl.ds(0, 96)])
        left(TO_PASS, colbuf.at[:, :, :, 0])
        left(TO_COLS, colbuf.at[:, :, :, 0, :, pl.ds(0, 112)])
        left(TO_SQ, sqrow.at[:, pl.ds(0, 192)])
        left(TO_SUM, crecv.at[pl.ds(1, 15)])
        left(TO_TOTAL, totbuf.at[pl.ds(0, 4)])

    z_first(0)
    lines[0][0].start()
    column_sums()
    sums_start()
    z_first(1)
    z_rest(0)
    z_rest(1)
    lines[0][0].near()
    z_first_take(0)
    lines[0][1].start()
    totals_start()
    lines[0][1].near()
    lines[1][0].start()
    z_first_take(1)
    lines[1][1].start()
    lines[0][0].finish()
    lines[0][1].finish()
    gram(0, 0)
    reduce_start(0, 0)
    lines[1][0].near()
    reduce_middle(0, 0)
    z_rest_take(0)
    z_rest_take(1)
    gram(0, 1)
    reduce_start(0, 1)
    lines[1][1].near()
    reduce_middle(0, 1)
    totals_finish()
    normalise(0)
    cols[0].start()
    rows[0].start()
    lines[1][0].finish()
    lines[1][1].finish()
    gram(1, 0)
    gram(1, 1)
    reduce_start(1, 0)
    cols[0].near()
    reduce_start(1, 1)
    reduce_middle(1, 0)
    cols[0].rest()
    rows[0].near()
    reduce_middle(1, 1)
    cols[0].other()
    normalise(1)
    cols[1].start()
    rows[1].start()
    cols[0].far()
    cols[1].near()
    cols[2].start()
    cols[1].rest()
    rows[1].near()
    cols[1].other()
    cols[2].near()
    cols[1].far()
    cols[2].rest()
    cols[2].other()
    cols[0].last()
    cols[1].last()
    cols[2].far()
    rows[0].finish()
    rows[1].finish()
    cols[0].passed()
    cols[1].passed()
    square(0)
    sq_rows[0].start()
    combine(0)
    cols[2].last()
    sq_rows[0].near()
    cols[2].passed()
    square(1)
    sq_rows[1].start()
    sq_rows[2].start()
    sq_rows[0].finish()
    combine(1)
    sq_rows[1].near()
    sq_rows[2].near()
    cube_even()
    sq_rows[1].finish()
    cube_odd(0)
    sq_rows[2].finish()
    cube_odd(1)
    all_left()
    emit()


def body(activations, out_grads):
    hbm = pl.BlockSpec(memory_space=pltpu.HBM)
    vmem = pl.BlockSpec(memory_space=pltpu.VMEM)
    part = (PART, BLOCK)
    half_part = (PART // 2, BLOCK)
    scratch = [
        pltpu.VMEM((2, 5, 2, BLOCK, HALF), BF16),
        pltpu.VMEM((2, BLOCK, HALF), BF16),
        pltpu.VMEM((2, 2, 4, 2, *part), BF16),
        pltpu.VMEM((2, 2, 4, *part), BF16),
        pltpu.VMEM((2, 2, 2, *half_part), BF16),
        pltpu.VMEM((2, 2, 2, *half_part), BF16),
        pltpu.VMEM((2, 2, 4, *half_part), BF16),
        pltpu.VMEM((2, 2, 4, *half_part), BF16),
        pltpu.VMEM((2, 2, *part), F32),
        pltpu.VMEM((2, PART, D), BF16),
        pltpu.VMEM((2, 4, 2, 2, 2, *part), BF16),
        pltpu.VMEM((2, HALF, D // 2), BF16),
        pltpu.VMEM((2, HALF, BLOCK), F32),
        pltpu.VMEM((HALF, 2 * BLOCK), BF16),
        pltpu.VMEM((2, 1, BLOCK), F32),
        pltpu.VMEM((16, 2, 1, BLOCK), F32),
        pltpu.VMEM((5, 2, 1, BLOCK), F32),
        pltpu.SemaphoreType.DMA((N_TO,)),
        pltpu.SemaphoreType.DMA((N_ID,)),
        pltpu.SemaphoreType.DMA((8,)),
    ]
    out = pl.pallas_call(
        kernel,
        out_shape=jax.ShapeDtypeStruct((2, 32, D), BF16),
        in_specs=[hbm, hbm],
        out_specs=vmem,
        scratch_shapes=scratch,
        compiler_params=pltpu.CompilerParams(
            collective_id=0, has_side_effects=True, vmem_limit_bytes=60 * 1024 * 1024
        ),
    )(activations, out_grads)
    return out[0].astype(F32), out[1].astype(F32)


def solution(mesh):
    placed = (P("tok", "blk"), P("tok", "blk"))
    return jax.shard_map(
        body,
        mesh=mesh,
        in_specs=placed,
        out_specs=(P(("tok", "blk"), None), P(("tok", "blk"), None)),
        check_vma=False,
    )
```

```python
import jax
import jax.numpy as jnp
from jax import lax
from jax.experimental import pallas as pl
from jax.experimental.pallas import tpu as pltpu
from jax.sharding import PartitionSpec as P

D = 4096
TOKENS = 8192
BLOCK = 512
HALF = 256
PART = 128

damping = 0.3
epsilon = 1e-06
divisor = 2.0

MESH = pl.DeviceIdType.MESH
F32 = jnp.float32
BF16 = jnp.bfloat16


class Ids:
    def __init__(self):
        self.next = 0

    def take(self, n):
        first = self.next
        self.next += n
        return first


IDS = Ids()
Z_ID = IDS.take(6)
X_ID = [[IDS.take(3) for _ in range(2)] for _ in range(2)]
D_ID = [[IDS.take(1) for _ in range(2)] for _ in range(2)]
Y1_ID = [[IDS.take(2) for _ in range(2)] for _ in range(2)]
Y2_ID = [[IDS.take(1) for _ in range(2)] for _ in range(2)]
ROW_ID = [IDS.take(7) for _ in range(2)]
LOW_ID = [IDS.take(1) for _ in range(2)]
COL_ID = [[IDS.take(4) for _ in range(2)] for _ in range(2)]
SQ_ID = [IDS.take(4) for _ in range(2)]
OUT_ID = IDS.take(1)
SUM_ID = IDS.take(1)
TOTAL_ID = IDS.take(1)
N_ID = IDS.next

(TO_X, TO_Z, TO_SIBLING, TO_Y1, TO_Y2, TO_ROWS, TO_LOW, TO_PASS, TO_COLS, TO_SQ, TO_SQ_PASS,
 TO_OUT, TO_SUM, TO_TOTAL, N_TO) = range(15)


class Line:
    arrivals = [(3, 0), (3, 1), (1, 1), (1, 0), (2, 0), (2, 1)]
    number = [0, 2, 1, 2, 2, 2]

    def __init__(self, send, wait, base, kind, ref, plus, minus, late):
        self.send, self.wait, self.base, self.kind, self.ref = send, wait, base, kind, ref
        self.plus, self.minus, self.late = plus, minus, late

    def put(self, k, where, to):
        r = self.ref(*where)
        self.send(self.base + self.number[k], r, r, to, self.kind)

    def arrived(self, k):
        pass

    def take(self, k):
        self.wait(self.base + self.number[k], self.ref(*self.arrivals[k]))
        self.arrived(k)

    def start(self):
        self.put(0, (0, 0), self.plus)
        self.put(2, (0, 1), self.minus)
        self.put(1, (0, 1), self.plus)
        self.put(3, (0, 0), self.minus)

    def near(self):
        self.take(0)
        self.put(4, (3, 0), self.plus)
        self.take(2)
        self.put(5, (1, 1), self.minus)

    def finish(self):
        self.wait(self.base + 2, self.late)


class Passed(Line):
    def __init__(self, send, wait, base, kind, ref, plus, minus, late, sibling, pass_kind, mirrored):
        super().__init__(send, wait, base, kind, ref, plus, minus, late)
        self.sibling, self.pass_kind, self.mirrored = sibling, pass_kind, mirrored

    def pass_on(self, where):
        r = self.ref(*where)
        self.send(self.base + 3, r, r, self.sibling, self.pass_kind)

    def arrived(self, k):
        self.pass_on(self.arrivals[k])

    def start(self):
        super().start()
        self.pass_on((0, 0))
        self.pass_on((0, 1))

    def finish(self):
        super().finish()
        for k in (1, 3, 4, 5):
            self.arrived(k)

    def passed(self):
        self.wait(self.base + 3, self.mirrored)


class Plane(Line):
    arrivals = Line.arrivals + [
        (0, None, 1), (3, None, 1), (1, None, 1), (2, 0, 1), (2, 1, 1)
    ]
    number = [0, 2, 1, 2, 3, 4, 5, 6, 6, 6, 6]

    def __init__(self, send, wait, base, kind, ref, plus, minus, late, across):
        super().__init__(send, wait, base, kind, ref, plus, minus, late)
        self.across = across

    def start(self):
        self.put(6, (0, None, 0), self.across)
        super().start()

    def other(self):
        self.take(6)
        self.put(7, (0, None, 1), self.plus)
        self.put(8, (0, None, 1), self.minus)

    def far(self):
        self.wait(self.base + 2, self.ref(3, None))
        self.take(4)
        self.put(9, (2, 0, 0), self.across)
        self.take(5)
        self.put(10, (2, 1, 0), self.across)

    def last(self):
        self.wait(self.base + 6, self.late)


def kernel(
    act_ref, grad_ref, out_ref,
    xall, give, gram_part, drecv, y1s, y1r, y2s, y2r, scaled,
    rowbuf, colbuf, sqcol, sq, low_out, low_in, obuf, csend, crecv, totbuf,
    ssem, rsem, lsem,
):
    tok, blk = lax.axis_index("tok"), lax.axis_index("blk")
    c, y, zl = tok % 2, (tok // 2) % 4, tok // 8
    x, zh = blk // 2, blk % 2

    def tok_of(zl_, y_, c_):
        return zl_ * 8 + y_ * 2 + c_

    def blk_of(x_, zh_):
        return x_ * 2 + zh_

    x_plus = (tok, blk_of((x + 1) % 4, zh))
    x_minus = (tok, blk_of((x + 3) % 4, zh))
    zh_mate = (tok, blk_of(x, 1 - zh))
    y_plus = (tok_of(zl, (y + 1) % 4, c), blk)
    y_minus = (tok_of(zl, (y + 3) % 4, c), blk)
    zl_mate = (tok_of(1 - zl, y, c), blk)
    z_cross = (tok_of(1 - zl, y, c), blk_of(x, 1 - zh))
    sibling = (tok_of(zl, y, 1 - c), blk)

    def place(to):
        return {"tok": to[0], "blk": to[1]}

    def row_of(s, y_):
        return ((y_ + s) % 2) * 2 + y_ // 2

    def keep(s, step):
        return row_of(s, (y + step) % 4)

    zh_of = (zh, 1 - zh)

    def out_tok(e, s):
        return 2 * (2 * keep(s, 0) + zh_of[e]) + c

    source_y = ((tok // 4) % 2) * 2 + (tok // 8 + blk // 4) % 2
    home = source_y == y

    def loads(src, dst, first):
        out = []
        for s in range(2):
            for k in range(2):
                cols = pl.ds(HALF * k + PART * s, PART)
                out.append(
                    pltpu.make_async_copy(
                        src.at[:, cols], dst(s).at[:, pl.ds(PART * k, PART)],
                        lsem.at[first + 2 * s + k],
                    )
                )
        return out

    def own_block(s):
        return xall.at[0, x, s]

    def give_block(s):
        return give.at[s]

    def all_loads(own_ref, give_ref):
        return loads(own_ref, own_block, 0) + loads(give_ref, give_block, 4)

    @pl.when(zl == 0)
    def _():
        for copy in all_loads(act_ref, grad_ref):
            copy.start()

    @pl.when(zl == 1)
    def _():
        for copy in all_loads(grad_ref, act_ref):
            copy.start()

    barrier = pltpu.get_barrier_semaphore()

    def greet(to):
        pl.semaphore_signal(barrier, inc=1, device_id=place(to), device_id_type=MESH)

    def greet_tok(j, carry):
        greet(((tok + j) % 16, blk))
        return carry

    def greet_blk(j, carry):
        greet((tok, (blk + j) % 8))
        return carry

    lax.fori_loop(1, 16, greet_tok, 0)
    lax.fori_loop(1, 8, greet_blk, 0)
    greet(z_cross)

    def greet_source(j, carry):
        to = (tok_of(j % 2, source_y, c), j // 2)

        @pl.when(jnp.logical_not((to[0] == tok) & (to[1] == blk)))
        def _():
            greet(to)

        return carry

    lax.fori_loop(0, 16, greet_source, 0)
    for copy in all_loads(act_ref, grad_ref):
        copy.wait()
    pl.semaphore_wait(barrier, 15 + 7 + 1 + 16 - home.astype(jnp.int32))

    def remote(k, src, dst, to, kind):
        return pltpu.make_async_remote_copy(
            src_ref=src, dst_ref=dst, send_sem=ssem.at[kind], recv_sem=rsem.at[k],
            device_id=place(to), device_id_type=MESH,
        )

    def send(k, src, dst, to, kind):
        remote(k, src, dst, to, kind).start()

    def wait(k, dst):
        remote(k, dst, dst, sibling, 0).wait_recv()

    def left(kind, src):
        remote(0, src, src, sibling, kind).wait_send()

    token_half = (pl.ds(0, HALF), pl.ds(HALF, HALF))

    def x_line(s, t):
        def ref(step, half):
            return xall.at[t, (x + step) % 4, s, token_half[half]]

        return Line(
            send, wait, X_ID[s][t], TO_X, ref, x_plus, x_minus, xall.at[t, (x + 2) % 4]
        )

    lines = [[x_line(s, t) for t in range(2)] for s in range(2)]

    def z_first(s):
        send(Z_ID + s, give.at[s], xall.at[1, x, s], zl_mate, TO_Z)

    def z_rest(s):
        send(Z_ID + 2 + s, give.at[s], xall.at[1, 4, s], z_cross, TO_Z)
        send(Z_ID + 4 + s, xall.at[0, x, s], xall.at[0, 4, s], zh_mate, TO_Z)

    def z_first_take(s):
        wait(Z_ID + s, xall.at[1, x, s])

    def z_rest_take(s):
        wait(Z_ID + 2 + s, xall.at[1, 4, s])
        wait(Z_ID + 4 + s, xall.at[0, 4, s])

    def column_sums():
        for which, ref in ((zl, own_block), (1 - zl, give_block)):
            for s in range(2):
                values = ref(s)[...].astype(F32)
                total = jnp.sum(values * values, axis=0, keepdims=True)
                for k in range(2):
                    csend[which, :, HALF * k + PART * s : HALF * k + PART * (s + 1)] = total[
                        :, PART * k : PART * (k + 1)
                    ]

    def sum_copy(j):
        return remote(SUM_ID, csend, crecv.at[j], ((tok + j) % 16, blk), TO_SUM)

    def sums_start():
        def step(j, carry):
            sum_copy(j).start()
            return carry

        lax.fori_loop(1, 16, step, 0)

    total_to = [(tok, blk_of((x + j) % 4, zh)) for j in (1, 2, 3)] + [zh_mate]

    def total_copy(j):
        slot = x if j < 3 else 4
        return remote(TOTAL_ID, totbuf.at[x], totbuf.at[slot], total_to[j], TO_TOTAL)

    def totals_start():
        wait(SUM_ID, crecv.at[pl.ds(1, 15)])
        total = csend[...]
        for j in range(1, 16):
            total = total + crecv[j]
        totbuf[x] = total
        for j in range(4):
            total_copy(j).start()

    def totals_finish():
        wait(TOTAL_ID, totbuf.at[pl.ds(0, 4)])

    def gram(s, g):
        cols = (x, 4)[g]

        def step(i, carry):
            to = (x + 3 + i) % 4
            for s2 in range(2):
                value = None
                for t in range(2):
                    term = lax.dot_general(
                        xall[t, to, s], xall[t, cols, s2],
                        (((0,), (0,)), ((), ())), preferred_element_type=F32,
                    )
                    value = term if value is None else value + term
                value = value.astype(BF16)
                for k in range(2):
                    for k2 in range(2):
                        start = HALF * k2 + PART * s2
                        gram_part[s, g, to, k, :, start : start + PART] = value[
                            PART * k : PART * (k + 1), PART * k2 : PART * (k2 + 1)
                        ]
            d_copy(s, g, to).start()
            return carry

        lax.fori_loop(0, 4, step, 0)

    def d_copy(s, g, to):
        return remote(
            D_ID[s][g], gram_part.at[s, g, to, 1 - c], drecv.at[s, g, to], sibling, TO_SIBLING
        )

    halves = (pl.ds(0, PART // 2), pl.ds(PART // 2, PART // 2))

    def both(s, g, to, half):
        mine = gram_part[s, g, to, c, halves[half]].astype(F32)
        return mine + drecv[s, g, to, halves[half]].astype(F32)

    def reduce_start(s, g):
        y1, y2, far, up, down = Y1_ID[s][g], Y2_ID[s][g], keep(s, 2), keep(s, 1), keep(s, 3)
        wait(D_ID[s][g], drecv.at[s, g])
        y1s[s, g, 0] = both(s, g, far, 0).astype(BF16)
        send(y1, y1s.at[s, g, 0], y1r.at[s, g, 0], y_plus, TO_Y1)
        y1s[s, g, 1] = both(s, g, far, 1).astype(BF16)
        send(y1 + 1, y1s.at[s, g, 1], y1r.at[s, g, 1], y_minus, TO_Y1)
        y2s[s, g, 0] = both(s, g, up, 1).astype(BF16)
        send(y2, y2s.at[s, g, 0], y2r.at[s, g, 0], y_plus, TO_Y2)
        y2s[s, g, 2] = both(s, g, down, 0).astype(BF16)
        send(y2, y2s.at[s, g, 2], y2r.at[s, g, 2], y_minus, TO_Y2)

    def reduce_middle(s, g):
        y1, y2, up, down = Y1_ID[s][g], Y2_ID[s][g], keep(s, 1), keep(s, 3)
        wait(y1, y1r.at[s, g, 0])
        y2s[s, g, 1] = (both(s, g, up, 0) + y1r[s, g, 0].astype(F32)).astype(BF16)
        send(y2, y2s.at[s, g, 1], y2r.at[s, g, 1], y_plus, TO_Y2)
        wait(y1 + 1, y1r.at[s, g, 1])
        y2s[s, g, 3] = (both(s, g, down, 1) + y1r[s, g, 1].astype(F32)).astype(BF16)
        send(y2, y2s.at[s, g, 3], y2r.at[s, g, 3], y_minus, TO_Y2)

    def eye(s, zh_, h):
        shape = (PART, BLOCK)
        r = lax.broadcasted_iota(jnp.int32, shape, 0) + HALF * c + PART * s
        k = lax.broadcasted_iota(jnp.int32, shape, 1)
        return (r + BLOCK * (2 * keep(s, 0) + zh_) == k + BLOCK * (2 * x + h)).astype(F32)

    def inverse(sums):
        return lax.rsqrt(sums / TOKENS + epsilon)

    def lane_block(block):
        return pl.ds(pl.multiple_of(block * BLOCK, BLOCK), BLOCK)

    def normalise(s):
        rows = pl.ds(pl.multiple_of(HALF * c + PART * s, PART), PART)
        inv_row = jnp.broadcast_to(inverse(totbuf[keep(s, 0), zl, :, rows]), (PART, PART))
        inv_row = jnp.concatenate([jnp.transpose(inv_row)] * 4, axis=1)
        for g in range(2):
            wait(Y2_ID[s][g], y2r.at[s, g])
            inv_col = inverse(totbuf[(x, 4)[g], zl])
            low = both(s, g, keep(s, 0), 0) + y2r[s, g, 1].astype(F32) + y2r[s, g, 2].astype(F32)
            high = both(s, g, keep(s, 0), 1) + y2r[s, g, 0].astype(F32) + y2r[s, g, 3].astype(F32)
            total = jnp.concatenate([low, high], axis=0)
            damped = total / TOKENS * inv_row * inv_col + damping * eye(s, zh, zh_of[g])
            value = damped / divisor
            half = value.astype(BF16)
            rowbuf[zh, s, zh_of[g], :, lane_block(x)] = half
            if g == 0:
                scaled[0, s] = value
                colbuf[keep(s, 0), zh, c, s] = half
                cols[s][0].start()
            else:
                low_out[s] = (value - half.astype(F32)).astype(BF16)
        rows_of[s].start()
        send(LOW_ID[s], low_out.at[s], low_in.at[s], zh_mate, TO_LOW)

    def partner(s):
        half = rowbuf[1 - zh, s, zh, :, lane_block(x)]
        colbuf[keep(s, 0), 1 - zh, c, s] = half
        cols[s][1].start()

    def partner_low(s):
        wait(LOW_ID[s], low_in.at[s])
        half = rowbuf[1 - zh, s, zh, :, lane_block(x)].astype(F32)
        scaled[1, s] = half + low_in[s].astype(F32)

    def row_plane(s):
        def ref(step, half, other=0):
            lanes = lane_block((x + step) % 4)
            r = rowbuf.at[zh_of[other], s]
            return r.at[:, :, lanes] if half is None else r.at[half, :, lanes]

        late = rowbuf.at[1 - zh, s, :, :, pl.ds(0, 3 * BLOCK)]
        return Plane(send, wait, ROW_ID[s], TO_ROWS, ref, x_plus, x_minus, late, zh_mate)

    def col_line(s, e):
        def ref(step, half):
            return colbuf.at[keep(s, step), zh_of[e], c, s, halves[half]]

        late = colbuf.at[pl.ds(0, 2), zh_of[e], c, s]
        return Passed(
            send, wait, COL_ID[s][e], TO_COLS, ref, y_plus, y_minus, late, sibling, TO_PASS,
            colbuf.at[:, zh_of[e], 1 - c, s],
        )

    def sq_line(e):
        def ref(step, half):
            return sqcol.at[keep(half, step), zh_of[e], c, half]

        late = sqcol.at[pl.ds(0, 2), zh_of[e], c]
        return Passed(
            send, wait, SQ_ID[e], TO_SQ, ref, y_plus, y_minus, late, sibling, TO_SQ_PASS,
            sqcol.at[:, zh_of[e], 1 - c],
        )

    rows_of = [row_plane(s) for s in range(2)]
    cols = [[col_line(s, e) for e in range(2)] for s in range(2)]
    sq_cols = [sq_line(e) for e in range(2)]

    def dot(e, p, right, lanes):
        return jnp.dot(
            rowbuf[zh_of[e], :, p].reshape(HALF, D // 2),
            right[:, p, :, :, :, lanes].reshape(D // 2, HALF),
            preferred_element_type=F32,
        )

    def over_lanes(body):
        def step(k, carry):
            body(pl.ds(pl.multiple_of(k * HALF, HALF), HALF))
            return carry

        lax.fori_loop(0, 2, step, 0)

    def square(e):
        def some(lanes):
            sq[e, :, lanes] = dot(e, 0, colbuf, lanes) + dot(e, 1, colbuf, lanes)

        over_lanes(some)
        for s in range(2):
            sqcol[keep(s, 0), zh_of[e], c, s] = sq[e, PART * s : PART * (s + 1)].astype(BF16)
        sq_cols[e].start()

    def combine(e):
        for s in range(2):
            scaled[e, s] = (
                4.0 * eye(s, zh_of[e], zh) - 6.0 * scaled[e, s]
                + 4.0 * sq[e, PART * s : PART * (s + 1)]
            )

    def cube_first():
        for e in range(2):
            def some(lanes):
                sq[e, :, lanes] = dot(e, zh, sqcol, lanes)

            over_lanes(some)

    def cube_second(e):
        def some(lanes):
            value = scaled[e, :, :, lanes].reshape(HALF, HALF) - sq[e, :, lanes]
            obuf[e, :, lanes] = (value - dot(e, 1 - zh, sqcol, lanes)).astype(BF16)

        over_lanes(some)
        for b in range(8):
            me = (out_tok(e, b // 4) == tok) & (blk == b)

            @pl.when(me)
            def _():
                out_ref[zl, :, lane_block(2 * x + zh)] = obuf[e, b * 32 : (b + 1) * 32]

            @pl.when(jnp.logical_not(me))
            def _():
                out_copy(e, b).start()

    def out_copy(e, b):
        return remote(
            OUT_ID, obuf.at[e, pl.ds(b * 32, 32)], out_ref.at[zl, :, lane_block(2 * x + zh)],
            (out_tok(e, b // 4), b), TO_OUT,
        )

    def emit():
        @pl.when(home)
        def _():
            wait(OUT_ID, out_ref.at[:, :, pl.ds(0, 15 * HALF)])
            left(TO_OUT, obuf.at[:, pl.ds(0, 15 * 16)])

        @pl.when(jnp.logical_not(home))
        def _():
            wait(OUT_ID, out_ref)
            left(TO_OUT, obuf)

    def all_left():
        left(TO_X, xall.at[:, pl.ds(0, 3)])
        left(TO_Z, xall.at[0, pl.ds(0, 3)])
        left(TO_SIBLING, gram_part.at[0])
        left(TO_Y1, y1s)
        left(TO_Y2, y2s)
        left(TO_ROWS, rowbuf.at[:, :, :, pl.ds(0, 112)])
        left(TO_LOW, low_out)
        left(TO_PASS, colbuf.at[pl.ds(0, 2)])
        left(TO_COLS, colbuf.at[pl.ds(0, 3), 0])
        left(TO_SQ, sqcol.at[pl.ds(0, 3), 0])
        left(TO_SQ_PASS, sqcol.at[pl.ds(0, 2)])
        left(TO_SUM, crecv.at[pl.ds(1, 15)])
        left(TO_TOTAL, totbuf.at[pl.ds(0, 4)])

    z_first(0)
    lines[0][0].start()
    column_sums()
    sums_start()
    z_first(1)
    z_rest(0)
    z_rest(1)
    lines[0][0].near()
    z_first_take(0)
    lines[0][1].start()
    totals_start()
    lines[0][1].near()
    lines[1][0].start()
    z_first_take(1)
    lines[1][1].start()
    lines[0][0].finish()
    lines[0][1].finish()
    gram(0, 0)
    reduce_start(0, 0)
    lines[1][0].near()
    z_rest_take(0)
    z_rest_take(1)
    gram(0, 1)
    reduce_middle(0, 0)
    reduce_start(0, 1)
    lines[1][1].near()
    reduce_middle(0, 1)
    totals_finish()
    normalise(0)
    lines[1][0].finish()
    lines[1][1].finish()
    gram(1, 0)
    gram(1, 1)
    reduce_start(1, 0)
    cols[0][0].near()
    rows_of[0].near()
    reduce_start(1, 1)
    reduce_middle(1, 0)
    rows_of[0].other()
    partner(0)
    reduce_middle(1, 1)
    cols[0][0].finish()
    rows_of[0].far()
    cols[0][1].near()
    normalise(1)
    rows_of[1].near()
    cols[1][0].near()
    cols[0][1].finish()
    rows_of[1].other()
    partner(1)
    cols[1][0].finish()
    cols[1][1].near()
    rows_of[1].far()
    cols[1][1].finish()
    for s in range(2):
        for e in range(2):
            cols[s][e].passed()
    square(0)
    combine(0)
    sq_cols[0].near()
    rows_of[0].last()
    rows_of[1].last()
    square(1)
    sq_cols[0].finish()
    partner_low(0)
    partner_low(1)
    combine(1)
    sq_cols[1].near()
    sq_cols[0].passed()
    cube_first()
    sq_cols[1].finish()
    sq_cols[1].passed()
    cube_second(0)
    cube_second(1)
    all_left()
    emit()


def body(activations, out_grads):
    hbm = pl.BlockSpec(memory_space=pltpu.HBM)
    vmem = pl.BlockSpec(memory_space=pltpu.VMEM)
    part = (PART, BLOCK)
    half_part = (PART // 2, BLOCK)
    scratch = [
        pltpu.VMEM((2, 5, 2, BLOCK, HALF), BF16),
        pltpu.VMEM((2, BLOCK, HALF), BF16),
        pltpu.VMEM((2, 2, 4, 2, *part), BF16),
        pltpu.VMEM((2, 2, 4, *part), BF16),
        pltpu.VMEM((2, 2, 2, *half_part), BF16),
        pltpu.VMEM((2, 2, 2, *half_part), BF16),
        pltpu.VMEM((2, 2, 4, *half_part), BF16),
        pltpu.VMEM((2, 2, 4, *half_part), BF16),
        pltpu.VMEM((2, 2, *part), F32),
        pltpu.VMEM((2, 2, 2, PART, D // 2), BF16),
        pltpu.VMEM((4, 2, 2, 2, *part), BF16),
        pltpu.VMEM((4, 2, 2, 2, *part), BF16),
        pltpu.VMEM((2, HALF, BLOCK), F32),
        pltpu.VMEM((2, *part), BF16),
        pltpu.VMEM((2, *part), BF16),
        pltpu.VMEM((2, HALF, BLOCK), BF16),
        pltpu.VMEM((2, 1, BLOCK), F32),
        pltpu.VMEM((16, 2, 1, BLOCK), F32),
        pltpu.VMEM((5, 2, 1, BLOCK), F32),
        pltpu.SemaphoreType.DMA((N_TO,)),
        pltpu.SemaphoreType.DMA((N_ID,)),
        pltpu.SemaphoreType.DMA((8,)),
    ]
    out = pl.pallas_call(
        kernel,
        out_shape=jax.ShapeDtypeStruct((2, 32, D), BF16),
        in_specs=[hbm, hbm],
        out_specs=vmem,
        scratch_shapes=scratch,
        compiler_params=pltpu.CompilerParams(
            collective_id=0, has_side_effects=True, vmem_limit_bytes=60 * 1024 * 1024
        ),
    )(activations, out_grads)
    return out[0].astype(F32), out[1].astype(F32)


def solution(mesh):
    placed = (P("tok", "blk"), P("tok", "blk"))
    return jax.shard_map(
        body,
        mesh=mesh,
        in_specs=placed,
        out_specs=(P(("tok", "blk"), None), P(("tok", "blk"), None)),
        check_vma=False,
    )
```

```python
import jax
import jax.numpy as jnp
from jax import lax
from jax.experimental import pallas as pl
from jax.experimental.pallas import tpu as pltpu
from jax.sharding import PartitionSpec as P

D = 4096
TOKENS = 8192
BLOCK = 512
HALF = 256
PART = 128

damping = 0.3
epsilon = 1e-06
divisor = 2.0

MESH = pl.DeviceIdType.MESH
F32 = jnp.float32
BF16 = jnp.bfloat16


class Ids:
    def __init__(self):
        self.next = 0

    def take(self, n):
        first = self.next
        self.next += n
        return first


IDS = Ids()
Z_ID = IDS.take(6)
X_ID = [[IDS.take(3) for _ in range(2)] for _ in range(2)]
D_ID = [[IDS.take(1) for _ in range(2)] for _ in range(2)]
Y1_ID = [[IDS.take(2) for _ in range(2)] for _ in range(2)]
Y2_ID = [[IDS.take(1) for _ in range(2)] for _ in range(2)]
ROW_ID = [IDS.take(8) for _ in range(2)]
LOW_ID = [IDS.take(1) for _ in range(2)]
COL_ID = [[IDS.take(4) for _ in range(2)] for _ in range(2)]
SQ_ID = [IDS.take(4) for _ in range(2)]
OUT_ID = IDS.take(1)
SUM_ID = IDS.take(1)
TOTAL_ID = IDS.take(1)
N_ID = IDS.next

(TO_X, TO_Z, TO_SIBLING, TO_Y1, TO_Y2, TO_ROWS, TO_LOW, TO_PASS, TO_COLS, TO_SQ, TO_SQ_PASS,
 TO_OUT, TO_SUM, TO_TOTAL, N_TO) = range(15)


class Line:
    arrivals = [(3, 0), (3, 1), (1, 1), (1, 0), (2, 0), (2, 1)]
    number = [0, 2, 1, 2, 2, 2]

    def __init__(self, send, wait, base, kind, ref, plus, minus, late):
        self.send, self.wait, self.base, self.kind, self.ref = send, wait, base, kind, ref
        self.plus, self.minus, self.late = plus, minus, late

    def put(self, k, where, to):
        r = self.ref(*where)
        self.send(self.base + self.number[k], r, r, to, self.kind)

    def arrived(self, k):
        pass

    def take(self, k):
        self.wait(self.base + self.number[k], self.ref(*self.arrivals[k]))
        self.arrived(k)

    def start(self):
        self.put(0, (0, 0), self.plus)
        self.put(2, (0, 1), self.minus)
        self.put(1, (0, 1), self.plus)
        self.put(3, (0, 0), self.minus)

    def near(self):
        self.take(0)
        self.put(4, (3, 0), self.plus)
        self.take(2)
        self.put(5, (1, 1), self.minus)

    def finish(self):
        self.wait(self.base + 2, self.late)


class Passed(Line):
    def __init__(self, send, wait, base, kind, ref, plus, minus, late, sibling, pass_kind, mirrored):
        super().__init__(send, wait, base, kind, ref, plus, minus, late)
        self.sibling, self.pass_kind, self.mirrored = sibling, pass_kind, mirrored

    def pass_on(self, where):
        r = self.ref(*where)
        self.send(self.base + 3, r, r, self.sibling, self.pass_kind)

    def arrived(self, k):
        self.pass_on(self.arrivals[k])

    def start(self):
        super().start()
        self.pass_on((0, 0))
        self.pass_on((0, 1))

    def finish(self):
        super().finish()
        for k in (1, 3, 4, 5):
            self.arrived(k)

    def passed(self):
        self.wait(self.base + 3, self.mirrored)


class Plane(Line):
    arrivals = Line.arrivals + [None, (3, None, 1), (1, None, 1), (2, 0, 1), (2, 1, 1)]
    number = [0, 2, 1, 2, 3, 4, 5, 6, 6, 6, 6]

    def __init__(self, send, wait, base, kind, ref, plus, minus, late, across, needed):
        super().__init__(send, wait, base, kind, ref, plus, minus, late)
        self.across, self.needed = across, needed

    def cross(self):
        r = self.ref(0, 1 - self.needed, 0)
        self.send(self.base + 5, r, r, self.across, self.kind)

    def start(self):
        r = self.ref(0, self.needed, 0)
        self.send(self.base + 7, r, r, self.across, self.kind)
        super().start()

    def take_needed(self):
        self.wait(self.base + 5, self.ref(0, self.needed, 1))

    def other(self):
        self.wait(self.base + 7, self.ref(0, 1 - self.needed, 1))
        self.put(7, (0, None, 1), self.plus)
        self.put(8, (0, None, 1), self.minus)

    def far(self):
        self.wait(self.base + 2, self.ref(3, None))
        self.take(4)
        self.put(9, (2, 0, 0), self.across)
        self.take(5)
        self.put(10, (2, 1, 0), self.across)

    def last(self):
        self.wait(self.base + 6, self.late)


def kernel(
    act_ref, grad_ref, out_ref,
    xall, give, gram_part, drecv, y1s, y1r, y2s, y2r, scaled,
    rowbuf, colbuf, sqcol, sq, low_out, low_in, obuf, csend, crecv, totbuf,
    ssem, rsem, lsem,
):
    tok, blk = lax.axis_index("tok"), lax.axis_index("blk")
    c, y, zl = tok % 2, (tok // 2) % 4, tok // 8
    x, zh = blk // 2, blk % 2

    def tok_of(zl_, y_, c_):
        return zl_ * 8 + y_ * 2 + c_

    def blk_of(x_, zh_):
        return x_ * 2 + zh_

    x_plus = (tok, blk_of((x + 1) % 4, zh))
    x_minus = (tok, blk_of((x + 3) % 4, zh))
    zh_mate = (tok, blk_of(x, 1 - zh))
    y_plus = (tok_of(zl, (y + 1) % 4, c), blk)
    y_minus = (tok_of(zl, (y + 3) % 4, c), blk)
    zl_mate = (tok_of(1 - zl, y, c), blk)
    z_cross = (tok_of(1 - zl, y, c), blk_of(x, 1 - zh))
    sibling = (tok_of(zl, y, 1 - c), blk)

    def place(to):
        return {"tok": to[0], "blk": to[1]}

    def row_of(s, y_):
        return ((y_ + s) % 2) * 2 + y_ // 2

    def keep(s, step):
        return row_of(s, (y + step) % 4)

    zh_of = (zh, 1 - zh)

    def out_tok(e, s):
        return 2 * (2 * keep(s, 0) + zh_of[e]) + c

    source_y = ((tok // 4) % 2) * 2 + (tok // 8 + blk // 4) % 2
    home = source_y == y

    def loads(src, dst, first):
        out = []
        for s in range(2):
            for k in range(2):
                cols = pl.ds(HALF * k + PART * s, PART)
                out.append(
                    pltpu.make_async_copy(
                        src.at[:, cols], dst(s).at[:, pl.ds(PART * k, PART)],
                        lsem.at[first + 2 * s + k],
                    )
                )
        return out

    def own_block(s):
        return xall.at[0, x, s]

    def give_block(s):
        return give.at[s]

    def all_loads(own_ref, give_ref):
        return loads(own_ref, own_block, 0) + loads(give_ref, give_block, 4)

    @pl.when(zl == 0)
    def _():
        for copy in all_loads(act_ref, grad_ref):
            copy.start()

    @pl.when(zl == 1)
    def _():
        for copy in all_loads(grad_ref, act_ref):
            copy.start()

    barrier = pltpu.get_barrier_semaphore()

    def greet(to):
        pl.semaphore_signal(barrier, inc=1, device_id=place(to), device_id_type=MESH)

    def greet_tok(j, carry):
        greet(((tok + j) % 16, blk))
        return carry

    def greet_blk(j, carry):
        greet((tok, (blk + j) % 8))
        return carry

    lax.fori_loop(1, 16, greet_tok, 0)
    lax.fori_loop(1, 8, greet_blk, 0)
    greet(z_cross)

    def greet_source(j, carry):
        to = (tok_of(j % 2, source_y, c), j // 2)

        @pl.when(jnp.logical_not((to[0] == tok) & (to[1] == blk)))
        def _():
            greet(to)

        return carry

    lax.fori_loop(0, 16, greet_source, 0)
    for copy in all_loads(act_ref, grad_ref):
        copy.wait()
    pl.semaphore_wait(barrier, 15 + 7 + 1 + 16 - home.astype(jnp.int32))

    def remote(k, src, dst, to, kind):
        return pltpu.make_async_remote_copy(
            src_ref=src, dst_ref=dst, send_sem=ssem.at[kind], recv_sem=rsem.at[k],
            device_id=place(to), device_id_type=MESH,
        )

    def send(k, src, dst, to, kind):
        remote(k, src, dst, to, kind).start()

    def wait(k, dst):
        remote(k, dst, dst, sibling, 0).wait_recv()

    def left(kind, src):
        remote(0, src, src, sibling, kind).wait_send()

    token_half = (pl.ds(0, HALF), pl.ds(HALF, HALF))

    def x_line(s, t):
        def ref(step, half):
            return xall.at[t, (x + step) % 4, s, token_half[half]]

        return Line(
            send, wait, X_ID[s][t], TO_X, ref, x_plus, x_minus, xall.at[t, (x + 2) % 4]
        )

    lines = [[x_line(s, t) for t in range(2)] for s in range(2)]

    def z_first(s):
        send(Z_ID + s, give.at[s], xall.at[1, x, s], zl_mate, TO_Z)

    def z_rest(s):
        send(Z_ID + 2 + s, give.at[s], xall.at[1, 4, s], z_cross, TO_Z)
        send(Z_ID + 4 + s, xall.at[0, x, s], xall.at[0, 4, s], zh_mate, TO_Z)

    def z_first_take(s):
        wait(Z_ID + s, xall.at[1, x, s])

    def z_rest_take(s):
        wait(Z_ID + 2 + s, xall.at[1, 4, s])
        wait(Z_ID + 4 + s, xall.at[0, 4, s])

    def column_sums():
        for which, ref in ((zl, own_block), (1 - zl, give_block)):
            for s in range(2):
                values = ref(s)[...].astype(F32)
                total = jnp.sum(values * values, axis=0, keepdims=True)
                for k in range(2):
                    csend[which, :, HALF * k + PART * s : HALF * k + PART * (s + 1)] = total[
                        :, PART * k : PART * (k + 1)
                    ]

    def sum_copy(j):
        return remote(SUM_ID, csend, crecv.at[j], ((tok + j) % 16, blk), TO_SUM)

    def sums_start():
        def step(j, carry):
            sum_copy(j).start()
            return carry

        lax.fori_loop(1, 16, step, 0)

    total_to = [(tok, blk_of((x + j) % 4, zh)) for j in (1, 2, 3)] + [zh_mate]

    def total_copy(j):
        slot = x if j < 3 else 4
        return remote(TOTAL_ID, totbuf.at[x], totbuf.at[slot], total_to[j], TO_TOTAL)

    def totals_start():
        wait(SUM_ID, crecv.at[pl.ds(1, 15)])
        total = csend[...]
        for j in range(1, 16):
            total = total + crecv[j]
        totbuf[x] = total
        for j in range(4):
            total_copy(j).start()

    def totals_finish():
        wait(TOTAL_ID, totbuf.at[pl.ds(0, 4)])

    def gram(s, g):
        cols = (x, 4)[g]

        def step(i, carry):
            to = (x + 3 + i) % 4
            for s2 in range(2):
                value = None
                for t in range(2):
                    term = lax.dot_general(
                        xall[t, to, s], xall[t, cols, s2],
                        (((0,), (0,)), ((), ())), preferred_element_type=F32,
                    )
                    value = term if value is None else value + term
                value = value.astype(BF16)
                for k in range(2):
                    for k2 in range(2):
                        start = HALF * k2 + PART * s2
                        gram_part[s, g, to, k, :, start : start + PART] = value[
                            PART * k : PART * (k + 1), PART * k2 : PART * (k2 + 1)
                        ]
            d_copy(s, g, to).start()
            return carry

        lax.fori_loop(0, 4, step, 0)

    def d_copy(s, g, to):
        return remote(
            D_ID[s][g], gram_part.at[s, g, to, 1 - c], drecv.at[s, g, to], sibling, TO_SIBLING
        )

    halves = (pl.ds(0, PART // 2), pl.ds(PART // 2, PART // 2))

    def both(s, g, to, half):
        mine = gram_part[s, g, to, c, halves[half]].astype(F32)
        return mine + drecv[s, g, to, halves[half]].astype(F32)

    def reduce_start(s, g):
        y1, y2, far, up, down = Y1_ID[s][g], Y2_ID[s][g], keep(s, 2), keep(s, 1), keep(s, 3)
        wait(D_ID[s][g], drecv.at[s, g])
        y1s[s, g, 0] = both(s, g, far, 0).astype(BF16)
        send(y1, y1s.at[s, g, 0], y1r.at[s, g, 0], y_plus, TO_Y1)
        y1s[s, g, 1] = both(s, g, far, 1).astype(BF16)
        send(y1 + 1, y1s.at[s, g, 1], y1r.at[s, g, 1], y_minus, TO_Y1)
        y2s[s, g, 0] = both(s, g, up, 1).astype(BF16)
        send(y2, y2s.at[s, g, 0], y2r.at[s, g, 0], y_plus, TO_Y2)
        y2s[s, g, 2] = both(s, g, down, 0).astype(BF16)
        send(y2, y2s.at[s, g, 2], y2r.at[s, g, 2], y_minus, TO_Y2)

    def reduce_middle(s, g):
        y1, y2, up, down = Y1_ID[s][g], Y2_ID[s][g], keep(s, 1), keep(s, 3)
        wait(y1, y1r.at[s, g, 0])
        y2s[s, g, 1] = (both(s, g, up, 0) + y1r[s, g, 0].astype(F32)).astype(BF16)
        send(y2, y2s.at[s, g, 1], y2r.at[s, g, 1], y_plus, TO_Y2)
        wait(y1 + 1, y1r.at[s, g, 1])
        y2s[s, g, 3] = (both(s, g, down, 1) + y1r[s, g, 1].astype(F32)).astype(BF16)
        send(y2, y2s.at[s, g, 3], y2r.at[s, g, 3], y_minus, TO_Y2)

    def eye(s, zh_, h):
        shape = (PART, BLOCK)
        r = lax.broadcasted_iota(jnp.int32, shape, 0) + HALF * c + PART * s
        k = lax.broadcasted_iota(jnp.int32, shape, 1)
        return (r + BLOCK * (2 * keep(s, 0) + zh_) == k + BLOCK * (2 * x + h)).astype(F32)

    def inverse(sums):
        return lax.rsqrt(sums / TOKENS + epsilon)

    def lane_block(block):
        return pl.ds(pl.multiple_of(block * BLOCK, BLOCK), BLOCK)

    def normalise(s):
        rows = pl.ds(pl.multiple_of(HALF * c + PART * s, PART), PART)
        inv_row = jnp.broadcast_to(inverse(totbuf[keep(s, 0), zl, :, rows]), (PART, PART))
        inv_row = jnp.concatenate([jnp.transpose(inv_row)] * 4, axis=1)
        for g in (0, 1) if s == 0 else (1, 0):
            wait(Y2_ID[s][g], y2r.at[s, g])
            inv_col = inverse(totbuf[(x, 4)[g], zl])
            low = both(s, g, keep(s, 0), 0) + y2r[s, g, 1].astype(F32) + y2r[s, g, 2].astype(F32)
            high = both(s, g, keep(s, 0), 1) + y2r[s, g, 0].astype(F32) + y2r[s, g, 3].astype(F32)
            total = jnp.concatenate([low, high], axis=0)
            damped = total / TOKENS * inv_row * inv_col + damping * eye(s, zh, zh_of[g])
            value = damped / divisor
            half = value.astype(BF16)
            rowbuf[zh, s, zh_of[g], :, lane_block(x)] = half
            if g == 0:
                scaled[0, s] = value
                colbuf[keep(s, 0), zh, c, s] = half
                cols[s][0].start()
            else:
                rows_of[s].cross()
                low_out[s] = (value - half.astype(F32)).astype(BF16)
        rows_of[s].start()
        send(LOW_ID[s], low_out.at[s], low_in.at[s], zh_mate, TO_LOW)

    def partner(s):
        half = rowbuf[1 - zh, s, zh, :, lane_block(x)]
        colbuf[keep(s, 0), 1 - zh, c, s] = half
        cols[s][1].start()

    def partner_low(s):
        wait(LOW_ID[s], low_in.at[s])
        half = rowbuf[1 - zh, s, zh, :, lane_block(x)].astype(F32)
        scaled[1, s] = half + low_in[s].astype(F32)

    def row_plane(s):
        def ref(step, half, other=0):
            lanes = lane_block((x + step) % 4)
            r = rowbuf.at[zh_of[other], s]
            return r.at[:, :, lanes] if half is None else r.at[half, :, lanes]

        late = rowbuf.at[1 - zh, s, :, :, pl.ds(0, 3 * BLOCK)]
        return Plane(
            send, wait, ROW_ID[s], TO_ROWS, ref, x_plus, x_minus, late, zh_mate, zh
        )

    def col_line(s, e):
        def ref(step, half):
            return colbuf.at[keep(s, step), zh_of[e], c, s, halves[half]]

        late = colbuf.at[pl.ds(0, 2), zh_of[e], c, s]
        return Passed(
            send, wait, COL_ID[s][e], TO_COLS, ref, y_plus, y_minus, late, sibling, TO_PASS,
            colbuf.at[:, zh_of[e], 1 - c, s],
        )

    def sq_line(e):
        def ref(step, half):
            return sqcol.at[keep(half, step), zh_of[e], c, half]

        late = sqcol.at[pl.ds(0, 2), zh_of[e], c]
        return Passed(
            send, wait, SQ_ID[e], TO_SQ, ref, y_plus, y_minus, late, sibling, TO_SQ_PASS,
            sqcol.at[:, zh_of[e], 1 - c],
        )

    rows_of = [row_plane(s) for s in range(2)]
    cols = [[col_line(s, e) for e in range(2)] for s in range(2)]
    sq_cols = [sq_line(e) for e in range(2)]

    def dot(e, p, right, lanes):
        return jnp.dot(
            rowbuf[zh_of[e], :, p].reshape(HALF, D // 2),
            right[:, p, :, :, :, lanes].reshape(D // 2, HALF),
            preferred_element_type=F32,
        )

    def over_lanes(body):
        def step(k, carry):
            body(pl.ds(pl.multiple_of(k * HALF, HALF), HALF))
            return carry

        lax.fori_loop(0, 2, step, 0)

    def square(e):
        def some(lanes):
            sq[e, :, lanes] = dot(e, 0, colbuf, lanes) + dot(e, 1, colbuf, lanes)

        over_lanes(some)
        for s in range(2):
            sqcol[keep(s, 0), zh_of[e], c, s] = sq[e, PART * s : PART * (s + 1)].astype(BF16)
        sq_cols[e].start()

    def combine(e):
        for s in range(2):
            scaled[e, s] = (
                4.0 * eye(s, zh_of[e], zh) - 6.0 * scaled[e, s]
                + 4.0 * sq[e, PART * s : PART * (s + 1)]
            )

    def cube_first():
        for e in range(2):
            def some(lanes):
                sq[e, :, lanes] = dot(e, zh, sqcol, lanes)

            over_lanes(some)

    def cube_second(e):
        def some(lanes):
            value = scaled[e, :, :, lanes].reshape(HALF, HALF) - sq[e, :, lanes]
            obuf[e, :, lanes] = (value - dot(e, 1 - zh, sqcol, lanes)).astype(BF16)

        over_lanes(some)
        for b in range(8):
            me = (out_tok(e, b // 4) == tok) & (blk == b)

            @pl.when(me)
            def _():
                out_ref[zl, :, lane_block(2 * x + zh)] = obuf[e, b * 32 : (b + 1) * 32]

            @pl.when(jnp.logical_not(me))
            def _():
                out_copy(e, b).start()

    def out_copy(e, b):
        return remote(
            OUT_ID, obuf.at[e, pl.ds(b * 32, 32)], out_ref.at[zl, :, lane_block(2 * x + zh)],
            (out_tok(e, b // 4), b), TO_OUT,
        )

    def emit():
        @pl.when(home)
        def _():
            wait(OUT_ID, out_ref.at[:, :, pl.ds(0, 15 * HALF)])
            left(TO_OUT, obuf.at[:, pl.ds(0, 15 * 16)])

        @pl.when(jnp.logical_not(home))
        def _():
            wait(OUT_ID, out_ref)
            left(TO_OUT, obuf)

    def all_left():
        left(TO_X, xall.at[:, pl.ds(0, 3)])
        left(TO_Z, xall.at[0, pl.ds(0, 3)])
        left(TO_SIBLING, gram_part.at[0])
        left(TO_Y1, y1s)
        left(TO_Y2, y2s)
        left(TO_ROWS, rowbuf.at[:, :, :, pl.ds(0, 112)])
        left(TO_LOW, low_out)
        left(TO_PASS, colbuf.at[pl.ds(0, 2)])
        left(TO_COLS, colbuf.at[pl.ds(0, 3), 0])
        left(TO_SQ, sqcol.at[pl.ds(0, 3), 0])
        left(TO_SQ_PASS, sqcol.at[pl.ds(0, 2)])
        left(TO_SUM, crecv.at[pl.ds(1, 15)])
        left(TO_TOTAL, totbuf.at[pl.ds(0, 4)])

    z_first(0)
    lines[0][0].start()
    column_sums()
    sums_start()
    z_first(1)
    z_rest(0)
    z_rest(1)
    lines[0][0].near()
    z_first_take(0)
    lines[0][1].start()
    totals_start()
    lines[0][1].near()
    lines[1][0].start()
    z_first_take(1)
    lines[1][1].start()
    lines[0][0].finish()
    lines[0][1].finish()
    gram(0, 0)
    reduce_start(0, 0)
    lines[1][0].near()
    z_rest_take(0)
    z_rest_take(1)
    gram(0, 1)
    reduce_middle(0, 0)
    reduce_start(0, 1)
    lines[1][1].near()
    reduce_middle(0, 1)
    totals_finish()
    normalise(0)
    lines[1][0].finish()
    lines[1][1].finish()
    gram(1, 1)
    gram(1, 0)
    reduce_start(1, 1)
    cols[0][0].near()
    rows_of[0].near()
    reduce_start(1, 0)
    reduce_middle(1, 1)
    rows_of[0].take_needed()
    partner(0)
    reduce_middle(1, 0)
    rows_of[0].other()
    cols[0][0].finish()
    rows_of[0].far()
    normalise(1)
    cols[0][1].near()
    cols[1][0].near()
    rows_of[1].near()
    cols[0][1].finish()
    rows_of[1].take_needed()
    partner(1)
    cols[1][0].finish()
    rows_of[1].other()
    cols[1][1].near()
    rows_of[1].far()
    cols[1][1].finish()
    for s in range(2):
        for e in range(2):
            cols[s][e].passed()
    square(0)
    rows_of[0].last()
    rows_of[1].last()
    square(1)
    combine(0)
    sq_cols[0].near()
    sq_cols[0].finish()
    partner_low(0)
    partner_low(1)
    combine(1)
    sq_cols[1].near()
    sq_cols[0].passed()
    cube_first()
    sq_cols[1].finish()
    sq_cols[1].passed()
    cube_second(0)
    cube_second(1)
    all_left()
    emit()


def body(activations, out_grads):
    hbm = pl.BlockSpec(memory_space=pltpu.HBM)
    vmem = pl.BlockSpec(memory_space=pltpu.VMEM)
    part = (PART, BLOCK)
    half_part = (PART // 2, BLOCK)
    scratch = [
        pltpu.VMEM((2, 5, 2, BLOCK, HALF), BF16),
        pltpu.VMEM((2, BLOCK, HALF), BF16),
        pltpu.VMEM((2, 2, 4, 2, *part), BF16),
        pltpu.VMEM((2, 2, 4, *part), BF16),
        pltpu.VMEM((2, 2, 2, *half_part), BF16),
        pltpu.VMEM((2, 2, 2, *half_part), BF16),
        pltpu.VMEM((2, 2, 4, *half_part), BF16),
        pltpu.VMEM((2, 2, 4, *half_part), BF16),
        pltpu.VMEM((2, 2, *part), F32),
        pltpu.VMEM((2, 2, 2, PART, D // 2), BF16),
        pltpu.VMEM((4, 2, 2, 2, *part), BF16),
        pltpu.VMEM((4, 2, 2, 2, *part), BF16),
        pltpu.VMEM((2, HALF, BLOCK), F32),
        pltpu.VMEM((2, *part), BF16),
        pltpu.VMEM((2, *part), BF16),
        pltpu.VMEM((2, HALF, BLOCK), BF16),
        pltpu.VMEM((2, 1, BLOCK), F32),
        pltpu.VMEM((16, 2, 1, BLOCK), F32),
        pltpu.VMEM((5, 2, 1, BLOCK), F32),
        pltpu.SemaphoreType.DMA((N_TO,)),
        pltpu.SemaphoreType.DMA((N_ID,)),
        pltpu.SemaphoreType.DMA((8,)),
    ]
    out = pl.pallas_call(
        kernel,
        out_shape=jax.ShapeDtypeStruct((2, 32, D), BF16),
        in_specs=[hbm, hbm],
        out_specs=vmem,
        scratch_shapes=scratch,
        compiler_params=pltpu.CompilerParams(
            collective_id=0, has_side_effects=True, vmem_limit_bytes=60 * 1024 * 1024
        ),
    )(activations, out_grads)
    return out[0].astype(F32), out[1].astype(F32)


def solution(mesh):
    placed = (P("tok", "blk"), P("tok", "blk"))
    return jax.shard_map(
        body,
        mesh=mesh,
        in_specs=placed,
        out_specs=(P(("tok", "blk"), None), P(("tok", "blk"), None)),
        check_vma=False,
    )
```

```python
import jax
import jax.numpy as jnp
from jax import lax
from jax.experimental import pallas as pl
from jax.experimental.pallas import tpu as pltpu
from jax.sharding import PartitionSpec as P

D = 4096
TOKENS = 8192
BLOCK = 512
HALF = 256
PART = 128

damping = 0.3
epsilon = 1e-06
divisor = 2.0

MESH = pl.DeviceIdType.MESH
F32 = jnp.float32
BF16 = jnp.bfloat16


class Ids:
    def __init__(self):
        self.next = 0

    def take(self, n):
        first = self.next
        self.next += n
        return first


IDS = Ids()
Z_ID = IDS.take(6)
X_ID = [[IDS.take(3) for _ in range(2)] for _ in range(2)]
D_ID = [[IDS.take(1) for _ in range(2)] for _ in range(2)]
Y1_ID = [[IDS.take(2) for _ in range(2)] for _ in range(2)]
Y2_ID = [[IDS.take(1) for _ in range(2)] for _ in range(2)]
ROW_ID = [IDS.take(8) for _ in range(2)]
LOW_ID = [IDS.take(1) for _ in range(2)]
COL_ID = [[IDS.take(5) for _ in range(2)] for _ in range(2)]
SQ_ID = [IDS.take(5) for _ in range(2)]
OUT_ID = IDS.take(1)
SUM_ID = IDS.take(1)
TOTAL_ID = IDS.take(1)
N_ID = IDS.next

(TO_X, TO_Z, TO_SIBLING, TO_Y1, TO_Y2, TO_ROWS, TO_LOW, TO_PASS, TO_COLS, TO_SQ, TO_SQ_PASS,
 TO_OUT, TO_SUM, TO_TOTAL, N_TO) = range(15)


class Line:
    arrivals = [(3, 0), (3, 1), (1, 1), (1, 0), (2, 0), (2, 1)]
    number = [0, 2, 1, 2, 2, 2]

    def __init__(self, send, wait, base, kind, ref, plus, minus, late):
        self.send, self.wait, self.base, self.kind, self.ref = send, wait, base, kind, ref
        self.plus, self.minus, self.late = plus, minus, late

    def put(self, k, where, to):
        r = self.ref(*where)
        self.send(self.base + self.number[k], r, r, to, self.kind)

    def arrived(self, k):
        pass

    def take(self, k):
        self.wait(self.base + self.number[k], self.ref(*self.arrivals[k]))
        self.arrived(k)

    def start(self):
        self.put(0, (0, 0), self.plus)
        self.put(2, (0, 1), self.minus)
        self.put(1, (0, 1), self.plus)
        self.put(3, (0, 0), self.minus)

    def near(self):
        self.take(0)
        self.put(4, (3, 0), self.plus)
        self.take(2)
        self.put(5, (1, 1), self.minus)

    def finish(self):
        self.wait(self.base + 2, self.late)


class Passed(Line):
    number = [0, 2, 1, 2, 4, 4]

    def __init__(self, send, wait, base, kind, ref, plus, minus, late, sibling, pass_kind, mirrored):
        super().__init__(send, wait, base, kind, ref, plus, minus, late)
        self.sibling, self.pass_kind, self.mirrored = sibling, pass_kind, mirrored

    def pass_on(self, where):
        r = self.ref(*where)
        self.send(self.base + 3, r, r, self.sibling, self.pass_kind)

    def arrived(self, k):
        self.pass_on(self.arrivals[k])

    def start(self):
        super().start()
        self.pass_on((0, 0))
        self.pass_on((0, 1))

    def rest(self):
        self.wait(self.base + 2, self.late)
        self.arrived(1)
        self.arrived(3)

    def finish(self):
        self.wait(self.base + 4, self.late)
        self.arrived(4)
        self.arrived(5)

    def passed(self):
        self.wait(self.base + 3, self.mirrored)


class Plane(Line):
    arrivals = Line.arrivals + [None, (3, None, 1), (1, None, 1), (2, 0, 1), (2, 1, 1)]
    number = [0, 2, 1, 2, 3, 4, 5, 6, 6, 6, 6]

    def __init__(self, send, wait, base, kind, ref, plus, minus, late, across, needed):
        super().__init__(send, wait, base, kind, ref, plus, minus, late)
        self.across, self.needed = across, needed

    def cross(self):
        r = self.ref(0, 1 - self.needed, 0)
        self.send(self.base + 5, r, r, self.across, self.kind)

    def start(self):
        r = self.ref(0, self.needed, 0)
        self.send(self.base + 7, r, r, self.across, self.kind)
        super().start()

    def take_needed(self):
        self.wait(self.base + 5, self.ref(0, self.needed, 1))

    def other(self):
        self.wait(self.base + 7, self.ref(0, 1 - self.needed, 1))
        self.put(7, (0, None, 1), self.plus)
        self.put(8, (0, None, 1), self.minus)

    def far(self):
        self.wait(self.base + 2, self.ref(3, None))
        self.take(4)
        self.put(9, (2, 0, 0), self.across)
        self.take(5)
        self.put(10, (2, 1, 0), self.across)

    def last(self):
        self.wait(self.base + 6, self.late)


def kernel(
    act_ref, grad_ref, out_ref,
    xall, give, gram_part, drecv, y1s, y1r, y2s, y2r, scaled,
    rowbuf, colbuf, sqcol, sq, low_out, low_in, obuf, csend, crecv, totbuf,
    ssem, rsem, lsem,
):
    tok, blk = lax.axis_index("tok"), lax.axis_index("blk")
    c, y, zl = tok % 2, (tok // 2) % 4, tok // 8
    x, zh = blk // 2, blk % 2

    def tok_of(zl_, y_, c_):
        return zl_ * 8 + y_ * 2 + c_

    def blk_of(x_, zh_):
        return x_ * 2 + zh_

    x_plus = (tok, blk_of((x + 1) % 4, zh))
    x_minus = (tok, blk_of((x + 3) % 4, zh))
    zh_mate = (tok, blk_of(x, 1 - zh))
    y_plus = (tok_of(zl, (y + 1) % 4, c), blk)
    y_minus = (tok_of(zl, (y + 3) % 4, c), blk)
    zl_mate = (tok_of(1 - zl, y, c), blk)
    z_cross = (tok_of(1 - zl, y, c), blk_of(x, 1 - zh))
    sibling = (tok_of(zl, y, 1 - c), blk)

    def place(to):
        return {"tok": to[0], "blk": to[1]}

    def row_of(s, y_):
        return ((y_ + s) % 2) * 2 + y_ // 2

    def keep(s, step):
        return row_of(s, (y + step) % 4)

    zh_of = (zh, 1 - zh)

    def out_tok(e, s):
        return 2 * (2 * keep(s, 0) + zh_of[e]) + c

    source_y = ((tok // 4) % 2) * 2 + (tok // 8 + blk // 4) % 2
    home = source_y == y

    def loads(src, dst, first):
        out = []
        for s in range(2):
            for k in range(2):
                cols = pl.ds(HALF * k + PART * s, PART)
                out.append(
                    pltpu.make_async_copy(
                        src.at[:, cols], dst(s).at[:, pl.ds(PART * k, PART)],
                        lsem.at[first + 2 * s + k],
                    )
                )
        return out

    def own_block(s):
        return xall.at[0, x, s]

    def give_block(s):
        return give.at[s]

    def all_loads(own_ref, give_ref):
        return loads(own_ref, own_block, 0) + loads(give_ref, give_block, 4)

    @pl.when(zl == 0)
    def _():
        for copy in all_loads(act_ref, grad_ref):
            copy.start()

    @pl.when(zl == 1)
    def _():
        for copy in all_loads(grad_ref, act_ref):
            copy.start()

    barrier = pltpu.get_barrier_semaphore()

    def greet(to):
        pl.semaphore_signal(barrier, inc=1, device_id=place(to), device_id_type=MESH)

    def greet_tok(j, carry):
        greet(((tok + j) % 16, blk))
        return carry

    def greet_blk(j, carry):
        greet((tok, (blk + j) % 8))
        return carry

    lax.fori_loop(1, 16, greet_tok, 0)
    lax.fori_loop(1, 8, greet_blk, 0)
    greet(z_cross)

    def greet_source(j, carry):
        to = (tok_of(j % 2, source_y, c), j // 2)

        @pl.when(jnp.logical_not((to[0] == tok) & (to[1] == blk)))
        def _():
            greet(to)

        return carry

    lax.fori_loop(0, 16, greet_source, 0)
    for copy in all_loads(act_ref, grad_ref):
        copy.wait()
    pl.semaphore_wait(barrier, 15 + 7 + 1 + 16 - home.astype(jnp.int32))

    def remote(k, src, dst, to, kind):
        return pltpu.make_async_remote_copy(
            src_ref=src, dst_ref=dst, send_sem=ssem.at[kind], recv_sem=rsem.at[k],
            device_id=place(to), device_id_type=MESH,
        )

    def send(k, src, dst, to, kind):
        remote(k, src, dst, to, kind).start()

    def wait(k, dst):
        remote(k, dst, dst, sibling, 0).wait_recv()

    def left(kind, src):
        remote(0, src, src, sibling, kind).wait_send()

    token_half = (pl.ds(0, HALF), pl.ds(HALF, HALF))

    def x_line(s, t):
        def ref(step, half):
            return xall.at[t, (x + step) % 4, s, token_half[half]]

        return Line(
            send, wait, X_ID[s][t], TO_X, ref, x_plus, x_minus, xall.at[t, (x + 2) % 4]
        )

    lines = [[x_line(s, t) for t in range(2)] for s in range(2)]

    def z_first(s):
        send(Z_ID + s, give.at[s], xall.at[1, x, s], zl_mate, TO_Z)

    def z_rest(s):
        send(Z_ID + 2 + s, give.at[s], xall.at[1, 4, s], z_cross, TO_Z)
        send(Z_ID + 4 + s, xall.at[0, x, s], xall.at[0, 4, s], zh_mate, TO_Z)

    def z_first_take(s):
        wait(Z_ID + s, xall.at[1, x, s])

    def z_rest_take(s):
        wait(Z_ID + 2 + s, xall.at[1, 4, s])
        wait(Z_ID + 4 + s, xall.at[0, 4, s])

    def column_sums():
        for which, ref in ((zl, own_block), (1 - zl, give_block)):
            for s in range(2):
                values = ref(s)[...].astype(F32)
                total = jnp.sum(values * values, axis=0, keepdims=True)
                for k in range(2):
                    csend[which, :, HALF * k + PART * s : HALF * k + PART * (s + 1)] = total[
                        :, PART * k : PART * (k + 1)
                    ]

    def sum_copy(j):
        return remote(SUM_ID, csend, crecv.at[j], ((tok + j) % 16, blk), TO_SUM)

    def sums_start():
        def step(j, carry):
            sum_copy(j).start()
            return carry

        lax.fori_loop(1, 16, step, 0)

    total_to = [(tok, blk_of((x + j) % 4, zh)) for j in (1, 2, 3)] + [zh_mate]

    def total_copy(j):
        slot = x if j < 3 else 4
        return remote(TOTAL_ID, totbuf.at[x], totbuf.at[slot], total_to[j], TO_TOTAL)

    def totals_start():
        wait(SUM_ID, crecv.at[pl.ds(1, 15)])
        total = csend[...]
        for j in range(1, 16):
            total = total + crecv[j]
        totbuf[x] = total
        for j in range(4):
            total_copy(j).start()

    def totals_finish():
        wait(TOTAL_ID, totbuf.at[pl.ds(0, 4)])

    def gram(s, g):
        cols = (x, 4)[g]

        def step(i, carry):
            to = (x + 3 + i) % 4
            for s2 in range(2):
                value = None
                for t in range(2):
                    term = lax.dot_general(
                        xall[t, to, s], xall[t, cols, s2],
                        (((0,), (0,)), ((), ())), preferred_element_type=F32,
                    )
                    value = term if value is None else value + term
                value = value.astype(BF16)
                for k in range(2):
                    for k2 in range(2):
                        start = HALF * k2 + PART * s2
                        gram_part[s, g, to, k, :, start : start + PART] = value[
                            PART * k : PART * (k + 1), PART * k2 : PART * (k2 + 1)
                        ]
            d_copy(s, g, to).start()
            return carry

        lax.fori_loop(0, 4, step, 0)

    def d_copy(s, g, to):
        return remote(
            D_ID[s][g], gram_part.at[s, g, to, 1 - c], drecv.at[s, g, to], sibling, TO_SIBLING
        )

    halves = (pl.ds(0, PART // 2), pl.ds(PART // 2, PART // 2))

    def both(s, g, to, half):
        mine = gram_part[s, g, to, c, halves[half]].astype(F32)
        return mine + drecv[s, g, to, halves[half]].astype(F32)

    def reduce_first(s, g):
        y1, far = Y1_ID[s][g], keep(s, 2)
        wait(D_ID[s][g], drecv.at[s, g])
        y1s[s, g, 0] = both(s, g, far, 0).astype(BF16)
        send(y1, y1s.at[s, g, 0], y1r.at[s, g, 0], y_plus, TO_Y1)
        y1s[s, g, 1] = both(s, g, far, 1).astype(BF16)
        send(y1 + 1, y1s.at[s, g, 1], y1r.at[s, g, 1], y_minus, TO_Y1)

    def reduce_own(s, g):
        y2, up, down = Y2_ID[s][g], keep(s, 1), keep(s, 3)
        y2s[s, g, 0] = both(s, g, up, 1).astype(BF16)
        send(y2, y2s.at[s, g, 0], y2r.at[s, g, 0], y_plus, TO_Y2)
        y2s[s, g, 2] = both(s, g, down, 0).astype(BF16)
        send(y2, y2s.at[s, g, 2], y2r.at[s, g, 2], y_minus, TO_Y2)

    def reduce_middle(s, g):
        y1, y2, up, down = Y1_ID[s][g], Y2_ID[s][g], keep(s, 1), keep(s, 3)
        wait(y1, y1r.at[s, g, 0])
        y2s[s, g, 1] = (both(s, g, up, 0) + y1r[s, g, 0].astype(F32)).astype(BF16)
        send(y2, y2s.at[s, g, 1], y2r.at[s, g, 1], y_plus, TO_Y2)
        wait(y1 + 1, y1r.at[s, g, 1])
        y2s[s, g, 3] = (both(s, g, down, 1) + y1r[s, g, 1].astype(F32)).astype(BF16)
        send(y2, y2s.at[s, g, 3], y2r.at[s, g, 3], y_minus, TO_Y2)

    def eye(s, zh_, h):
        shape = (PART, BLOCK)
        r = lax.broadcasted_iota(jnp.int32, shape, 0) + HALF * c + PART * s
        k = lax.broadcasted_iota(jnp.int32, shape, 1)
        return (r + BLOCK * (2 * keep(s, 0) + zh_) == k + BLOCK * (2 * x + h)).astype(F32)

    def inverse(sums):
        return lax.rsqrt(sums / TOKENS + epsilon)

    def lane_block(block):
        return pl.ds(pl.multiple_of(block * BLOCK, BLOCK), BLOCK)

    def normalise(s):
        rows = pl.ds(pl.multiple_of(HALF * c + PART * s, PART), PART)
        inv_row = jnp.broadcast_to(inverse(totbuf[keep(s, 0), zl, :, rows]), (PART, PART))
        inv_row = jnp.concatenate([jnp.transpose(inv_row)] * 4, axis=1)
        for g in (0, 1) if s == 0 else (1, 0):
            wait(Y2_ID[s][g], y2r.at[s, g])
            inv_col = inverse(totbuf[(x, 4)[g], zl])
            low = both(s, g, keep(s, 0), 0) + y2r[s, g, 1].astype(F32) + y2r[s, g, 2].astype(F32)
            high = both(s, g, keep(s, 0), 1) + y2r[s, g, 0].astype(F32) + y2r[s, g, 3].astype(F32)
            total = jnp.concatenate([low, high], axis=0)
            damped = total / TOKENS * inv_row * inv_col + damping * eye(s, zh, zh_of[g])
            value = damped / divisor
            half = value.astype(BF16)
            rowbuf[zh, s, zh_of[g], :, lane_block(x)] = half
            if g == 0:
                scaled[0, s] = value
                colbuf[keep(s, 0), zh, c, s] = half
                cols[s][0].start()
            else:
                rows_of[s].cross()
                low_out[s] = (value - half.astype(F32)).astype(BF16)
        rows_of[s].start()
        send(LOW_ID[s], low_out.at[s], low_in.at[s], zh_mate, TO_LOW)

    def partner(s):
        half = rowbuf[1 - zh, s, zh, :, lane_block(x)]
        colbuf[keep(s, 0), 1 - zh, c, s] = half
        cols[s][1].start()

    def partner_low(s):
        wait(LOW_ID[s], low_in.at[s])
        half = rowbuf[1 - zh, s, zh, :, lane_block(x)].astype(F32)
        scaled[1, s] = half + low_in[s].astype(F32)

    def row_plane(s):
        def ref(step, half, other=0):
            lanes = lane_block((x + step) % 4)
            r = rowbuf.at[zh_of[other], s]
            return r.at[:, :, lanes] if half is None else r.at[half, :, lanes]

        late = rowbuf.at[1 - zh, s, :, :, pl.ds(0, 3 * BLOCK)]
        return Plane(
            send, wait, ROW_ID[s], TO_ROWS, ref, x_plus, x_minus, late, zh_mate, zh
        )

    def col_line(s, e):
        def ref(step, half):
            return colbuf.at[keep(s, step), zh_of[e], c, s, halves[half]]

        late = colbuf.at[0, zh_of[e], c, s]
        return Passed(
            send, wait, COL_ID[s][e], TO_COLS, ref, y_plus, y_minus, late, sibling, TO_PASS,
            colbuf.at[:, zh_of[e], 1 - c, s],
        )

    def sq_line(e):
        def ref(step, half):
            return sqcol.at[keep(half, step), zh_of[e], c, half]

        late = sqcol.at[0, zh_of[e], c]
        return Passed(
            send, wait, SQ_ID[e], TO_SQ, ref, y_plus, y_minus, late, sibling, TO_SQ_PASS,
            sqcol.at[:, zh_of[e], 1 - c],
        )

    rows_of = [row_plane(s) for s in range(2)]
    cols = [[col_line(s, e) for e in range(2)] for s in range(2)]
    sq_cols = [sq_line(e) for e in range(2)]

    def dot(e, p, right, lanes):
        return jnp.dot(
            rowbuf[zh_of[e], :, p].reshape(HALF, D // 2),
            right[:, p, :, :, :, lanes].reshape(D // 2, HALF),
            preferred_element_type=F32,
        )

    def over_lanes(body):
        def step(k, carry):
            body(pl.ds(pl.multiple_of(k * HALF, HALF), HALF))
            return carry

        lax.fori_loop(0, 2, step, 0)

    def square(e):
        def some(lanes):
            sq[e, :, lanes] = dot(e, 0, colbuf, lanes) + dot(e, 1, colbuf, lanes)

        over_lanes(some)
        for s in range(2):
            sqcol[keep(s, 0), zh_of[e], c, s] = sq[e, PART * s : PART * (s + 1)].astype(BF16)
        sq_cols[e].start()

    def combine(e):
        for s in range(2):
            scaled[e, s] = (
                4.0 * eye(s, zh_of[e], zh) - 6.0 * scaled[e, s]
                + 4.0 * sq[e, PART * s : PART * (s + 1)]
            )

    def cube_first():
        for e in range(2):
            def some(lanes):
                sq[e, :, lanes] = dot(e, zh, sqcol, lanes)

            over_lanes(some)

    def cube_second(e):
        def some(lanes):
            value = scaled[e, :, :, lanes].reshape(HALF, HALF) - sq[e, :, lanes]
            obuf[e, :, lanes] = (value - dot(e, 1 - zh, sqcol, lanes)).astype(BF16)

        over_lanes(some)
        for b in range(8):
            me = (out_tok(e, b // 4) == tok) & (blk == b)

            @pl.when(me)
            def _():
                out_ref[zl, :, lane_block(2 * x + zh)] = obuf[e, b * 32 : (b + 1) * 32]

            @pl.when(jnp.logical_not(me))
            def _():
                out_copy(e, b).start()

    def out_copy(e, b):
        return remote(
            OUT_ID, obuf.at[e, pl.ds(b * 32, 32)], out_ref.at[zl, :, lane_block(2 * x + zh)],
            (out_tok(e, b // 4), b), TO_OUT,
        )

    def emit():
        @pl.when(home)
        def _():
            wait(OUT_ID, out_ref.at[:, :, pl.ds(0, 15 * HALF)])
            left(TO_OUT, obuf.at[:, pl.ds(0, 15 * 16)])

        @pl.when(jnp.logical_not(home))
        def _():
            wait(OUT_ID, out_ref)
            left(TO_OUT, obuf)

    def all_left():
        left(TO_X, xall.at[:, pl.ds(0, 3)])
        left(TO_Z, xall.at[0, pl.ds(0, 3)])
        left(TO_SIBLING, gram_part.at[0])
        left(TO_Y1, y1s)
        left(TO_Y2, y2s)
        left(TO_ROWS, rowbuf.at[:, :, :, pl.ds(0, 112)])
        left(TO_LOW, low_out)
        left(TO_PASS, colbuf.at[pl.ds(0, 2)])
        left(TO_COLS, colbuf.at[pl.ds(0, 3), 0])
        left(TO_SQ, sqcol.at[pl.ds(0, 3), 0])
        left(TO_SQ_PASS, sqcol.at[pl.ds(0, 2)])
        left(TO_SUM, crecv.at[pl.ds(1, 15)])
        left(TO_TOTAL, totbuf.at[pl.ds(0, 4)])

    z_first(0)
    lines[0][0].start()
    column_sums()
    sums_start()
    z_first(1)
    z_rest(0)
    z_rest(1)
    lines[0][0].near()
    z_first_take(0)
    lines[0][1].start()
    totals_start()
    lines[0][1].near()
    lines[1][0].start()
    z_first_take(1)
    lines[1][1].start()
    lines[0][0].finish()
    lines[0][1].finish()
    gram(0, 0)
    reduce_first(0, 0)
    reduce_own(0, 0)
    lines[1][0].near()
    z_rest_take(0)
    z_rest_take(1)
    gram(0, 1)
    reduce_middle(0, 0)
    reduce_first(0, 1)
    reduce_own(0, 1)
    lines[1][1].near()
    reduce_middle(0, 1)
    totals_finish()
    normalise(0)
    lines[1][0].finish()
    lines[1][1].finish()
    gram(1, 1)
    gram(1, 0)
    reduce_first(1, 1)
    reduce_first(1, 0)
    reduce_own(1, 1)
    reduce_own(1, 0)
    rows_of[0].near()
    reduce_middle(1, 1)
    rows_of[0].take_needed()
    rows_of[0].other()
    reduce_middle(1, 0)
    cols[0][0].near()
    partner(0)
    cols[0][0].rest()
    rows_of[0].far()
    normalise(1)
    cols[0][0].finish()
    cols[0][1].near()
    cols[1][0].near()
    cols[0][1].rest()
    rows_of[1].near()
    rows_of[1].take_needed()
    partner(1)
    cols[0][1].finish()
    cols[1][0].rest()
    rows_of[1].other()
    cols[1][0].finish()
    cols[1][1].near()
    rows_of[1].far()
    cols[1][1].rest()
    cols[1][1].finish()
    for s in range(2):
        for e in range(2):
            cols[s][e].passed()
    square(0)
    rows_of[0].last()
    rows_of[1].last()
    square(1)
    sq_cols[0].near()
    combine(0)
    partner_low(0)
    partner_low(1)
    combine(1)
    sq_cols[1].near()
    sq_cols[0].rest()
    sq_cols[0].finish()
    sq_cols[1].rest()
    sq_cols[0].passed()
    cube_first()
    sq_cols[1].finish()
    sq_cols[1].passed()
    cube_second(0)
    cube_second(1)
    all_left()
    emit()


def body(activations, out_grads):
    hbm = pl.BlockSpec(memory_space=pltpu.HBM)
    vmem = pl.BlockSpec(memory_space=pltpu.VMEM)
    part = (PART, BLOCK)
    half_part = (PART // 2, BLOCK)
    scratch = [
        pltpu.VMEM((2, 5, 2, BLOCK, HALF), BF16),
        pltpu.VMEM((2, BLOCK, HALF), BF16),
        pltpu.VMEM((2, 2, 4, 2, *part), BF16),
        pltpu.VMEM((2, 2, 4, *part), BF16),
        pltpu.VMEM((2, 2, 2, *half_part), BF16),
        pltpu.VMEM((2, 2, 2, *half_part), BF16),
        pltpu.VMEM((2, 2, 4, *half_part), BF16),
        pltpu.VMEM((2, 2, 4, *half_part), BF16),
        pltpu.VMEM((2, 2, *part), F32),
        pltpu.VMEM((2, 2, 2, PART, D // 2), BF16),
        pltpu.VMEM((4, 2, 2, 2, *part), BF16),
        pltpu.VMEM((4, 2, 2, 2, *part), BF16),
        pltpu.VMEM((2, HALF, BLOCK), F32),
        pltpu.VMEM((2, *part), BF16),
        pltpu.VMEM((2, *part), BF16),
        pltpu.VMEM((2, HALF, BLOCK), BF16),
        pltpu.VMEM((2, 1, BLOCK), F32),
        pltpu.VMEM((16, 2, 1, BLOCK), F32),
        pltpu.VMEM((5, 2, 1, BLOCK), F32),
        pltpu.SemaphoreType.DMA((N_TO,)),
        pltpu.SemaphoreType.DMA((N_ID,)),
        pltpu.SemaphoreType.DMA((8,)),
    ]
    out = pl.pallas_call(
        kernel,
        out_shape=jax.ShapeDtypeStruct((2, 32, D), BF16),
        in_specs=[hbm, hbm],
        out_specs=vmem,
        scratch_shapes=scratch,
        compiler_params=pltpu.CompilerParams(
            collective_id=0, has_side_effects=True, vmem_limit_bytes=60 * 1024 * 1024
        ),
    )(activations, out_grads)
    return out[0].astype(F32), out[1].astype(F32)


def solution(mesh):
    placed = (P("tok", "blk"), P("tok", "blk"))
    return jax.shard_map(
        body,
        mesh=mesh,
        in_specs=placed,
        out_specs=(P(("tok", "blk"), None), P(("tok", "blk"), None)),
        check_vma=False,
    )
```

```python
import jax
import jax.numpy as jnp
from jax import lax
from jax.experimental import pallas as pl
from jax.experimental.pallas import tpu as pltpu
from jax.sharding import PartitionSpec as P

D = 4096
TOKENS = 8192
BLOCK = 512
HALF = 256
PART = 128

damping = 0.3
epsilon = 1e-06
divisor = 2.0

MESH = pl.DeviceIdType.MESH
F32 = jnp.float32
BF16 = jnp.bfloat16


class Ids:
    def __init__(self):
        self.next = 0

    def take(self, n):
        first = self.next
        self.next += n
        return first


IDS = Ids()
Z_ID = IDS.take(6)
X_ID = [[IDS.take(4) for _ in range(2)] for _ in range(2)]
D_ID = [[IDS.take(1) for _ in range(2)] for _ in range(2)]
Y1_ID = [[IDS.take(2) for _ in range(2)] for _ in range(2)]
Y2_ID = [[IDS.take(1) for _ in range(2)] for _ in range(2)]
ROW_ID = [IDS.take(8) for _ in range(2)]
LOW_ID = [IDS.take(1) for _ in range(2)]
COL_ID = [[IDS.take(5) for _ in range(2)] for _ in range(2)]
SQ_ID = [IDS.take(5) for _ in range(2)]
OUT_ID = IDS.take(1)
SUM_ID = IDS.take(1)
TOTAL_ID = IDS.take(1)
N_ID = IDS.next

(TO_X, TO_Z, TO_SIBLING, TO_Y1, TO_Y2, TO_ROWS, TO_LOW, TO_PASS, TO_COLS, TO_SQ, TO_SQ_PASS,
 TO_OUT, TO_SUM, TO_TOTAL, N_TO) = range(15)


class Line:
    arrivals = [(3, 0), (3, 1), (1, 1), (1, 0), (2, 0), (2, 1)]
    number = [0, 2, 1, 2, 3, 3]

    def __init__(self, send, wait, base, kind, ref, plus, minus, late):
        self.send, self.wait, self.base, self.kind, self.ref = send, wait, base, kind, ref
        self.plus, self.minus, self.late = plus, minus, late

    def put(self, k, where, to):
        r = self.ref(*where)
        self.send(self.base + self.number[k], r, r, to, self.kind)

    def arrived(self, k):
        pass

    def take(self, k):
        self.wait(self.base + self.number[k], self.ref(*self.arrivals[k]))
        self.arrived(k)

    def start(self):
        self.put(0, (0, 0), self.plus)
        self.put(2, (0, 1), self.minus)
        self.put(1, (0, 1), self.plus)
        self.put(3, (0, 0), self.minus)

    def near(self):
        self.take(0)
        self.put(4, (3, 0), self.plus)
        self.take(2)
        self.put(5, (1, 1), self.minus)

    def rest(self):
        self.wait(self.base + 2, self.late)

    def finish(self):
        self.wait(self.base + 3, self.late)


class Passed(Line):
    number = [0, 2, 1, 2, 4, 4]

    def __init__(self, send, wait, base, kind, ref, plus, minus, late, sibling, pass_kind, mirrored):
        super().__init__(send, wait, base, kind, ref, plus, minus, late)
        self.sibling, self.pass_kind, self.mirrored = sibling, pass_kind, mirrored

    def pass_on(self, where):
        r = self.ref(*where)
        self.send(self.base + 3, r, r, self.sibling, self.pass_kind)

    def arrived(self, k):
        self.pass_on(self.arrivals[k])

    def start(self):
        super().start()
        self.pass_on((0, 0))
        self.pass_on((0, 1))

    def rest(self):
        self.wait(self.base + 2, self.late)
        self.arrived(1)
        self.arrived(3)

    def finish(self):
        self.wait(self.base + 4, self.late)
        self.arrived(4)
        self.arrived(5)

    def passed(self):
        self.wait(self.base + 3, self.mirrored)


class Plane(Line):
    arrivals = Line.arrivals + [None, (3, None, 1), (1, None, 1), (2, 0, 1), (2, 1, 1)]
    number = [0, 2, 1, 2, 3, 4, 5, 6, 6, 6, 6]

    def __init__(self, send, wait, base, kind, ref, plus, minus, late, across, needed):
        super().__init__(send, wait, base, kind, ref, plus, minus, late)
        self.across, self.needed = across, needed

    def cross(self):
        r = self.ref(0, 1 - self.needed, 0)
        self.send(self.base + 5, r, r, self.across, self.kind)

    def start(self):
        r = self.ref(0, self.needed, 0)
        self.send(self.base + 7, r, r, self.across, self.kind)
        super().start()

    def take_needed(self):
        self.wait(self.base + 5, self.ref(0, self.needed, 1))

    def other(self):
        self.wait(self.base + 7, self.ref(0, 1 - self.needed, 1))
        self.put(7, (0, None, 1), self.plus)
        self.put(8, (0, None, 1), self.minus)

    def far(self):
        self.wait(self.base + 2, self.ref(3, None))
        self.take(4)
        self.put(9, (2, 0, 0), self.across)
        self.take(5)
        self.put(10, (2, 1, 0), self.across)

    def last(self):
        self.wait(self.base + 6, self.late)


def kernel(
    act_ref, grad_ref, out_ref,
    xall, give, gram_part, drecv, y1s, y1r, y2s, y2r, scaled,
    rowbuf, colbuf, sqcol, sq, low_out, low_in, obuf, csend, crecv, totbuf,
    ssem, rsem, lsem,
):
    tok, blk = lax.axis_index("tok"), lax.axis_index("blk")
    c, y, zl = tok % 2, (tok // 2) % 4, tok // 8
    x, zh = blk // 2, blk % 2

    def tok_of(zl_, y_, c_):
        return zl_ * 8 + y_ * 2 + c_

    def blk_of(x_, zh_):
        return x_ * 2 + zh_

    x_plus = (tok, blk_of((x + 1) % 4, zh))
    x_minus = (tok, blk_of((x + 3) % 4, zh))
    zh_mate = (tok, blk_of(x, 1 - zh))
    y_plus = (tok_of(zl, (y + 1) % 4, c), blk)
    y_minus = (tok_of(zl, (y + 3) % 4, c), blk)
    zl_mate = (tok_of(1 - zl, y, c), blk)
    z_cross = (tok_of(1 - zl, y, c), blk_of(x, 1 - zh))
    sibling = (tok_of(zl, y, 1 - c), blk)

    def place(to):
        return {"tok": to[0], "blk": to[1]}

    def row_of(s, y_):
        return ((y_ + s) % 2) * 2 + y_ // 2

    def keep(s, step):
        return row_of(s, (y + step) % 4)

    zh_of = (zh, 1 - zh)

    def out_tok(e, s):
        return 2 * (2 * keep(s, 0) + zh_of[e]) + c

    source_y = ((tok // 4) % 2) * 2 + (tok // 8 + blk // 4) % 2
    home = source_y == y

    def loads(src, dst, first):
        out = []
        for s in range(2):
            for k in range(2):
                cols = pl.ds(HALF * k + PART * s, PART)
                out.append(
                    pltpu.make_async_copy(
                        src.at[:, cols], dst(s).at[:, pl.ds(PART * k, PART)],
                        lsem.at[first + 2 * s + k],
                    )
                )
        return out

    def own_block(s):
        return xall.at[0, x, s]

    def give_block(s):
        return give.at[s]

    def all_loads(own_ref, give_ref):
        return loads(own_ref, own_block, 0) + loads(give_ref, give_block, 4)

    @pl.when(zl == 0)
    def _():
        for copy in all_loads(act_ref, grad_ref):
            copy.start()

    @pl.when(zl == 1)
    def _():
        for copy in all_loads(grad_ref, act_ref):
            copy.start()

    barrier = pltpu.get_barrier_semaphore()

    def greet(to):
        pl.semaphore_signal(barrier, inc=1, device_id=place(to), device_id_type=MESH)

    def greet_tok(j, carry):
        greet(((tok + j) % 16, blk))
        return carry

    def greet_blk(j, carry):
        greet((tok, (blk + j) % 8))
        return carry

    lax.fori_loop(1, 16, greet_tok, 0)
    lax.fori_loop(1, 8, greet_blk, 0)
    greet(z_cross)

    def greet_source(j, carry):
        to = (tok_of(j % 2, source_y, c), j // 2)

        @pl.when(jnp.logical_not((to[0] == tok) & (to[1] == blk)))
        def _():
            greet(to)

        return carry

    lax.fori_loop(0, 16, greet_source, 0)
    for copy in all_loads(act_ref, grad_ref):
        copy.wait()
    pl.semaphore_wait(barrier, 15 + 7 + 1 + 16 - home.astype(jnp.int32))

    def remote(k, src, dst, to, kind):
        return pltpu.make_async_remote_copy(
            src_ref=src, dst_ref=dst, send_sem=ssem.at[kind], recv_sem=rsem.at[k],
            device_id=place(to), device_id_type=MESH,
        )

    def send(k, src, dst, to, kind):
        remote(k, src, dst, to, kind).start()

    def wait(k, dst):
        remote(k, dst, dst, sibling, 0).wait_recv()

    def left(kind, src):
        remote(0, src, src, sibling, kind).wait_send()

    token_half = (pl.ds(0, HALF), pl.ds(HALF, HALF))

    def x_line(s, t):
        def ref(step, half):
            return xall.at[t, (x + step) % 4, s, token_half[half]]

        return Line(
            send, wait, X_ID[s][t], TO_X, ref, x_plus, x_minus, xall.at[t, (x + 2) % 4, s]
        )

    lines = [[x_line(s, t) for t in range(2)] for s in range(2)]

    def z_first(s):
        send(Z_ID + s, give.at[s], xall.at[1, x, s], zl_mate, TO_Z)

    def z_rest(s):
        send(Z_ID + 2 + s, give.at[s], xall.at[1, 4, s], z_cross, TO_Z)
        send(Z_ID + 4 + s, xall.at[0, x, s], xall.at[0, 4, s], zh_mate, TO_Z)

    def z_first_take(s):
        wait(Z_ID + s, xall.at[1, x, s])

    def z_rest_take(s):
        wait(Z_ID + 2 + s, xall.at[1, 4, s])
        wait(Z_ID + 4 + s, xall.at[0, 4, s])

    def column_sums():
        for which, ref in ((zl, own_block), (1 - zl, give_block)):
            for s in range(2):
                values = ref(s)[...].astype(F32)
                total = jnp.sum(values * values, axis=0, keepdims=True)
                for k in range(2):
                    csend[which, :, HALF * k + PART * s : HALF * k + PART * (s + 1)] = total[
                        :, PART * k : PART * (k + 1)
                    ]

    def sum_copy(j):
        return remote(SUM_ID, csend, crecv.at[j], ((tok + j) % 16, blk), TO_SUM)

    def sums_start():
        def step(j, carry):
            sum_copy(j).start()
            return carry

        lax.fori_loop(1, 16, step, 0)

    total_to = [(tok, blk_of((x + j) % 4, zh)) for j in (1, 2, 3)] + [zh_mate]

    def total_copy(j):
        slot = x if j < 3 else 4
        return remote(TOTAL_ID, totbuf.at[x], totbuf.at[slot], total_to[j], TO_TOTAL)

    def totals_start():
        wait(SUM_ID, crecv.at[pl.ds(1, 15)])
        total = csend[...]
        for j in range(1, 16):
            total = total + crecv[j]
        totbuf[x] = total
        for j in range(4):
            total_copy(j).start()

    def totals_finish():
        wait(TOTAL_ID, totbuf.at[pl.ds(0, 4)])

    def gram(s, gs, begin, end):
        def step(i, carry):
            to = (x + 3 + i) % 4
            for g in gs:
                for s2 in range(2):
                    value = None
                    for t in range(2):
                        term = lax.dot_general(
                            xall[t, to, s], xall[t, (x, 4)[g], s2],
                            (((0,), (0,)), ((), ())), preferred_element_type=F32,
                        )
                        value = term if value is None else value + term
                    value = value.astype(BF16)
                    for k in range(2):
                        for k2 in range(2):
                            start = HALF * k2 + PART * s2
                            gram_part[s, g, to, k, :, start : start + PART] = value[
                                PART * k : PART * (k + 1), PART * k2 : PART * (k2 + 1)
                            ]
                d_copy(s, g, to).start()
            return carry

        lax.fori_loop(begin, end, step, 0)

    def d_copy(s, g, to):
        return remote(
            D_ID[s][g], gram_part.at[s, g, to, 1 - c], drecv.at[s, g, to], sibling, TO_SIBLING
        )

    halves = (pl.ds(0, PART // 2), pl.ds(PART // 2, PART // 2))

    def both(s, g, to, half):
        mine = gram_part[s, g, to, c, halves[half]].astype(F32)
        return mine + drecv[s, g, to, halves[half]].astype(F32)

    def reduce_first(s, g):
        y1, far = Y1_ID[s][g], keep(s, 2)
        wait(D_ID[s][g], drecv.at[s, g])
        y1s[s, g, 0] = both(s, g, far, 0).astype(BF16)
        send(y1, y1s.at[s, g, 0], y1r.at[s, g, 0], y_plus, TO_Y1)
        y1s[s, g, 1] = both(s, g, far, 1).astype(BF16)
        send(y1 + 1, y1s.at[s, g, 1], y1r.at[s, g, 1], y_minus, TO_Y1)

    def reduce_own(s, g):
        y2, up, down = Y2_ID[s][g], keep(s, 1), keep(s, 3)
        y2s[s, g, 0] = both(s, g, up, 1).astype(BF16)
        send(y2, y2s.at[s, g, 0], y2r.at[s, g, 0], y_plus, TO_Y2)
        y2s[s, g, 2] = both(s, g, down, 0).astype(BF16)
        send(y2, y2s.at[s, g, 2], y2r.at[s, g, 2], y_minus, TO_Y2)

    def reduce_middle(s, g):
        y1, y2, up, down = Y1_ID[s][g], Y2_ID[s][g], keep(s, 1), keep(s, 3)
        wait(y1, y1r.at[s, g, 0])
        y2s[s, g, 1] = (both(s, g, up, 0) + y1r[s, g, 0].astype(F32)).astype(BF16)
        send(y2, y2s.at[s, g, 1], y2r.at[s, g, 1], y_plus, TO_Y2)
        wait(y1 + 1, y1r.at[s, g, 1])
        y2s[s, g, 3] = (both(s, g, down, 1) + y1r[s, g, 1].astype(F32)).astype(BF16)
        send(y2, y2s.at[s, g, 3], y2r.at[s, g, 3], y_minus, TO_Y2)

    def eye(s, zh_, h):
        shape = (PART, BLOCK)
        r = lax.broadcasted_iota(jnp.int32, shape, 0) + HALF * c + PART * s
        k = lax.broadcasted_iota(jnp.int32, shape, 1)
        return (r + BLOCK * (2 * keep(s, 0) + zh_) == k + BLOCK * (2 * x + h)).astype(F32)

    def inverse(sums):
        return lax.rsqrt(sums / TOKENS + epsilon)

    def lane_block(block):
        return pl.ds(pl.multiple_of(block * BLOCK, BLOCK), BLOCK)

    def normalise(s):
        rows = pl.ds(pl.multiple_of(HALF * c + PART * s, PART), PART)
        inv_row = jnp.broadcast_to(inverse(totbuf[keep(s, 0), zl, :, rows]), (PART, PART))
        inv_row = jnp.concatenate([jnp.transpose(inv_row)] * 4, axis=1)
        for g in (0, 1) if s == 0 else (1, 0):
            wait(Y2_ID[s][g], y2r.at[s, g])
            inv_col = inverse(totbuf[(x, 4)[g], zl])
            low = both(s, g, keep(s, 0), 0) + y2r[s, g, 1].astype(F32) + y2r[s, g, 2].astype(F32)
            high = both(s, g, keep(s, 0), 1) + y2r[s, g, 0].astype(F32) + y2r[s, g, 3].astype(F32)
            total = jnp.concatenate([low, high], axis=0)
            damped = total / TOKENS * inv_row * inv_col + damping * eye(s, zh, zh_of[g])
            value = damped / divisor
            half = value.astype(BF16)
            rowbuf[zh, s, zh_of[g], :, lane_block(x)] = half
            if g == 0:
                scaled[0, s] = value
                colbuf[keep(s, 0), zh, c, s] = half
                cols[s][0].start()
            else:
                rows_of[s].cross()
                low_out[s] = (value - half.astype(F32)).astype(BF16)
        rows_of[s].start()
        send(LOW_ID[s], low_out.at[s], low_in.at[s], zh_mate, TO_LOW)

    def partner(s):
        half = rowbuf[1 - zh, s, zh, :, lane_block(x)]
        colbuf[keep(s, 0), 1 - zh, c, s] = half
        cols[s][1].start()

    def partner_low(s):
        wait(LOW_ID[s], low_in.at[s])
        half = rowbuf[1 - zh, s, zh, :, lane_block(x)].astype(F32)
        scaled[1, s] = half + low_in[s].astype(F32)

    def row_plane(s):
        def ref(step, half, other=0):
            lanes = lane_block((x + step) % 4)
            r = rowbuf.at[zh_of[other], s]
            return r.at[:, :, lanes] if half is None else r.at[half, :, lanes]

        late = rowbuf.at[1 - zh, s, :, :, pl.ds(0, 3 * BLOCK)]
        return Plane(
            send, wait, ROW_ID[s], TO_ROWS, ref, x_plus, x_minus, late, zh_mate, zh
        )

    def col_line(s, e):
        def ref(step, half):
            return colbuf.at[keep(s, step), zh_of[e], c, s, halves[half]]

        late = colbuf.at[0, zh_of[e], c, s]
        return Passed(
            send, wait, COL_ID[s][e], TO_COLS, ref, y_plus, y_minus, late, sibling, TO_PASS,
            colbuf.at[:, zh_of[e], 1 - c, s],
        )

    def sq_line(e):
        def ref(step, half):
            return sqcol.at[keep(half, step), zh_of[e], c, half]

        late = sqcol.at[0, zh_of[e], c]
        return Passed(
            send, wait, SQ_ID[e], TO_SQ, ref, y_plus, y_minus, late, sibling, TO_SQ_PASS,
            sqcol.at[:, zh_of[e], 1 - c],
        )

    rows_of = [row_plane(s) for s in range(2)]
    cols = [[col_line(s, e) for e in range(2)] for s in range(2)]
    sq_cols = [sq_line(e) for e in range(2)]

    def dot(e, p, right, lanes):
        return jnp.dot(
            rowbuf[zh_of[e], :, p].reshape(HALF, D // 2),
            right[:, p, :, :, :, lanes].reshape(D // 2, HALF),
            preferred_element_type=F32,
        )

    def over_lanes(body):
        def step(k, carry):
            body(pl.ds(pl.multiple_of(k * HALF, HALF), HALF))
            return carry

        lax.fori_loop(0, 2, step, 0)

    def square(e):
        def some(lanes):
            sq[e, :, lanes] = dot(e, 0, colbuf, lanes) + dot(e, 1, colbuf, lanes)

        over_lanes(some)
        for s in range(2):
            sqcol[keep(s, 0), zh_of[e], c, s] = sq[e, PART * s : PART * (s + 1)].astype(BF16)
        sq_cols[e].start()

    def combine(e):
        for s in range(2):
            scaled[e, s] = (
                4.0 * eye(s, zh_of[e], zh) - 6.0 * scaled[e, s]
                + 4.0 * sq[e, PART * s : PART * (s + 1)]
            )

    def cube_first():
        for e in range(2):
            def some(lanes):
                sq[e, :, lanes] = dot(e, zh, sqcol, lanes)

            over_lanes(some)

    def cube_second(e):
        def some(lanes):
            value = scaled[e, :, :, lanes].reshape(HALF, HALF) - sq[e, :, lanes]
            obuf[e, :, lanes] = (value - dot(e, 1 - zh, sqcol, lanes)).astype(BF16)

        over_lanes(some)
        for b in range(8):
            me = (out_tok(e, b // 4) == tok) & (blk == b)

            @pl.when(me)
            def _():
                out_ref[zl, :, lane_block(2 * x + zh)] = obuf[e, b * 32 : (b + 1) * 32]

            @pl.when(jnp.logical_not(me))
            def _():
                out_copy(e, b).start()

    def out_copy(e, b):
        return remote(
            OUT_ID, obuf.at[e, pl.ds(b * 32, 32)], out_ref.at[zl, :, lane_block(2 * x + zh)],
            (out_tok(e, b // 4), b), TO_OUT,
        )

    def emit():
        @pl.when(home)
        def _():
            wait(OUT_ID, out_ref.at[:, :, pl.ds(0, 15 * HALF)])
            left(TO_OUT, obuf.at[:, pl.ds(0, 15 * 16)])

        @pl.when(jnp.logical_not(home))
        def _():
            wait(OUT_ID, out_ref)
            left(TO_OUT, obuf)

    def all_left():
        left(TO_X, xall.at[:, pl.ds(0, 3)])
        left(TO_Z, xall.at[0, pl.ds(0, 3)])
        left(TO_SIBLING, gram_part.at[0])
        left(TO_Y1, y1s)
        left(TO_Y2, y2s)
        left(TO_ROWS, rowbuf.at[:, :, :, pl.ds(0, 112)])
        left(TO_LOW, low_out)
        left(TO_PASS, colbuf.at[pl.ds(0, 2)])
        left(TO_COLS, colbuf.at[pl.ds(0, 3), 0])
        left(TO_SQ, sqcol.at[pl.ds(0, 3), 0])
        left(TO_SQ_PASS, sqcol.at[pl.ds(0, 2)])
        left(TO_SUM, crecv.at[pl.ds(1, 15)])
        left(TO_TOTAL, totbuf.at[pl.ds(0, 4)])

    z_first(0)
    lines[0][0].start()
    column_sums()
    sums_start()
    z_first(1)
    z_rest(0)
    z_rest(1)
    lines[0][0].near()
    z_first_take(0)
    lines[0][1].start()
    totals_start()
    lines[0][1].near()
    lines[1][0].start()
    z_first_take(1)
    lines[1][1].start()
    lines[0][0].rest()
    lines[0][0].finish()
    lines[0][1].rest()
    lines[0][1].finish()
    gram(0, (0,), 0, 4)
    reduce_first(0, 0)
    reduce_own(0, 0)
    lines[1][0].near()
    z_rest_take(0)
    z_rest_take(1)
    gram(0, (1,), 0, 4)
    reduce_middle(0, 0)
    reduce_first(0, 1)
    reduce_own(0, 1)
    lines[1][1].near()
    reduce_middle(0, 1)
    totals_finish()
    lines[1][0].rest()
    lines[1][1].rest()
    gram(1, (1, 0), 0, 3)
    normalise(0)
    lines[1][0].finish()
    lines[1][1].finish()
    gram(1, (1, 0), 3, 4)
    reduce_first(1, 1)
    reduce_first(1, 0)
    reduce_own(1, 1)
    reduce_own(1, 0)
    rows_of[0].near()
    reduce_middle(1, 1)
    rows_of[0].take_needed()
    rows_of[0].other()
    reduce_middle(1, 0)
    cols[0][0].near()
    partner(0)
    cols[0][0].rest()
    rows_of[0].far()
    normalise(1)
    cols[0][0].finish()
    cols[0][1].near()
    cols[1][0].near()
    cols[0][1].rest()
    rows_of[1].near()
    rows_of[1].take_needed()
    partner(1)
    cols[0][1].finish()
    cols[1][0].rest()
    rows_of[1].other()
    cols[1][0].finish()
    cols[1][1].near()
    rows_of[1].far()
    cols[1][1].rest()
    cols[1][1].finish()
    for s in range(2):
        for e in range(2):
            cols[s][e].passed()
    square(0)
    rows_of[0].last()
    rows_of[1].last()
    square(1)
    sq_cols[0].near()
    combine(0)
    partner_low(0)
    partner_low(1)
    combine(1)
    sq_cols[1].near()
    sq_cols[0].rest()
    sq_cols[0].finish()
    sq_cols[1].rest()
    sq_cols[0].passed()
    cube_first()
    sq_cols[1].finish()
    sq_cols[1].passed()
    cube_second(0)
    cube_second(1)
    all_left()
    emit()


def body(activations, out_grads):
    hbm = pl.BlockSpec(memory_space=pltpu.HBM)
    vmem = pl.BlockSpec(memory_space=pltpu.VMEM)
    part = (PART, BLOCK)
    half_part = (PART // 2, BLOCK)
    scratch = [
        pltpu.VMEM((2, 5, 2, BLOCK, HALF), BF16),
        pltpu.VMEM((2, BLOCK, HALF), BF16),
        pltpu.VMEM((2, 2, 4, 2, *part), BF16),
        pltpu.VMEM((2, 2, 4, *part), BF16),
        pltpu.VMEM((2, 2, 2, *half_part), BF16),
        pltpu.VMEM((2, 2, 2, *half_part), BF16),
        pltpu.VMEM((2, 2, 4, *half_part), BF16),
        pltpu.VMEM((2, 2, 4, *half_part), BF16),
        pltpu.VMEM((2, 2, *part), F32),
        pltpu.VMEM((2, 2, 2, PART, D // 2), BF16),
        pltpu.VMEM((4, 2, 2, 2, *part), BF16),
        pltpu.VMEM((4, 2, 2, 2, *part), BF16),
        pltpu.VMEM((2, HALF, BLOCK), F32),
        pltpu.VMEM((2, *part), BF16),
        pltpu.VMEM((2, *part), BF16),
        pltpu.VMEM((2, HALF, BLOCK), BF16),
        pltpu.VMEM((2, 1, BLOCK), F32),
        pltpu.VMEM((16, 2, 1, BLOCK), F32),
        pltpu.VMEM((5, 2, 1, BLOCK), F32),
        pltpu.SemaphoreType.DMA((N_TO,)),
        pltpu.SemaphoreType.DMA((N_ID,)),
        pltpu.SemaphoreType.DMA((8,)),
    ]
    out = pl.pallas_call(
        kernel,
        out_shape=pltpu.VMEM((2, 32, D), BF16),
        in_specs=[hbm, hbm],
        out_specs=vmem,
        scratch_shapes=scratch,
        compiler_params=pltpu.CompilerParams(
            collective_id=0, has_side_effects=True, vmem_limit_bytes=60 * 1024 * 1024
        ),
    )(activations, out_grads)
    return out[0].astype(F32), out[1].astype(F32)


def solution(mesh):
    placed = (P("tok", "blk"), P("tok", "blk"))
    return jax.shard_map(
        body,
        mesh=mesh,
        in_specs=placed,
        out_specs=(P(("tok", "blk"), None), P(("tok", "blk"), None)),
        check_vma=False,
    )
```

```python
import jax
import jax.numpy as jnp
from jax import lax
from jax.experimental import pallas as pl
from jax.experimental.pallas import tpu as pltpu
from jax.sharding import PartitionSpec as P

D = 4096
TOKENS = 8192
BLOCK = 512
HALF = 256
PART = 128

damping = 0.3
epsilon = 1e-06
divisor = 2.0

MESH = pl.DeviceIdType.MESH
F32 = jnp.float32
BF16 = jnp.bfloat16


class Ids:
    def __init__(self):
        self.next = 0

    def take(self, n):
        first = self.next
        self.next += n
        return first


IDS = Ids()
Z_ID = IDS.take(6)
X_ID = [[IDS.take(4) for _ in range(2)] for _ in range(2)]
D_ID = [[IDS.take(1) for _ in range(2)] for _ in range(2)]
Y1_ID = [[IDS.take(2) for _ in range(2)] for _ in range(2)]
Y2_ID = [[IDS.take(1) for _ in range(2)] for _ in range(2)]
ROW_ID = [IDS.take(8) for _ in range(2)]
LOW_ID = [IDS.take(1) for _ in range(2)]
COL_ID = [[IDS.take(5) for _ in range(2)] for _ in range(2)]
SQ_ID = [IDS.take(5) for _ in range(2)]
OUT_ID = IDS.take(1)
SUM_ID = IDS.take(1)
TOTAL_ID = IDS.take(1)
N_ID = IDS.next

(TO_X, TO_Z, TO_SIBLING, TO_Y1, TO_Y2, TO_ROWS, TO_LOW, TO_PASS, TO_COLS, TO_SQ, TO_SQ_PASS,
 TO_OUT, TO_SUM, TO_TOTAL, N_TO) = range(15)


class Line:
    arrivals = [(3, 0), (3, 1), (1, 1), (1, 0), (2, 0), (2, 1)]
    number = [0, 2, 1, 2, 3, 3]

    def __init__(self, send, wait, base, kind, ref, plus, minus, late):
        self.send, self.wait, self.base, self.kind, self.ref = send, wait, base, kind, ref
        self.plus, self.minus, self.late = plus, minus, late

    def put(self, k, where, to):
        r = self.ref(*where)
        self.send(self.base + self.number[k], r, r, to, self.kind)

    def arrived(self, k):
        pass

    def take(self, k):
        self.wait(self.base + self.number[k], self.ref(*self.arrivals[k]))
        self.arrived(k)

    def start(self):
        self.put(0, (0, 0), self.plus)
        self.put(2, (0, 1), self.minus)
        self.put(1, (0, 1), self.plus)
        self.put(3, (0, 0), self.minus)

    def near(self):
        self.take(0)
        self.put(4, (3, 0), self.plus)
        self.take(2)
        self.put(5, (1, 1), self.minus)

    def rest(self):
        self.wait(self.base + 2, self.late)

    def finish(self):
        self.wait(self.base + 3, self.late)


class Passed(Line):
    number = [0, 2, 1, 2, 4, 4]

    def __init__(self, send, wait, base, kind, ref, plus, minus, late, sibling, pass_kind, mirrored):
        super().__init__(send, wait, base, kind, ref, plus, minus, late)
        self.sibling, self.pass_kind, self.mirrored = sibling, pass_kind, mirrored

    def pass_on(self, where):
        r = self.ref(*where)
        self.send(self.base + 3, r, r, self.sibling, self.pass_kind)

    def arrived(self, k):
        self.pass_on(self.arrivals[k])

    def start(self):
        super().start()
        self.pass_on((0, 0))
        self.pass_on((0, 1))

    def rest(self):
        self.wait(self.base + 2, self.late)
        self.arrived(1)
        self.arrived(3)

    def finish(self):
        self.wait(self.base + 4, self.late)
        self.arrived(4)
        self.arrived(5)

    def passed(self):
        self.wait(self.base + 3, self.mirrored)


class Plane(Line):
    arrivals = Line.arrivals + [None, (3, None, 1), (1, None, 1), (2, 0, 1), (2, 1, 1)]
    number = [0, 2, 1, 2, 3, 4, 5, 6, 6, 6, 6]

    def __init__(self, send, wait, base, kind, ref, plus, minus, late, across, needed):
        super().__init__(send, wait, base, kind, ref, plus, minus, late)
        self.across, self.needed = across, needed

    def cross(self):
        r = self.ref(0, 1 - self.needed, 0)
        self.send(self.base + 5, r, r, self.across, self.kind)

    def start(self):
        r = self.ref(0, self.needed, 0)
        self.send(self.base + 7, r, r, self.across, self.kind)
        super().start()

    def take_needed(self):
        self.wait(self.base + 5, self.ref(0, self.needed, 1))

    def other(self):
        self.wait(self.base + 7, self.ref(0, 1 - self.needed, 1))
        self.put(7, (0, None, 1), self.plus)
        self.put(8, (0, None, 1), self.minus)

    def far(self):
        self.wait(self.base + 2, self.ref(3, None))
        self.take(4)
        self.put(9, (2, 0, 0), self.across)
        self.take(5)
        self.put(10, (2, 1, 0), self.across)

    def last(self):
        self.wait(self.base + 6, self.late)


def kernel(
    act_ref, grad_ref, out_ref,
    xall, give, gram_part, drecv, y1s, y1r, y2s, y2r, scaled,
    rowbuf, colbuf, sqcol, sq, low_out, low_in, obuf, csend, crecv, totbuf,
    ssem, rsem, lsem,
):
    tok, blk = lax.axis_index("tok"), lax.axis_index("blk")
    c, y, zl = tok % 2, (tok // 2) % 4, tok // 8
    x, zh = blk // 2, blk % 2

    def tok_of(zl_, y_, c_):
        return zl_ * 8 + y_ * 2 + c_

    def blk_of(x_, zh_):
        return x_ * 2 + zh_

    x_plus = (tok, blk_of((x + 1) % 4, zh))
    x_minus = (tok, blk_of((x + 3) % 4, zh))
    zh_mate = (tok, blk_of(x, 1 - zh))
    y_plus = (tok_of(zl, (y + 1) % 4, c), blk)
    y_minus = (tok_of(zl, (y + 3) % 4, c), blk)
    zl_mate = (tok_of(1 - zl, y, c), blk)
    z_cross = (tok_of(1 - zl, y, c), blk_of(x, 1 - zh))
    sibling = (tok_of(zl, y, 1 - c), blk)

    def place(to):
        return {"tok": to[0], "blk": to[1]}

    def row_of(s, y_):
        return ((y_ + s) % 2) * 2 + y_ // 2

    def keep(s, step):
        return row_of(s, (y + step) % 4)

    zh_of = (zh, 1 - zh)

    def out_tok(e, s):
        return 2 * (2 * keep(s, 0) + zh_of[e]) + c

    source_y = ((tok // 4) % 2) * 2 + (tok // 8 + blk // 4) % 2
    home = source_y == y

    def loads(src, dst, first):
        out = []
        for s in range(2):
            for k in range(2):
                cols = pl.ds(HALF * k + PART * s, PART)
                out.append(
                    pltpu.make_async_copy(
                        src.at[:, cols], dst(s).at[:, pl.ds(PART * k, PART)],
                        lsem.at[first + 2 * s + k],
                    )
                )
        return out

    def own_block(s):
        return xall.at[0, x, s]

    def give_block(s):
        return give.at[s]

    def all_loads(own_ref, give_ref):
        return loads(own_ref, own_block, 0) + loads(give_ref, give_block, 4)

    @pl.when(zl == 0)
    def _():
        for copy in all_loads(act_ref, grad_ref):
            copy.start()

    @pl.when(zl == 1)
    def _():
        for copy in all_loads(grad_ref, act_ref):
            copy.start()

    barrier = pltpu.get_barrier_semaphore()

    def greet(to):
        pl.semaphore_signal(barrier, inc=1, device_id=place(to), device_id_type=MESH)

    def greet_tok(j, carry):
        greet(((tok + j) % 16, blk))
        return carry

    def greet_blk(j, carry):
        greet((tok, (blk + j) % 8))
        return carry

    lax.fori_loop(1, 16, greet_tok, 0)
    lax.fori_loop(1, 8, greet_blk, 0)
    greet(z_cross)

    def greet_source(j, carry):
        to = (tok_of(j % 2, source_y, c), j // 2)

        @pl.when(jnp.logical_not((to[0] == tok) & (to[1] == blk)))
        def _():
            greet(to)

        return carry

    lax.fori_loop(0, 16, greet_source, 0)
    for copy in all_loads(act_ref, grad_ref):
        copy.wait()
    pl.semaphore_wait(barrier, 15 + 7 + 1 + 16 - home.astype(jnp.int32))

    def remote(k, src, dst, to, kind):
        return pltpu.make_async_remote_copy(
            src_ref=src, dst_ref=dst, send_sem=ssem.at[kind], recv_sem=rsem.at[k],
            device_id=place(to), device_id_type=MESH,
        )

    def send(k, src, dst, to, kind):
        remote(k, src, dst, to, kind).start()

    def wait(k, dst):
        remote(k, dst, dst, sibling, 0).wait_recv()

    def left(kind, src):
        remote(0, src, src, sibling, kind).wait_send()

    token_half = (pl.ds(0, HALF), pl.ds(HALF, HALF))

    def x_line(s, t):
        def ref(step, half):
            return xall.at[t, (x + step) % 4, s, token_half[half]]

        return Line(
            send, wait, X_ID[s][t], TO_X, ref, x_plus, x_minus, xall.at[t, (x + 2) % 4, s]
        )

    lines = [[x_line(s, t) for t in range(2)] for s in range(2)]

    def z_first(s):
        send(Z_ID + s, give.at[s], xall.at[1, x, s], zl_mate, TO_Z)

    def z_rest(s):
        send(Z_ID + 2 + s, give.at[s], xall.at[1, 4, s], z_cross, TO_Z)
        send(Z_ID + 4 + s, xall.at[0, x, s], xall.at[0, 4, s], zh_mate, TO_Z)

    def z_first_take(s):
        wait(Z_ID + s, xall.at[1, x, s])

    def z_rest_take(s):
        wait(Z_ID + 2 + s, xall.at[1, 4, s])
        wait(Z_ID + 4 + s, xall.at[0, 4, s])

    def column_sums():
        for which, ref in ((zl, own_block), (1 - zl, give_block)):
            for s in range(2):
                values = ref(s)[...].astype(F32)
                total = jnp.sum(values * values, axis=0, keepdims=True)
                for k in range(2):
                    csend[which, :, HALF * k + PART * s : HALF * k + PART * (s + 1)] = total[
                        :, PART * k : PART * (k + 1)
                    ]

    def sum_copy(j):
        return remote(SUM_ID, csend, crecv.at[j], ((tok + j) % 16, blk), TO_SUM)

    def sums_start():
        def step(j, carry):
            sum_copy(j).start()
            return carry

        lax.fori_loop(1, 16, step, 0)

    total_to = [(tok, blk_of((x + j) % 4, zh)) for j in (1, 2, 3)] + [zh_mate]

    def total_copy(j):
        slot = x if j < 3 else 4
        return remote(TOTAL_ID, totbuf.at[x], totbuf.at[slot], total_to[j], TO_TOTAL)

    def totals_start():
        wait(SUM_ID, crecv.at[pl.ds(1, 15)])
        total = csend[...]
        for j in range(1, 16):
            total = total + crecv[j]
        totbuf[x] = total
        for j in range(4):
            total_copy(j).start()

    def totals_finish():
        wait(TOTAL_ID, totbuf.at[pl.ds(0, 4)])

    def gram(s, gs, begin, end):
        def step(i, carry):
            to = (x + 3 + i) % 4
            for g in gs:
                for s2 in range(2):
                    value = None
                    for t in range(2):
                        term = lax.dot_general(
                            xall[t, to, s], xall[t, (x, 4)[g], s2],
                            (((0,), (0,)), ((), ())), preferred_element_type=F32,
                        )
                        value = term if value is None else value + term
                    value = value.astype(BF16)
                    for k in range(2):
                        for k2 in range(2):
                            start = HALF * k2 + PART * s2
                            gram_part[s, g, to, k, :, start : start + PART] = value[
                                PART * k : PART * (k + 1), PART * k2 : PART * (k2 + 1)
                            ]
                d_copy(s, g, to).start()
            return carry

        lax.fori_loop(begin, end, step, 0)

    def d_copy(s, g, to):
        return remote(
            D_ID[s][g], gram_part.at[s, g, to, 1 - c], drecv.at[s, g, to], sibling, TO_SIBLING
        )

    halves = (pl.ds(0, PART // 2), pl.ds(PART // 2, PART // 2))

    def both(s, g, to, half):
        mine = gram_part[s, g, to, c, halves[half]].astype(F32)
        return mine + drecv[s, g, to, halves[half]].astype(F32)

    def reduce_first(s, g):
        y1, far = Y1_ID[s][g], keep(s, 2)
        wait(D_ID[s][g], drecv.at[s, g])
        y1s[s, g, 0] = both(s, g, far, 0).astype(BF16)
        send(y1, y1s.at[s, g, 0], y1r.at[s, g, 0], y_plus, TO_Y1)
        y1s[s, g, 1] = both(s, g, far, 1).astype(BF16)
        send(y1 + 1, y1s.at[s, g, 1], y1r.at[s, g, 1], y_minus, TO_Y1)

    def reduce_own(s, g):
        y2, up, down = Y2_ID[s][g], keep(s, 1), keep(s, 3)
        y2s[s, g, 0] = both(s, g, up, 1).astype(BF16)
        send(y2, y2s.at[s, g, 0], y2r.at[s, g, 0], y_plus, TO_Y2)
        y2s[s, g, 2] = both(s, g, down, 0).astype(BF16)
        send(y2, y2s.at[s, g, 2], y2r.at[s, g, 2], y_minus, TO_Y2)

    def reduce_middle(s, g):
        y1, y2, up, down = Y1_ID[s][g], Y2_ID[s][g], keep(s, 1), keep(s, 3)
        wait(y1, y1r.at[s, g, 0])
        y2s[s, g, 1] = (both(s, g, up, 0) + y1r[s, g, 0].astype(F32)).astype(BF16)
        send(y2, y2s.at[s, g, 1], y2r.at[s, g, 1], y_plus, TO_Y2)
        wait(y1 + 1, y1r.at[s, g, 1])
        y2s[s, g, 3] = (both(s, g, down, 1) + y1r[s, g, 1].astype(F32)).astype(BF16)
        send(y2, y2s.at[s, g, 3], y2r.at[s, g, 3], y_minus, TO_Y2)

    def eye(s, zh_, h):
        shape = (PART, BLOCK)
        r = lax.broadcasted_iota(jnp.int32, shape, 0) + HALF * c + PART * s
        k = lax.broadcasted_iota(jnp.int32, shape, 1)
        return (r + BLOCK * (2 * keep(s, 0) + zh_) == k + BLOCK * (2 * x + h)).astype(F32)

    def inverse(sums):
        return lax.rsqrt(sums / TOKENS + epsilon)

    def lane_block(block):
        return pl.ds(pl.multiple_of(block * BLOCK, BLOCK), BLOCK)

    def normalise(s, g):
        rows = pl.ds(pl.multiple_of(HALF * c + PART * s, PART), PART)
        inv_row = jnp.broadcast_to(inverse(totbuf[keep(s, 0), zl, :, rows]), (PART, PART))
        inv_row = jnp.concatenate([jnp.transpose(inv_row)] * 4, axis=1)
        wait(Y2_ID[s][g], y2r.at[s, g])
        inv_col = inverse(totbuf[(x, 4)[g], zl])
        low = both(s, g, keep(s, 0), 0) + y2r[s, g, 1].astype(F32) + y2r[s, g, 2].astype(F32)
        high = both(s, g, keep(s, 0), 1) + y2r[s, g, 0].astype(F32) + y2r[s, g, 3].astype(F32)
        total = jnp.concatenate([low, high], axis=0)
        damped = total / TOKENS * inv_row * inv_col + damping * eye(s, zh, zh_of[g])
        value = damped / divisor
        half = value.astype(BF16)
        rowbuf[zh, s, zh_of[g], :, lane_block(x)] = half
        if g == 0:
            scaled[0, s] = value
            colbuf[keep(s, 0), zh, c, s] = half
            cols[s][0].start()
        else:
            rows_of[s].cross()
            low_out[s] = (value - half.astype(F32)).astype(BF16)

    def rows_start(s):
        rows_of[s].start()
        send(LOW_ID[s], low_out.at[s], low_in.at[s], zh_mate, TO_LOW)

    def partner(s):
        half = rowbuf[1 - zh, s, zh, :, lane_block(x)]
        colbuf[keep(s, 0), 1 - zh, c, s] = half
        cols[s][1].start()

    def partner_low(s):
        wait(LOW_ID[s], low_in.at[s])
        half = rowbuf[1 - zh, s, zh, :, lane_block(x)].astype(F32)
        scaled[1, s] = half + low_in[s].astype(F32)

    def row_plane(s):
        def ref(step, half, other=0):
            lanes = lane_block((x + step) % 4)
            r = rowbuf.at[zh_of[other], s]
            return r.at[:, :, lanes] if half is None else r.at[half, :, lanes]

        late = rowbuf.at[1 - zh, s, :, :, pl.ds(0, 3 * BLOCK)]
        return Plane(
            send, wait, ROW_ID[s], TO_ROWS, ref, x_plus, x_minus, late, zh_mate, zh
        )

    def col_line(s, e):
        def ref(step, half):
            return colbuf.at[keep(s, step), zh_of[e], c, s, halves[half]]

        late = colbuf.at[0, zh_of[e], c, s]
        return Passed(
            send, wait, COL_ID[s][e], TO_COLS, ref, y_plus, y_minus, late, sibling, TO_PASS,
            colbuf.at[:, zh_of[e], 1 - c, s],
        )

    def sq_line(e):
        def ref(step, half):
            return sqcol.at[keep(half, step), zh_of[e], c, half]

        late = sqcol.at[0, zh_of[e], c]
        return Passed(
            send, wait, SQ_ID[e], TO_SQ, ref, y_plus, y_minus, late, sibling, TO_SQ_PASS,
            sqcol.at[:, zh_of[e], 1 - c],
        )

    rows_of = [row_plane(s) for s in range(2)]
    cols = [[col_line(s, e) for e in range(2)] for s in range(2)]
    sq_cols = [sq_line(e) for e in range(2)]

    def dot(e, p, right, lanes):
        return jnp.dot(
            rowbuf[zh_of[e], :, p].reshape(HALF, D // 2),
            right[:, p, :, :, :, lanes].reshape(D // 2, HALF),
            preferred_element_type=F32,
        )

    def over_lanes(body):
        def step(k, carry):
            body(pl.ds(pl.multiple_of(k * HALF, HALF), HALF))
            return carry

        lax.fori_loop(0, 2, step, 0)

    def square_first():
        def some(lanes):
            sq[0, :, lanes] = dot(0, zh, colbuf, lanes)

        over_lanes(some)

    def square(e):
        def some(lanes):
            if e == 0:
                sq[e, :, lanes] = sq[e, :, lanes] + dot(e, 1 - zh, colbuf, lanes)
            else:
                sq[e, :, lanes] = dot(e, 0, colbuf, lanes) + dot(e, 1, colbuf, lanes)

        over_lanes(some)
        for s in range(2):
            sqcol[keep(s, 0), zh_of[e], c, s] = sq[e, PART * s : PART * (s + 1)].astype(BF16)
        sq_cols[e].start()

    def combine(e):
        for s in range(2):
            scaled[e, s] = (
                4.0 * eye(s, zh_of[e], zh) - 6.0 * scaled[e, s]
                + 4.0 * sq[e, PART * s : PART * (s + 1)]
            )

    def cube_first():
        for e in range(2):
            def some(lanes):
                sq[e, :, lanes] = dot(e, zh, sqcol, lanes)

            over_lanes(some)

    def cube_second(e):
        def some(lanes):
            value = scaled[e, :, :, lanes].reshape(HALF, HALF) - sq[e, :, lanes]
            obuf[e, :, lanes] = (value - dot(e, 1 - zh, sqcol, lanes)).astype(BF16)

        over_lanes(some)
        for b in (0, 4, 2, 6, 1, 5, 3, 7):
            me = (out_tok(e, b // 4) == tok) & (blk == b)

            @pl.when(me)
            def _():
                out_ref[zl, :, lane_block(2 * x + zh)] = obuf[e, b * 32 : (b + 1) * 32]

            @pl.when(jnp.logical_not(me))
            def _():
                out_copy(e, b).start()

    def out_copy(e, b):
        return remote(
            OUT_ID, obuf.at[e, pl.ds(b * 32, 32)], out_ref.at[zl, :, lane_block(2 * x + zh)],
            (out_tok(e, b // 4), b), TO_OUT,
        )

    def emit():
        @pl.when(home)
        def _():
            wait(OUT_ID, out_ref.at[:, :, pl.ds(0, 15 * HALF)])
            left(TO_OUT, obuf.at[:, pl.ds(0, 15 * 16)])

        @pl.when(jnp.logical_not(home))
        def _():
            wait(OUT_ID, out_ref)
            left(TO_OUT, obuf)

    def all_left():
        left(TO_X, xall.at[:, pl.ds(0, 3)])
        left(TO_Z, xall.at[0, pl.ds(0, 3)])
        left(TO_SIBLING, gram_part.at[0])
        left(TO_Y1, y1s)
        left(TO_Y2, y2s)
        left(TO_ROWS, rowbuf.at[:, :, :, pl.ds(0, 112)])
        left(TO_LOW, low_out)
        left(TO_PASS, colbuf.at[pl.ds(0, 2)])
        left(TO_COLS, colbuf.at[pl.ds(0, 3), 0])
        left(TO_SQ, sqcol.at[pl.ds(0, 3), 0])
        left(TO_SQ_PASS, sqcol.at[pl.ds(0, 2)])
        left(TO_SUM, crecv.at[pl.ds(1, 15)])
        left(TO_TOTAL, totbuf.at[pl.ds(0, 4)])

    z_first(0)
    lines[0][0].start()
    column_sums()
    sums_start()
    z_first(1)
    z_rest(0)
    z_rest(1)
    lines[0][0].near()
    z_first_take(0)
    lines[0][1].start()
    totals_start()
    lines[0][1].near()
    lines[1][0].start()
    z_first_take(1)
    lines[1][1].start()
    lines[0][0].rest()
    lines[0][0].finish()
    lines[0][1].rest()
    lines[0][1].finish()
    gram(0, (0,), 0, 4)
    reduce_first(0, 0)
    reduce_own(0, 0)
    lines[1][0].near()
    z_rest_take(0)
    z_rest_take(1)
    reduce_middle(0, 0)
    gram(0, (1,), 0, 4)
    totals_finish()
    reduce_first(0, 1)
    reduce_own(0, 1)
    lines[1][1].near()
    normalise(0, 0)
    reduce_middle(0, 1)
    lines[1][0].rest()
    lines[1][1].rest()
    gram(1, (1, 0), 0, 3)
    cols[0][0].near()
    normalise(0, 1)
    rows_start(0)
    cols[0][0].rest()
    lines[1][0].finish()
    lines[1][1].finish()
    gram(1, (1, 0), 3, 4)
    reduce_first(1, 1)
    reduce_first(1, 0)
    reduce_own(1, 1)
    reduce_own(1, 0)
    reduce_middle(1, 1)
    rows_of[0].near()
    reduce_middle(1, 0)
    rows_of[0].take_needed()
    partner(0)
    rows_of[0].other()
    cols[0][0].finish()
    normalise(1, 1)
    normalise(1, 0)
    rows_start(1)
    cols[0][1].near()
    rows_of[0].far()
    cols[1][0].near()
    cols[0][1].rest()
    rows_of[1].near()
    rows_of[1].take_needed()
    partner(1)
    cols[1][0].rest()
    rows_of[1].other()
    cols[1][1].near()
    cols[0][1].finish()
    cols[1][0].finish()
    rows_of[1].far()
    cols[0][0].passed()
    cols[1][0].passed()
    square_first()
    cols[1][1].rest()
    cols[1][1].finish()
    cols[0][1].passed()
    cols[1][1].passed()
    square(0)
    rows_of[0].last()
    rows_of[1].last()
    square(1)
    sq_cols[0].near()
    combine(0)
    partner_low(0)
    partner_low(1)
    combine(1)
    sq_cols[1].near()
    sq_cols[0].rest()
    sq_cols[0].finish()
    sq_cols[1].rest()
    sq_cols[0].passed()
    cube_first()
    sq_cols[1].finish()
    sq_cols[1].passed()
    cube_second(0)
    cube_second(1)
    all_left()
    emit()


def body(activations, out_grads):
    hbm = pl.BlockSpec(memory_space=pltpu.HBM)
    vmem = pl.BlockSpec(memory_space=pltpu.VMEM)
    part = (PART, BLOCK)
    half_part = (PART // 2, BLOCK)
    scratch = [
        pltpu.VMEM((2, 5, 2, BLOCK, HALF), BF16),
        pltpu.VMEM((2, BLOCK, HALF), BF16),
        pltpu.VMEM((2, 2, 4, 2, *part), BF16),
        pltpu.VMEM((2, 2, 4, *part), BF16),
        pltpu.VMEM((2, 2, 2, *half_part), BF16),
        pltpu.VMEM((2, 2, 2, *half_part), BF16),
        pltpu.VMEM((2, 2, 4, *half_part), BF16),
        pltpu.VMEM((2, 2, 4, *half_part), BF16),
        pltpu.VMEM((2, 2, *part), F32),
        pltpu.VMEM((2, 2, 2, PART, D // 2), BF16),
        pltpu.VMEM((4, 2, 2, 2, *part), BF16),
        pltpu.VMEM((4, 2, 2, 2, *part), BF16),
        pltpu.VMEM((2, HALF, BLOCK), F32),
        pltpu.VMEM((2, *part), BF16),
        pltpu.VMEM((2, *part), BF16),
        pltpu.VMEM((2, HALF, BLOCK), BF16),
        pltpu.VMEM((2, 1, BLOCK), F32),
        pltpu.VMEM((16, 2, 1, BLOCK), F32),
        pltpu.VMEM((5, 2, 1, BLOCK), F32),
        pltpu.SemaphoreType.DMA((N_TO,)),
        pltpu.SemaphoreType.DMA((N_ID,)),
        pltpu.SemaphoreType.DMA((8,)),
    ]
    out = pl.pallas_call(
        kernel,
        out_shape=pltpu.VMEM((2, 32, D), BF16),
        in_specs=[hbm, hbm],
        out_specs=vmem,
        scratch_shapes=scratch,
        compiler_params=pltpu.CompilerParams(
            collective_id=0, has_side_effects=True, vmem_limit_bytes=60 * 1024 * 1024
        ),
    )(activations, out_grads)
    return out[0].astype(F32), out[1].astype(F32)


def solution(mesh):
    placed = (P("tok", "blk"), P("tok", "blk"))
    return jax.shard_map(
        body,
        mesh=mesh,
        in_specs=placed,
        out_specs=(P(("tok", "blk"), None), P(("tok", "blk"), None)),
        check_vma=False,
    )
```

```python
import jax
import jax.numpy as jnp
from jax import lax
from jax.experimental import pallas as pl
from jax.experimental.pallas import tpu as pltpu
from jax.sharding import PartitionSpec as P

D = 4096
TOKENS = 8192
BLOCK = 512
HALF = 256
PART = 128

damping = 0.3
epsilon = 1e-06
divisor = 2.0

MESH = pl.DeviceIdType.MESH
F32 = jnp.float32
BF16 = jnp.bfloat16


class Ids:
    def __init__(self):
        self.next = 0

    def take(self, n):
        first = self.next
        self.next += n
        return first


IDS = Ids()
Z_ID = IDS.take(6)
X_ID = [[IDS.take(4) for _ in range(2)] for _ in range(2)]
D_ID = [[IDS.take(1) for _ in range(2)] for _ in range(2)]
Y1_ID = [[IDS.take(2) for _ in range(2)] for _ in range(2)]
Y2_ID = [[IDS.take(1) for _ in range(2)] for _ in range(2)]
ROW_ID = [IDS.take(8) for _ in range(2)]
LOW_ID = [IDS.take(1) for _ in range(2)]
COL_ID = [[IDS.take(5) for _ in range(2)] for _ in range(2)]
SQ_ID = [IDS.take(5) for _ in range(2)]
OUT_ID = IDS.take(1)
SUM_ID = IDS.take(1)
TOTAL_ID = IDS.take(1)
N_ID = IDS.next

(TO_X, TO_Z, TO_SIBLING, TO_Y1, TO_Y2, TO_ROWS, TO_LOW, TO_PASS, TO_COLS, TO_SQ, TO_SQ_PASS,
 TO_OUT, TO_SUM, TO_TOTAL, N_TO) = range(15)


class Line:
    arrivals = [(3, 0), (3, 1), (1, 1), (1, 0), (2, 0), (2, 1)]
    number = [0, 2, 1, 2, 3, 3]

    def __init__(self, send, wait, base, kind, ref, plus, minus, late):
        self.send, self.wait, self.base, self.kind, self.ref = send, wait, base, kind, ref
        self.plus, self.minus, self.late = plus, minus, late

    def put(self, k, where, to):
        r = self.ref(*where)
        self.send(self.base + self.number[k], r, r, to, self.kind)

    def arrived(self, k):
        pass

    def take(self, k):
        self.wait(self.base + self.number[k], self.ref(*self.arrivals[k]))
        self.arrived(k)

    def start(self):
        self.put(0, (0, 0), self.plus)
        self.put(2, (0, 1), self.minus)
        self.put(1, (0, 1), self.plus)
        self.put(3, (0, 0), self.minus)

    def near(self):
        self.take(0)
        self.put(4, (3, 0), self.plus)
        self.take(2)
        self.put(5, (1, 1), self.minus)

    def rest(self):
        self.wait(self.base + 2, self.late)

    def finish(self):
        self.wait(self.base + 3, self.late)


class Passed(Line):
    number = [0, 2, 1, 2, 4, 4]

    def __init__(self, send, wait, base, kind, ref, plus, minus, late, sibling, pass_kind, mirrored):
        super().__init__(send, wait, base, kind, ref, plus, minus, late)
        self.sibling, self.pass_kind, self.mirrored = sibling, pass_kind, mirrored

    def pass_on(self, where):
        r = self.ref(*where)
        self.send(self.base + 3, r, r, self.sibling, self.pass_kind)

    def arrived(self, k):
        self.pass_on(self.arrivals[k])

    def start(self):
        super().start()
        self.pass_on((0, 0))
        self.pass_on((0, 1))

    def rest(self):
        self.wait(self.base + 2, self.late)
        self.arrived(1)
        self.arrived(3)

    def finish(self):
        self.wait(self.base + 4, self.late)
        self.arrived(4)
        self.arrived(5)

    def passed(self):
        self.wait(self.base + 3, self.mirrored)


class Plane(Line):
    arrivals = Line.arrivals + [None, (3, None, 1), (1, None, 1), (2, 0, 1), (2, 1, 1)]
    number = [0, 2, 1, 2, 3, 4, 5, 6, 6, 6, 6]

    def __init__(self, send, wait, base, kind, ref, plus, minus, late, across, needed):
        super().__init__(send, wait, base, kind, ref, plus, minus, late)
        self.across, self.needed = across, needed

    def cross(self):
        r = self.ref(0, 1 - self.needed, 0)
        self.send(self.base + 5, r, r, self.across, self.kind)

    def start(self):
        r = self.ref(0, self.needed, 0)
        self.send(self.base + 7, r, r, self.across, self.kind)
        super().start()

    def take_needed(self):
        self.wait(self.base + 5, self.ref(0, self.needed, 1))

    def other(self):
        self.wait(self.base + 7, self.ref(0, 1 - self.needed, 1))
        self.put(7, (0, None, 1), self.plus)
        self.put(8, (0, None, 1), self.minus)

    def far(self):
        self.wait(self.base + 2, self.ref(3, None))
        self.take(4)
        self.put(9, (2, 0, 0), self.across)
        self.take(5)
        self.put(10, (2, 1, 0), self.across)

    def last(self):
        self.wait(self.base + 6, self.late)


def kernel(
    act_ref, grad_ref, out_ref,
    xall, give, gram_part, drecv, y1s, y1r, y2s, y2r, scaled,
    rowbuf, colbuf, sqcol, sq, low_out, low_in, obuf, csend, crecv, totbuf,
    ssem, rsem, lsem,
):
    tok, blk = lax.axis_index("tok"), lax.axis_index("blk")
    c, y, zl = tok % 2, (tok // 2) % 4, tok // 8
    x, zh = blk // 2, blk % 2

    def tok_of(zl_, y_, c_):
        return zl_ * 8 + y_ * 2 + c_

    def blk_of(x_, zh_):
        return x_ * 2 + zh_

    x_plus = (tok, blk_of((x + 1) % 4, zh))
    x_minus = (tok, blk_of((x + 3) % 4, zh))
    zh_mate = (tok, blk_of(x, 1 - zh))
    y_plus = (tok_of(zl, (y + 1) % 4, c), blk)
    y_minus = (tok_of(zl, (y + 3) % 4, c), blk)
    zl_mate = (tok_of(1 - zl, y, c), blk)
    z_cross = (tok_of(1 - zl, y, c), blk_of(x, 1 - zh))
    sibling = (tok_of(zl, y, 1 - c), blk)

    def place(to):
        return {"tok": to[0], "blk": to[1]}

    def row_of(s, y_):
        return ((y_ + s) % 2) * 2 + y_ // 2

    def keep(s, step):
        return row_of(s, (y + step) % 4)

    zh_of = (zh, 1 - zh)

    def out_tok(e, s):
        return 2 * (2 * keep(s, 0) + zh_of[e]) + c

    source_y = ((tok // 4) % 2) * 2 + (tok // 8 + blk // 4) % 2
    home = source_y == y

    def loads(src, dst, first):
        out = []
        for s in range(2):
            for k in range(2):
                cols = pl.ds(HALF * k + PART * s, PART)
                out.append(
                    pltpu.make_async_copy(
                        src.at[:, cols], dst(s).at[:, pl.ds(PART * k, PART)],
                        lsem.at[first + 2 * s + k],
                    )
                )
        return out

    def own_block(s):
        return xall.at[0, x, s]

    def give_block(s):
        return give.at[s]

    def all_loads(own_ref, give_ref):
        return loads(own_ref, own_block, 0) + loads(give_ref, give_block, 4)

    @pl.when(zl == 0)
    def _():
        for copy in all_loads(act_ref, grad_ref):
            copy.start()

    @pl.when(zl == 1)
    def _():
        for copy in all_loads(grad_ref, act_ref):
            copy.start()

    barrier = pltpu.get_barrier_semaphore()

    def greet(to):
        pl.semaphore_signal(barrier, inc=1, device_id=place(to), device_id_type=MESH)

    def greet_tok(j, carry):
        greet(((tok + j) % 16, blk))
        return carry

    lax.fori_loop(1, 16, greet_tok, 0)
    for to in (x_plus, x_minus, zh_mate, z_cross):
        greet(to)
    for copy in all_loads(act_ref, grad_ref):
        copy.wait()
    pl.semaphore_wait(barrier, 15 + 4)

    def remote(k, src, dst, to, kind):
        return pltpu.make_async_remote_copy(
            src_ref=src, dst_ref=dst, send_sem=ssem.at[kind], recv_sem=rsem.at[k],
            device_id=place(to), device_id_type=MESH,
        )

    def send(k, src, dst, to, kind):
        remote(k, src, dst, to, kind).start()

    def wait(k, dst):
        remote(k, dst, dst, sibling, 0).wait_recv()

    def left(kind, src):
        remote(0, src, src, sibling, kind).wait_send()

    token_half = (pl.ds(0, HALF), pl.ds(HALF, HALF))

    def x_line(s, t):
        def ref(step, half):
            return xall.at[t, (x + step) % 4, s, token_half[half]]

        return Line(
            send, wait, X_ID[s][t], TO_X, ref, x_plus, x_minus, xall.at[t, (x + 2) % 4, s]
        )

    lines = [[x_line(s, t) for t in range(2)] for s in range(2)]

    def z_first(s):
        send(Z_ID + s, give.at[s], xall.at[1, x, s], zl_mate, TO_Z)

    def z_rest(s):
        send(Z_ID + 2 + s, give.at[s], xall.at[1, 4, s], z_cross, TO_Z)
        send(Z_ID + 4 + s, xall.at[0, x, s], xall.at[0, 4, s], zh_mate, TO_Z)

    def z_first_take(s):
        wait(Z_ID + s, xall.at[1, x, s])

    def z_rest_take(s):
        wait(Z_ID + 2 + s, xall.at[1, 4, s])
        wait(Z_ID + 4 + s, xall.at[0, 4, s])

    def column_sums():
        for which, ref in ((zl, own_block), (1 - zl, give_block)):
            for s in range(2):
                values = ref(s)[...].astype(F32)
                total = jnp.sum(values * values, axis=0, keepdims=True)
                for k in range(2):
                    csend[which, :, HALF * k + PART * s : HALF * k + PART * (s + 1)] = total[
                        :, PART * k : PART * (k + 1)
                    ]

    def sum_copy(j):
        return remote(SUM_ID, csend, crecv.at[j], ((tok + j) % 16, blk), TO_SUM)

    def sums_start():
        def step(j, carry):
            sum_copy(j).start()
            return carry

        lax.fori_loop(1, 16, step, 0)

    total_to = [(tok, blk_of((x + j) % 4, zh)) for j in (1, 2, 3)] + [zh_mate]

    def total_copy(j):
        slot = x if j < 3 else 4
        return remote(TOTAL_ID, totbuf.at[x], totbuf.at[slot], total_to[j], TO_TOTAL)

    def totals_start():
        wait(SUM_ID, crecv.at[pl.ds(1, 15)])
        total = csend[...]
        for j in range(1, 16):
            total = total + crecv[j]
        totbuf[x] = total
        for j in range(4):
            total_copy(j).start()

    def totals_finish():
        wait(TOTAL_ID, totbuf.at[pl.ds(0, 4)])

    def gram(s, gs, begin, end):
        def step(i, carry):
            to = (x + 3 + i) % 4
            for g in gs:
                for s2 in range(2):
                    value = None
                    for t in range(2):
                        term = lax.dot_general(
                            xall[t, to, s], xall[t, (x, 4)[g], s2],
                            (((0,), (0,)), ((), ())), preferred_element_type=F32,
                        )
                        value = term if value is None else value + term
                    value = value.astype(BF16)
                    for k in range(2):
                        for k2 in range(2):
                            start = HALF * k2 + PART * s2
                            gram_part[s, g, to, k, :, start : start + PART] = value[
                                PART * k : PART * (k + 1), PART * k2 : PART * (k2 + 1)
                            ]
                d_copy(s, g, to).start()
            return carry

        lax.fori_loop(begin, end, step, 0)

    def d_copy(s, g, to):
        return remote(
            D_ID[s][g], gram_part.at[s, g, to, 1 - c], drecv.at[s, g, to], sibling, TO_SIBLING
        )

    halves = (pl.ds(0, PART // 2), pl.ds(PART // 2, PART // 2))

    def both(s, g, to, half):
        mine = gram_part[s, g, to, c, halves[half]].astype(F32)
        return mine + drecv[s, g, to, halves[half]].astype(F32)

    def reduce_first(s, g):
        y1, far = Y1_ID[s][g], keep(s, 2)
        wait(D_ID[s][g], drecv.at[s, g])
        y1s[s, g, 0] = both(s, g, far, 0).astype(BF16)
        send(y1, y1s.at[s, g, 0], y1r.at[s, g, 0], y_plus, TO_Y1)
        y1s[s, g, 1] = both(s, g, far, 1).astype(BF16)
        send(y1 + 1, y1s.at[s, g, 1], y1r.at[s, g, 1], y_minus, TO_Y1)

    def reduce_own(s, g):
        y2, up, down = Y2_ID[s][g], keep(s, 1), keep(s, 3)
        y2s[s, g, 0] = both(s, g, up, 1).astype(BF16)
        send(y2, y2s.at[s, g, 0], y2r.at[s, g, 0], y_plus, TO_Y2)
        y2s[s, g, 2] = both(s, g, down, 0).astype(BF16)
        send(y2, y2s.at[s, g, 2], y2r.at[s, g, 2], y_minus, TO_Y2)

    def reduce_middle(s, g):
        y1, y2, up, down = Y1_ID[s][g], Y2_ID[s][g], keep(s, 1), keep(s, 3)
        wait(y1, y1r.at[s, g, 0])
        y2s[s, g, 1] = (both(s, g, up, 0) + y1r[s, g, 0].astype(F32)).astype(BF16)
        send(y2, y2s.at[s, g, 1], y2r.at[s, g, 1], y_plus, TO_Y2)
        wait(y1 + 1, y1r.at[s, g, 1])
        y2s[s, g, 3] = (both(s, g, down, 1) + y1r[s, g, 1].astype(F32)).astype(BF16)
        send(y2, y2s.at[s, g, 3], y2r.at[s, g, 3], y_minus, TO_Y2)

    def eye(s, zh_, h):
        shape = (PART, BLOCK)
        r = lax.broadcasted_iota(jnp.int32, shape, 0) + HALF * c + PART * s
        k = lax.broadcasted_iota(jnp.int32, shape, 1)
        return (r + BLOCK * (2 * keep(s, 0) + zh_) == k + BLOCK * (2 * x + h)).astype(F32)

    def inverse(sums):
        return lax.rsqrt(sums / TOKENS + epsilon)

    def lane_block(block):
        return pl.ds(pl.multiple_of(block * BLOCK, BLOCK), BLOCK)

    def normalise(s):
        rows = pl.ds(pl.multiple_of(HALF * c + PART * s, PART), PART)
        inv_row = jnp.broadcast_to(inverse(totbuf[keep(s, 0), zl, :, rows]), (PART, PART))
        inv_row = jnp.concatenate([jnp.transpose(inv_row)] * 4, axis=1)
        for g in (0, 1) if s == 0 else (1, 0):
            wait(Y2_ID[s][g], y2r.at[s, g])
            inv_col = inverse(totbuf[(x, 4)[g], zl])
            low = both(s, g, keep(s, 0), 0) + y2r[s, g, 1].astype(F32) + y2r[s, g, 2].astype(F32)
            high = both(s, g, keep(s, 0), 1) + y2r[s, g, 0].astype(F32) + y2r[s, g, 3].astype(F32)
            total = jnp.concatenate([low, high], axis=0)
            damped = total / TOKENS * inv_row * inv_col + damping * eye(s, zh, zh_of[g])
            value = damped / divisor
            half = value.astype(BF16)
            rowbuf[zh, s, zh_of[g], :, lane_block(x)] = half
            if g == 0:
                scaled[0, s] = value
                colbuf[keep(s, 0), zh, c, s] = half
                cols[s][0].start()
            else:
                rows_of[s].cross()
                low_out[s] = (value - half.astype(F32)).astype(BF16)
        rows_of[s].start()
        send(LOW_ID[s], low_out.at[s], low_in.at[s], zh_mate, TO_LOW)

    def partner(s):
        half = rowbuf[1 - zh, s, zh, :, lane_block(x)]
        colbuf[keep(s, 0), 1 - zh, c, s] = half
        cols[s][1].start()

    def partner_low(s):
        wait(LOW_ID[s], low_in.at[s])
        half = rowbuf[1 - zh, s, zh, :, lane_block(x)].astype(F32)
        scaled[1, s] = half + low_in[s].astype(F32)

    def row_plane(s):
        def ref(step, half, other=0):
            lanes = lane_block((x + step) % 4)
            r = rowbuf.at[zh_of[other], s]
            return r.at[:, :, lanes] if half is None else r.at[half, :, lanes]

        late = rowbuf.at[1 - zh, s, :, :, pl.ds(0, 3 * BLOCK)]
        return Plane(
            send, wait, ROW_ID[s], TO_ROWS, ref, x_plus, x_minus, late, zh_mate, zh
        )

    def col_line(s, e):
        def ref(step, half):
            return colbuf.at[keep(s, step), zh_of[e], c, s, halves[half]]

        late = colbuf.at[0, zh_of[e], c, s]
        return Passed(
            send, wait, COL_ID[s][e], TO_COLS, ref, y_plus, y_minus, late, sibling, TO_PASS,
            colbuf.at[:, zh_of[e], 1 - c, s],
        )

    def sq_line(e):
        def ref(step, half):
            return sqcol.at[keep(half, step), zh_of[e], c, half]

        late = sqcol.at[0, zh_of[e], c]
        return Passed(
            send, wait, SQ_ID[e], TO_SQ, ref, y_plus, y_minus, late, sibling, TO_SQ_PASS,
            sqcol.at[:, zh_of[e], 1 - c],
        )

    rows_of = [row_plane(s) for s in range(2)]
    cols = [[col_line(s, e) for e in range(2)] for s in range(2)]
    sq_cols = [sq_line(e) for e in range(2)]

    def dot(e, p, right, lanes):
        return jnp.dot(
            rowbuf[zh_of[e], :, p].reshape(HALF, D // 2),
            right[:, p, :, :, :, lanes].reshape(D // 2, HALF),
            preferred_element_type=F32,
        )

    def over_lanes(body):
        def step(k, carry):
            body(pl.ds(pl.multiple_of(k * HALF, HALF), HALF))
            return carry

        lax.fori_loop(0, 2, step, 0)

    def square_first():
        def some(lanes):
            sq[0, :, lanes] = dot(0, zh, colbuf, lanes)

        over_lanes(some)

    def square(e):
        def some(lanes):
            if e == 0:
                sq[e, :, lanes] = sq[e, :, lanes] + dot(e, 1 - zh, colbuf, lanes)
            else:
                sq[e, :, lanes] = dot(e, 0, colbuf, lanes) + dot(e, 1, colbuf, lanes)

        over_lanes(some)
        for s in range(2):
            sqcol[keep(s, 0), zh_of[e], c, s] = sq[e, PART * s : PART * (s + 1)].astype(BF16)
        sq_cols[e].start()

    def combine(e):
        for s in range(2):
            scaled[e, s] = (
                4.0 * eye(s, zh_of[e], zh) - 6.0 * scaled[e, s]
                + 4.0 * sq[e, PART * s : PART * (s + 1)]
            )

    def cube_first():
        for e in range(2):
            def some(lanes):
                sq[e, :, lanes] = dot(e, zh, sqcol, lanes)

            over_lanes(some)

    def cube_second(e):
        def some(lanes):
            value = scaled[e, :, :, lanes].reshape(HALF, HALF) - sq[e, :, lanes]
            obuf[e, :, lanes] = (value - dot(e, 1 - zh, sqcol, lanes)).astype(BF16)

        over_lanes(some)
        for b in (0, 4, 2, 6, 1, 5, 3, 7):
            me = (out_tok(e, b // 4) == tok) & (blk == b)

            @pl.when(me)
            def _():
                out_ref[zl, :, lane_block(2 * x + zh)] = obuf[e, b * 32 : (b + 1) * 32]

            @pl.when(jnp.logical_not(me))
            def _():
                out_copy(e, b).start()

    def out_copy(e, b):
        return remote(
            OUT_ID, obuf.at[e, pl.ds(b * 32, 32)], out_ref.at[zl, :, lane_block(2 * x + zh)],
            (out_tok(e, b // 4), b), TO_OUT,
        )

    def emit():
        @pl.when(home)
        def _():
            wait(OUT_ID, out_ref.at[:, :, pl.ds(0, 15 * HALF)])
            left(TO_OUT, obuf.at[:, pl.ds(0, 15 * 16)])

        @pl.when(jnp.logical_not(home))
        def _():
            wait(OUT_ID, out_ref)
            left(TO_OUT, obuf)

    def all_left():
        left(TO_X, xall.at[:, pl.ds(0, 3)])
        left(TO_Z, xall.at[0, pl.ds(0, 3)])
        left(TO_SIBLING, gram_part.at[0])
        left(TO_Y1, y1s)
        left(TO_Y2, y2s)
        left(TO_ROWS, rowbuf.at[:, :, :, pl.ds(0, 112)])
        left(TO_LOW, low_out)
        left(TO_PASS, colbuf.at[pl.ds(0, 2)])
        left(TO_COLS, colbuf.at[pl.ds(0, 3), 0])
        left(TO_SQ, sqcol.at[pl.ds(0, 3), 0])
        left(TO_SQ_PASS, sqcol.at[pl.ds(0, 2)])
        left(TO_SUM, crecv.at[pl.ds(1, 15)])
        left(TO_TOTAL, totbuf.at[pl.ds(0, 4)])

    z_first(0)
    lines[0][0].start()
    column_sums()
    sums_start()
    z_first(1)
    z_rest(0)
    z_rest(1)
    lines[0][0].near()
    z_first_take(0)
    lines[0][1].start()
    totals_start()
    lines[0][1].near()
    lines[1][0].start()
    z_first_take(1)
    lines[1][1].start()
    lines[0][0].rest()
    lines[0][0].finish()
    lines[0][1].rest()
    lines[0][1].finish()
    gram(0, (0,), 0, 4)
    reduce_first(0, 0)
    reduce_own(0, 0)
    lines[1][0].near()
    z_rest_take(0)
    z_rest_take(1)
    gram(0, (1,), 0, 4)
    reduce_middle(0, 0)
    reduce_first(0, 1)
    reduce_own(0, 1)
    lines[1][1].near()
    reduce_middle(0, 1)
    totals_finish()
    lines[1][0].rest()
    lines[1][1].rest()
    gram(1, (1, 0), 0, 3)
    normalise(0)
    lines[1][0].finish()
    lines[1][1].finish()
    gram(1, (1, 0), 3, 4)
    reduce_first(1, 1)
    reduce_first(1, 0)
    reduce_own(1, 1)
    reduce_own(1, 0)
    reduce_middle(1, 1)
    rows_of[0].near()
    reduce_middle(1, 0)
    rows_of[0].take_needed()
    partner(0)
    cols[0][0].near()
    rows_of[0].other()
    cols[0][0].rest()
    normalise(1)
    cols[0][1].near()
    rows_of[0].far()
    cols[1][0].near()
    cols[0][0].finish()
    cols[0][1].rest()
    rows_of[1].near()
    rows_of[1].take_needed()
    partner(1)
    cols[1][0].rest()
    rows_of[1].other()
    cols[1][1].near()
    cols[0][1].finish()
    cols[1][0].finish()
    rows_of[1].far()
    cols[0][0].passed()
    cols[1][0].passed()
    square_first()
    cols[1][1].rest()
    cols[1][1].finish()
    cols[0][1].passed()
    cols[1][1].passed()
    square(0)
    rows_of[0].last()
    rows_of[1].last()
    square(1)
    sq_cols[0].near()
    combine(0)
    partner_low(0)
    partner_low(1)
    combine(1)
    sq_cols[1].near()
    sq_cols[0].rest()
    sq_cols[0].finish()
    sq_cols[1].rest()
    sq_cols[0].passed()
    cube_first()
    sq_cols[1].finish()
    sq_cols[1].passed()
    cube_second(0)
    cube_second(1)
    all_left()
    emit()


def body(activations, out_grads):
    hbm = pl.BlockSpec(memory_space=pltpu.HBM)
    vmem = pl.BlockSpec(memory_space=pltpu.VMEM)
    part = (PART, BLOCK)
    half_part = (PART // 2, BLOCK)
    scratch = [
        pltpu.VMEM((2, 5, 2, BLOCK, HALF), BF16),
        pltpu.VMEM((2, BLOCK, HALF), BF16),
        pltpu.VMEM((2, 2, 4, 2, *part), BF16),
        pltpu.VMEM((2, 2, 4, *part), BF16),
        pltpu.VMEM((2, 2, 2, *half_part), BF16),
        pltpu.VMEM((2, 2, 2, *half_part), BF16),
        pltpu.VMEM((2, 2, 4, *half_part), BF16),
        pltpu.VMEM((2, 2, 4, *half_part), BF16),
        pltpu.VMEM((2, 2, *part), F32),
        pltpu.VMEM((2, 2, 2, PART, D // 2), BF16),
        pltpu.VMEM((4, 2, 2, 2, *part), BF16),
        pltpu.VMEM((4, 2, 2, 2, *part), BF16),
        pltpu.VMEM((2, HALF, BLOCK), F32),
        pltpu.VMEM((2, *part), BF16),
        pltpu.VMEM((2, *part), BF16),
        pltpu.VMEM((2, HALF, BLOCK), BF16),
        pltpu.VMEM((2, 1, BLOCK), F32),
        pltpu.VMEM((16, 2, 1, BLOCK), F32),
        pltpu.VMEM((5, 2, 1, BLOCK), F32),
        pltpu.SemaphoreType.DMA((N_TO,)),
        pltpu.SemaphoreType.DMA((N_ID,)),
        pltpu.SemaphoreType.DMA((8,)),
    ]
    out = pl.pallas_call(
        kernel,
        out_shape=pltpu.VMEM((2, 32, D), BF16),
        in_specs=[hbm, hbm],
        out_specs=vmem,
        scratch_shapes=scratch,
        compiler_params=pltpu.CompilerParams(
            collective_id=0, has_side_effects=True, vmem_limit_bytes=60 * 1024 * 1024
        ),
    )(activations, out_grads)
    return out[0].astype(F32), out[1].astype(F32)


def solution(mesh):
    placed = (P("tok", "blk"), P("tok", "blk"))
    return jax.shard_map(
        body,
        mesh=mesh,
        in_specs=placed,
        out_specs=(P(("tok", "blk"), None), P(("tok", "blk"), None)),
        check_vma=False,
    )
```

```python
import jax
import jax.numpy as jnp
from jax import lax
from jax.experimental import pallas as pl
from jax.experimental.pallas import tpu as pltpu
from jax.sharding import PartitionSpec as P

D = 4096
TOKENS = 8192
BLOCK = 512
HALF = 256
PART = 128

damping = 0.3
epsilon = 1e-06
divisor = 2.0

MESH = pl.DeviceIdType.MESH
F32 = jnp.float32
BF16 = jnp.bfloat16


class Ids:
    def __init__(self):
        self.next = 0

    def take(self, n):
        first = self.next
        self.next += n
        return first


IDS = Ids()
Z_ID = IDS.take(6)
X_ID = [[IDS.take(4) for _ in range(2)] for _ in range(2)]
D_ID = [[IDS.take(1) for _ in range(2)] for _ in range(2)]
Y1_ID = [[IDS.take(2) for _ in range(2)] for _ in range(2)]
Y2_ID = [[IDS.take(1) for _ in range(2)] for _ in range(2)]
ROW_ID = [IDS.take(8) for _ in range(2)]
LOW_ID = [IDS.take(1) for _ in range(2)]
COL_ID = [[IDS.take(5) for _ in range(2)] for _ in range(2)]
SQ_ID = [IDS.take(5) for _ in range(2)]
OUT_ID = IDS.take(1)
SUM_ID = IDS.take(1)
TOTAL_ID = IDS.take(1)
N_ID = IDS.next

(TO_X, TO_Z, TO_SIBLING, TO_Y1, TO_Y2, TO_ROWS, TO_LOW, TO_PASS, TO_COLS, TO_SQ, TO_SQ_PASS,
 TO_OUT, TO_SUM, TO_TOTAL, N_TO) = range(15)


class Line:
    arrivals = [(3, 0), (3, 1), (1, 1), (1, 0), (2, 0), (2, 1)]
    number = [0, 2, 1, 2, 3, 3]

    def __init__(self, send, wait, base, kind, ref, plus, minus, late):
        self.send, self.wait, self.base, self.kind, self.ref = send, wait, base, kind, ref
        self.plus, self.minus, self.late = plus, minus, late

    def put(self, k, where, to):
        r = self.ref(*where)
        self.send(self.base + self.number[k], r, r, to, self.kind)

    def arrived(self, k):
        pass

    def take(self, k):
        self.wait(self.base + self.number[k], self.ref(*self.arrivals[k]))
        self.arrived(k)

    def start(self):
        self.put(0, (0, 0), self.plus)
        self.put(2, (0, 1), self.minus)
        self.put(1, (0, 1), self.plus)
        self.put(3, (0, 0), self.minus)

    def near(self):
        self.take(0)
        self.put(4, (3, 0), self.plus)
        self.take(2)
        self.put(5, (1, 1), self.minus)

    def rest(self):
        self.wait(self.base + 2, self.late)

    def finish(self):
        self.wait(self.base + 3, self.late)


class Passed(Line):
    number = [0, 2, 1, 2, 4, 4]

    def __init__(self, send, wait, base, kind, ref, plus, minus, late, sibling, pass_kind, mirrored):
        super().__init__(send, wait, base, kind, ref, plus, minus, late)
        self.sibling, self.pass_kind, self.mirrored = sibling, pass_kind, mirrored

    def pass_on(self, where):
        r = self.ref(*where)
        self.send(self.base + 3, r, r, self.sibling, self.pass_kind)

    def arrived(self, k):
        self.pass_on(self.arrivals[k])

    def start(self):
        super().start()
        self.pass_on((0, 0))
        self.pass_on((0, 1))

    def start_direct(self, far):
        self.start()
        self.put(4, (0, 0), far)
        self.put(5, (0, 1), far)

    def near_direct(self):
        self.take(0)
        self.take(2)

    def rest(self):
        self.wait(self.base + 2, self.late)
        self.arrived(1)
        self.arrived(3)

    def finish(self):
        self.wait(self.base + 4, self.late)
        self.arrived(4)
        self.arrived(5)

    def passed(self):
        self.wait(self.base + 3, self.mirrored)


class Plane(Line):
    arrivals = Line.arrivals + [None, (3, None, 1), (1, None, 1), (2, 0, 1), (2, 1, 1)]
    number = [0, 2, 1, 2, 3, 4, 5, 6, 6, 6, 6]

    def __init__(self, send, wait, base, kind, ref, plus, minus, late, across):
        super().__init__(send, wait, base, kind, ref, plus, minus, late)
        self.across = across

    def cross(self, half):
        r = self.ref(0, half, 0)
        self.send(self.base + (7, 5)[half], r, r, self.across, self.kind)

    def start_half(self, half):
        if half == 0:
            self.put(0, (0, 0), self.plus)
            self.put(3, (0, 0), self.minus)
        else:
            self.put(2, (0, 1), self.minus)
            self.put(1, (0, 1), self.plus)

    def take_needed(self):
        self.wait(self.base + 5, self.ref(0, 1, 1))

    def other(self):
        self.wait(self.base + 7, self.ref(0, 0, 1))
        self.put(7, (0, None, 1), self.plus)
        self.put(8, (0, None, 1), self.minus)

    def near_half(self, half):
        if half == 0:
            self.take(0)
            self.put(4, (3, 0), self.plus)
        else:
            self.take(2)
            self.put(5, (1, 1), self.minus)

    def far(self):
        self.wait(self.base + 2, self.ref(3, None))
        self.take(4)
        self.put(9, (2, 0, 0), self.across)
        self.take(5)
        self.put(10, (2, 1, 0), self.across)

    def last(self):
        self.wait(self.base + 6, self.late)


def kernel(
    act_ref, grad_ref, out_ref,
    xall, give, gram_part, drecv, y1s, y1r, y2s, y2r, scaled,
    rowbuf, colbuf, sqcol, sq, low_out, low_in, obuf, csend, crecv, totbuf,
    ssem, rsem, lsem,
):
    tok, blk = lax.axis_index("tok"), lax.axis_index("blk")
    c, y, zl = tok % 2, (tok // 2) % 4, tok // 8
    x, zh = blk // 2, blk % 2

    def tok_of(zl_, y_, c_):
        return zl_ * 8 + y_ * 2 + c_

    def blk_of(x_, zh_):
        return x_ * 2 + zh_

    x_plus = (tok, blk_of((x + 1) % 4, zh))
    x_minus = (tok, blk_of((x + 3) % 4, zh))
    zh_mate = (tok, blk_of(x, 1 - zh))
    y_plus = (tok_of(zl, (y + 1) % 4, c), blk)
    y_minus = (tok_of(zl, (y + 3) % 4, c), blk)
    y_far = (tok_of(zl, (y + 2) % 4, c), blk)
    zl_mate = (tok_of(1 - zl, y, c), blk)
    z_cross = (tok_of(1 - zl, y, c), blk_of(x, 1 - zh))
    sibling = (tok_of(zl, y, 1 - c), blk)

    def place(to):
        return {"tok": to[0], "blk": to[1]}

    def row_of(s, y_):
        return ((y_ + s) % 2) * 2 + y_ // 2

    def keep(s, step):
        return row_of(s, (y + step) % 4)

    zh_of = (zh, 1 - zh)

    def out_tok(e, s):
        return 2 * (2 * keep(s, 0) + zh_of[e]) + c

    source_y = ((tok // 4) % 2) * 2 + (tok // 8 + blk // 4) % 2
    home = source_y == y

    def loads(src, dst, first):
        out = []
        for s in range(2):
            for k in range(2):
                cols = pl.ds(HALF * k + PART * s, PART)
                out.append(
                    pltpu.make_async_copy(
                        src.at[:, cols], dst(s).at[:, pl.ds(PART * k, PART)],
                        lsem.at[first + 2 * s + k],
                    )
                )
        return out

    def own_block(s):
        return xall.at[0, x, s]

    def give_block(s):
        return give.at[s]

    def all_loads(own_ref, give_ref):
        return loads(own_ref, own_block, 0) + loads(give_ref, give_block, 4)

    @pl.when(zl == 0)
    def _():
        for copy in all_loads(act_ref, grad_ref):
            copy.start()

    @pl.when(zl == 1)
    def _():
        for copy in all_loads(grad_ref, act_ref):
            copy.start()

    barrier = pltpu.get_barrier_semaphore()

    def greet(to):
        pl.semaphore_signal(barrier, inc=1, device_id=place(to), device_id_type=MESH)

    def greet_tok(j, carry):
        greet(((tok + j) % 16, blk))
        return carry

    lax.fori_loop(1, 16, greet_tok, 0)
    for to in (x_plus, x_minus, zh_mate, z_cross):
        greet(to)
    for copy in all_loads(act_ref, grad_ref):
        copy.wait()
    pl.semaphore_wait(barrier, 15 + 4)

    def remote(k, src, dst, to, kind):
        return pltpu.make_async_remote_copy(
            src_ref=src, dst_ref=dst, send_sem=ssem.at[kind], recv_sem=rsem.at[k],
            device_id=place(to), device_id_type=MESH,
        )

    def send(k, src, dst, to, kind):
        remote(k, src, dst, to, kind).start()

    def wait(k, dst):
        remote(k, dst, dst, sibling, 0).wait_recv()

    def left(kind, src):
        remote(0, src, src, sibling, kind).wait_send()

    token_half = (pl.ds(0, HALF), pl.ds(HALF, HALF))

    def x_line(s, t):
        def ref(step, half):
            return xall.at[t, (x + step) % 4, s, token_half[half]]

        return Line(
            send, wait, X_ID[s][t], TO_X, ref, x_plus, x_minus, xall.at[t, (x + 2) % 4, s]
        )

    lines = [[x_line(s, t) for t in range(2)] for s in range(2)]

    def z_first(s):
        send(Z_ID + s, give.at[s], xall.at[1, x, s], zl_mate, TO_Z)

    def z_rest(s):
        send(Z_ID + 2 + s, give.at[s], xall.at[1, 4, s], z_cross, TO_Z)
        send(Z_ID + 4 + s, xall.at[0, x, s], xall.at[0, 4, s], zh_mate, TO_Z)

    def z_first_take(s):
        wait(Z_ID + s, xall.at[1, x, s])

    def z_rest_take(s):
        wait(Z_ID + 2 + s, xall.at[1, 4, s])
        wait(Z_ID + 4 + s, xall.at[0, 4, s])

    def column_sums():
        for which, ref in ((zl, own_block), (1 - zl, give_block)):
            for s in range(2):
                values = ref(s)[...].astype(F32)
                total = jnp.sum(values * values, axis=0, keepdims=True)
                for k in range(2):
                    csend[which, :, HALF * k + PART * s : HALF * k + PART * (s + 1)] = total[
                        :, PART * k : PART * (k + 1)
                    ]

    def sum_copy(j):
        return remote(SUM_ID, csend, crecv.at[j], ((tok + j) % 16, blk), TO_SUM)

    def sums_start():
        def step(j, carry):
            sum_copy(j).start()
            return carry

        lax.fori_loop(1, 16, step, 0)

    total_to = [(tok, blk_of((x + j) % 4, zh)) for j in (1, 2, 3)] + [zh_mate]

    def total_copy(j):
        slot = x if j < 3 else 4
        return remote(TOTAL_ID, totbuf.at[x], totbuf.at[slot], total_to[j], TO_TOTAL)

    def totals_start():
        wait(SUM_ID, crecv.at[pl.ds(1, 15)])
        total = csend[...]
        for j in range(1, 16):
            total = total + crecv[j]
        totbuf[x] = total
        for j in range(4):
            total_copy(j).start()

    def totals_finish():
        wait(TOTAL_ID, totbuf.at[pl.ds(0, 4)])

    def gram(s, gs, begin, end):
        def step(i, carry):
            to = (x + 3 + i) % 4
            for g in gs:
                for s2 in range(2):
                    value = None
                    for t in range(2):
                        term = lax.dot_general(
                            xall[t, to, s], xall[t, (x, 4)[g], s2],
                            (((0,), (0,)), ((), ())), preferred_element_type=F32,
                        )
                        value = term if value is None else value + term
                    value = value.astype(BF16)
                    for k in range(2):
                        for k2 in range(2):
                            start = HALF * k2 + PART * s2
                            gram_part[s, g, to, k, :, start : start + PART] = value[
                                PART * k : PART * (k + 1), PART * k2 : PART * (k2 + 1)
                            ]
                d_copy(s, g, to).start()
            return carry

        lax.fori_loop(begin, end, step, 0)

    def d_copy(s, g, to):
        return remote(
            D_ID[s][g], gram_part.at[s, g, to, 1 - c], drecv.at[s, g, to], sibling, TO_SIBLING
        )

    halves = (pl.ds(0, PART // 2), pl.ds(PART // 2, PART // 2))

    def both(s, g, to, half):
        mine = gram_part[s, g, to, c, halves[half]].astype(F32)
        return mine + drecv[s, g, to, halves[half]].astype(F32)

    def reduce_first(s, g):
        y1, far = Y1_ID[s][g], keep(s, 2)
        wait(D_ID[s][g], drecv.at[s, g])
        y1s[s, g, 0] = both(s, g, far, 0).astype(BF16)
        send(y1, y1s.at[s, g, 0], y1r.at[s, g, 0], y_plus, TO_Y1)
        y1s[s, g, 1] = both(s, g, far, 1).astype(BF16)
        send(y1 + 1, y1s.at[s, g, 1], y1r.at[s, g, 1], y_minus, TO_Y1)

    def reduce_own(s, g):
        y2, up, down = Y2_ID[s][g], keep(s, 1), keep(s, 3)
        y2s[s, g, 0] = both(s, g, up, 1).astype(BF16)
        send(y2, y2s.at[s, g, 0], y2r.at[s, g, 0], y_plus, TO_Y2)
        y2s[s, g, 2] = both(s, g, down, 0).astype(BF16)
        send(y2, y2s.at[s, g, 2], y2r.at[s, g, 2], y_minus, TO_Y2)

    def reduce_middle(s, g):
        y1, y2, up, down = Y1_ID[s][g], Y2_ID[s][g], keep(s, 1), keep(s, 3)
        wait(y1, y1r.at[s, g, 0])
        y2s[s, g, 1] = (both(s, g, up, 0) + y1r[s, g, 0].astype(F32)).astype(BF16)
        send(y2, y2s.at[s, g, 1], y2r.at[s, g, 1], y_plus, TO_Y2)
        wait(y1 + 1, y1r.at[s, g, 1])
        y2s[s, g, 3] = (both(s, g, down, 1) + y1r[s, g, 1].astype(F32)).astype(BF16)
        send(y2, y2s.at[s, g, 3], y2r.at[s, g, 3], y_minus, TO_Y2)

    def eye(s, zh_, h):
        shape = (PART, BLOCK)
        r = lax.broadcasted_iota(jnp.int32, shape, 0) + HALF * c + PART * s
        k = lax.broadcasted_iota(jnp.int32, shape, 1)
        return (r + BLOCK * (2 * keep(s, 0) + zh_) == k + BLOCK * (2 * x + h)).astype(F32)

    def inverse(sums):
        return lax.rsqrt(sums / TOKENS + epsilon)

    def lane_block(block):
        return pl.ds(pl.multiple_of(block * BLOCK, BLOCK), BLOCK)

    def normalise(s, g):
        rows = pl.ds(pl.multiple_of(HALF * c + PART * s, PART), PART)
        inv_row = jnp.broadcast_to(inverse(totbuf[keep(s, 0), zl, :, rows]), (PART, PART))
        inv_row = jnp.concatenate([jnp.transpose(inv_row)] * 4, axis=1)
        wait(Y2_ID[s][g], y2r.at[s, g])
        inv_col = inverse(totbuf[(x, 4)[g], zl])
        low = both(s, g, keep(s, 0), 0) + y2r[s, g, 1].astype(F32) + y2r[s, g, 2].astype(F32)
        high = both(s, g, keep(s, 0), 1) + y2r[s, g, 0].astype(F32) + y2r[s, g, 3].astype(F32)
        total = jnp.concatenate([low, high], axis=0)
        damped = total / TOKENS * inv_row * inv_col + damping * eye(s, zh, zh_of[g])
        value = damped / divisor
        half = value.astype(BF16)
        rowbuf[zh, s, zh_of[g], :, lane_block(x)] = half
        if g == 0:
            scaled[0, s] = value
            colbuf[keep(s, 0), zh, c, s] = half
            cols[s][0].start()
        else:
            rows_of[s].cross(1)
            low_out[s] = (value - half.astype(F32)).astype(BF16)
        rows_of[s].start_half(g)

    def rows_start(s):
        rows_of[s].cross(0)
        if s == 0:
            low_send(s)

    def low_send(s):
        send(LOW_ID[s], low_out.at[s], low_in.at[s], zh_mate, TO_LOW)

    def partner(s):
        half = rowbuf[1 - zh, s, zh, :, lane_block(x)]
        colbuf[keep(s, 0), 1 - zh, c, s] = half
        if s == 0:
            cols[s][1].start()
        else:
            cols[s][1].start_direct(y_far)

    def partner_low(s):
        wait(LOW_ID[s], low_in.at[s])
        half = rowbuf[1 - zh, s, zh, :, lane_block(x)].astype(F32)
        scaled[1, s] = half + low_in[s].astype(F32)

    def row_plane(s):
        def ref(step, half, other=0):
            lanes = lane_block((x + step) % 4)
            r = rowbuf.at[zh_of[other], s]
            return r.at[:, :, lanes] if half is None else r.at[zh_of[(half + other) % 2], :, lanes]

        late = rowbuf.at[1 - zh, s, :, :, pl.ds(0, 3 * BLOCK)]
        return Plane(
            send, wait, ROW_ID[s], TO_ROWS, ref, x_plus, x_minus, late, zh_mate
        )

    def col_line(s, e):
        def ref(step, half):
            return colbuf.at[keep(s, step), zh_of[e], c, s, halves[half]]

        late = colbuf.at[0, zh_of[e], c, s]
        return Passed(
            send, wait, COL_ID[s][e], TO_COLS, ref, y_plus, y_minus, late, sibling, TO_PASS,
            colbuf.at[:, zh_of[e], 1 - c, s],
        )

    def sq_line(e):
        def ref(step, half):
            return sqcol.at[keep(half, step), zh_of[e], c, half]

        late = sqcol.at[0, zh_of[e], c]
        return Passed(
            send, wait, SQ_ID[e], TO_SQ, ref, y_plus, y_minus, late, sibling, TO_SQ_PASS,
            sqcol.at[:, zh_of[e], 1 - c],
        )

    rows_of = [row_plane(s) for s in range(2)]
    cols = [[col_line(s, e) for e in range(2)] for s in range(2)]
    sq_cols = [sq_line(e) for e in range(2)]

    def dot(e, p, right, lanes):
        return jnp.dot(
            rowbuf[zh_of[e], :, p].reshape(HALF, D // 2),
            right[:, p, :, :, :, lanes].reshape(D // 2, HALF),
            preferred_element_type=F32,
        )

    def over_lanes(body):
        def step(k, carry):
            body(pl.ds(pl.multiple_of(k * HALF, HALF), HALF))
            return carry

        lax.fori_loop(0, 2, step, 0)

    def square_first():
        def some(lanes):
            sq[0, :, lanes] = dot(0, zh, colbuf, lanes)

        over_lanes(some)

    def square(e):
        def some(lanes):
            if e == 0:
                sq[e, :, lanes] = sq[e, :, lanes] + dot(e, 1 - zh, colbuf, lanes)
            else:
                sq[e, :, lanes] = dot(e, 0, colbuf, lanes) + dot(e, 1, colbuf, lanes)

        over_lanes(some)
        for s in range(2):
            sqcol[keep(s, 0), zh_of[e], c, s] = sq[e, PART * s : PART * (s + 1)].astype(BF16)
        sq_cols[e].start()

    def combine(e):
        for s in range(2):
            scaled[e, s] = (
                4.0 * eye(s, zh_of[e], zh) - 6.0 * scaled[e, s]
                + 4.0 * sq[e, PART * s : PART * (s + 1)]
            )

    def cube_first():
        for e in range(2):
            def some(lanes):
                sq[e, :, lanes] = dot(e, zh, sqcol, lanes)

            over_lanes(some)

    def cube_second(e):
        def some(lanes):
            value = scaled[e, :, :, lanes].reshape(HALF, HALF) - sq[e, :, lanes]
            obuf[e, :, lanes] = (value - dot(e, 1 - zh, sqcol, lanes)).astype(BF16)

        over_lanes(some)
        for b in (0, 4, 2, 6, 1, 5, 3, 7):
            me = (out_tok(e, b // 4) == tok) & (blk == b)

            @pl.when(me)
            def _():
                out_ref[zl, :, lane_block(2 * x + zh)] = obuf[e, b * 32 : (b + 1) * 32]

            @pl.when(jnp.logical_not(me))
            def _():
                out_copy(e, b).start()

    def out_copy(e, b):
        return remote(
            OUT_ID, obuf.at[e, pl.ds(b * 32, 32)], out_ref.at[zl, :, lane_block(2 * x + zh)],
            (out_tok(e, b // 4), b), TO_OUT,
        )

    def emit():
        @pl.when(home)
        def _():
            wait(OUT_ID, out_ref.at[:, :, pl.ds(0, 15 * HALF)])
            left(TO_OUT, obuf.at[:, pl.ds(0, 15 * 16)])

        @pl.when(jnp.logical_not(home))
        def _():
            wait(OUT_ID, out_ref)
            left(TO_OUT, obuf)

    def all_left():
        left(TO_X, xall.at[:, pl.ds(0, 3)])
        left(TO_Z, xall.at[0, pl.ds(0, 3)])
        left(TO_SIBLING, gram_part.at[0])
        left(TO_Y1, y1s)
        left(TO_Y2, y2s)
        left(TO_ROWS, rowbuf.at[:, :, :, pl.ds(0, 112)])
        left(TO_LOW, low_out)
        left(TO_PASS, colbuf.at[pl.ds(0, 2)])
        left(TO_COLS, colbuf.at[pl.ds(0, 3), 0])
        left(TO_SQ, sqcol.at[pl.ds(0, 3), 0])
        left(TO_SQ_PASS, sqcol.at[pl.ds(0, 2)])
        left(TO_SUM, crecv.at[pl.ds(1, 15)])
        left(TO_TOTAL, totbuf.at[pl.ds(0, 4)])

    z_first(0)
    lines[0][0].start()
    column_sums()
    sums_start()
    z_first(1)
    z_rest(0)
    z_rest(1)
    lines[0][0].near()
    z_first_take(0)
    lines[0][1].start()
    totals_start()
    lines[0][1].near()
    lines[1][0].start()
    z_first_take(1)
    lines[1][1].start()
    lines[0][0].rest()
    lines[0][0].finish()
    lines[0][1].rest()
    lines[0][1].finish()
    gram(0, (0,), 0, 4)
    reduce_first(0, 0)
    reduce_own(0, 0)
    lines[1][0].near()
    z_rest_take(0)
    z_rest_take(1)
    gram(0, (1,), 0, 4)
    reduce_middle(0, 0)
    reduce_first(0, 1)
    reduce_own(0, 1)
    lines[1][1].near()
    totals_finish()
    reduce_middle(0, 1)
    normalise(0, 0)
    lines[1][0].rest()
    lines[1][1].rest()
    gram(1, (1, 0), 0, 3)
    normalise(0, 1)
    rows_start(0)
    lines[1][0].finish()
    lines[1][1].finish()
    gram(1, (1, 0), 3, 4)
    reduce_first(1, 1)
    reduce_first(1, 0)
    reduce_own(1, 1)
    reduce_own(1, 0)
    rows_of[0].near_half(0)
    cols[0][0].near()
    reduce_middle(1, 1)
    rows_of[0].near_half(1)
    reduce_middle(1, 0)
    rows_of[0].take_needed()
    partner(0)
    rows_of[0].other()
    cols[0][0].rest()
    rows_of[0].far()
    normalise(1, 1)
    normalise(1, 0)
    rows_start(1)
    cols[0][1].near()
    cols[0][0].finish()
    cols[1][0].near()
    rows_of[1].take_needed()
    partner(1)
    rows_of[1].near_half(1)
    cols[0][1].rest()
    rows_of[1].near_half(0)
    rows_of[1].other()
    cols[1][0].rest()
    cols[1][1].near_direct()
    cols[0][1].finish()
    cols[1][0].finish()
    rows_of[1].far()
    low_send(1)
    cols[0][0].passed()
    cols[1][0].passed()
    square_first()
    cols[1][1].rest()
    cols[1][1].finish()
    cols[0][1].passed()
    cols[1][1].passed()
    square(0)
    rows_of[0].last()
    rows_of[1].last()
    square(1)
    sq_cols[0].near()
    combine(0)
    partner_low(0)
    partner_low(1)
    combine(1)
    sq_cols[1].near()
    sq_cols[0].rest()
    sq_cols[0].finish()
    sq_cols[1].rest()
    sq_cols[0].passed()
    cube_first()
    sq_cols[1].finish()
    sq_cols[1].passed()
    cube_second(0)
    cube_second(1)
    all_left()
    emit()


def body(activations, out_grads):
    hbm = pl.BlockSpec(memory_space=pltpu.HBM)
    vmem = pl.BlockSpec(memory_space=pltpu.VMEM)
    part = (PART, BLOCK)
    half_part = (PART // 2, BLOCK)
    scratch = [
        pltpu.VMEM((2, 5, 2, BLOCK, HALF), BF16),
        pltpu.VMEM((2, BLOCK, HALF), BF16),
        pltpu.VMEM((2, 2, 4, 2, *part), BF16),
        pltpu.VMEM((2, 2, 4, *part), BF16),
        pltpu.VMEM((2, 2, 2, *half_part), BF16),
        pltpu.VMEM((2, 2, 2, *half_part), BF16),
        pltpu.VMEM((2, 2, 4, *half_part), BF16),
        pltpu.VMEM((2, 2, 4, *half_part), BF16),
        pltpu.VMEM((2, 2, *part), F32),
        pltpu.VMEM((2, 2, 2, PART, D // 2), BF16),
        pltpu.VMEM((4, 2, 2, 2, *part), BF16),
        pltpu.VMEM((4, 2, 2, 2, *part), BF16),
        pltpu.VMEM((2, HALF, BLOCK), F32),
        pltpu.VMEM((2, *part), BF16),
        pltpu.VMEM((2, *part), BF16),
        pltpu.VMEM((2, HALF, BLOCK), BF16),
        pltpu.VMEM((2, 1, BLOCK), F32),
        pltpu.VMEM((16, 2, 1, BLOCK), F32),
        pltpu.VMEM((5, 2, 1, BLOCK), F32),
        pltpu.SemaphoreType.DMA((N_TO,)),
        pltpu.SemaphoreType.DMA((N_ID,)),
        pltpu.SemaphoreType.DMA((8,)),
    ]
    out = pl.pallas_call(
        kernel,
        out_shape=pltpu.VMEM((2, 32, D), BF16),
        in_specs=[hbm, hbm],
        out_specs=vmem,
        scratch_shapes=scratch,
        compiler_params=pltpu.CompilerParams(
            collective_id=0, has_side_effects=True, vmem_limit_bytes=60 * 1024 * 1024
        ),
    )(activations, out_grads)
    return out[0].astype(F32), out[1].astype(F32)


def solution(mesh):
    placed = (P("tok", "blk"), P("tok", "blk"))
    return jax.shard_map(
        body,
        mesh=mesh,
        in_specs=placed,
        out_specs=(P(("tok", "blk"), None), P(("tok", "blk"), None)),
        check_vma=False,
    )
```

```python
import jax
import jax.numpy as jnp
from jax import lax
from jax.experimental import pallas as pl
from jax.experimental.pallas import tpu as pltpu
from jax.sharding import PartitionSpec as P

D = 4096
TOKENS = 8192
BLOCK = 512
HALF = 256
PART = 128

damping = 0.3
epsilon = 1e-06
divisor = 2.0

MESH = pl.DeviceIdType.MESH
F32 = jnp.float32
BF16 = jnp.bfloat16


class Ids:
    def __init__(self):
        self.next = 0

    def take(self, n):
        first = self.next
        self.next += n
        return first


IDS = Ids()
Z_ID = IDS.take(6)
X_ID = [[IDS.take(4) for _ in range(2)] for _ in range(2)]
D_ID = [[IDS.take(1) for _ in range(2)] for _ in range(2)]
Y1_ID = [[IDS.take(2) for _ in range(2)] for _ in range(2)]
Y2_ID = [[IDS.take(1) for _ in range(2)] for _ in range(2)]
ROW_ID = [IDS.take(8) for _ in range(2)]
LOW_ID = [IDS.take(1) for _ in range(2)]
COL_ID = [[IDS.take(5) for _ in range(2)] for _ in range(2)]
SQ_ID = [IDS.take(5) for _ in range(2)]
OUT_ID = IDS.take(1)
SUM_ID = IDS.take(1)
TOTAL_ID = IDS.take(1)
N_ID = IDS.next

(TO_X, TO_Z, TO_SIBLING, TO_Y1, TO_Y2, TO_ROWS, TO_LOW, TO_PASS, TO_COLS, TO_SQ, TO_SQ_PASS,
 TO_OUT, TO_SUM, TO_TOTAL, N_TO) = range(15)


class Line:
    arrivals = [(3, 0), (3, 1), (1, 1), (1, 0), (2, 0), (2, 1)]
    number = [0, 2, 1, 2, 3, 3]

    def __init__(self, send, wait, base, kind, ref, plus, minus, late):
        self.send, self.wait, self.base, self.kind, self.ref = send, wait, base, kind, ref
        self.plus, self.minus, self.late = plus, minus, late

    def put(self, k, where, to):
        r = self.ref(*where)
        self.send(self.base + self.number[k], r, r, to, self.kind)

    def arrived(self, k):
        pass

    def take(self, k):
        self.wait(self.base + self.number[k], self.ref(*self.arrivals[k]))
        self.arrived(k)

    def start(self):
        self.put(0, (0, 0), self.plus)
        self.put(2, (0, 1), self.minus)
        self.put(1, (0, 1), self.plus)
        self.put(3, (0, 0), self.minus)

    def near(self):
        self.take(0)
        self.put(4, (3, 0), self.plus)
        self.take(2)
        self.put(5, (1, 1), self.minus)

    def rest(self):
        self.wait(self.base + 2, self.late)

    def finish(self):
        self.wait(self.base + 3, self.late)


class Passed(Line):
    number = [0, 2, 1, 2, 4, 4]

    def __init__(self, send, wait, base, kind, ref, plus, minus, late, sibling, pass_kind, mirrored):
        super().__init__(send, wait, base, kind, ref, plus, minus, late)
        self.sibling, self.pass_kind, self.mirrored = sibling, pass_kind, mirrored

    def pass_on(self, where):
        r = self.ref(*where)
        self.send(self.base + 3, r, r, self.sibling, self.pass_kind)

    def arrived(self, k):
        self.pass_on(self.arrivals[k])

    def start(self):
        super().start()
        self.pass_on((0, 0))
        self.pass_on((0, 1))

    def start_set(self, half):
        for k, to in ((0, self.plus), (3, self.minus)) if half == 0 else (
            (2, self.minus), (1, self.plus)
        ):
            self.put(k, (0, half), to)
        self.pass_on((0, half))

    def start_direct(self, far):
        self.start()
        self.put(4, (0, 0), far)
        self.put(5, (0, 1), far)

    def near_direct(self):
        self.take(0)
        self.take(2)

    def rest(self):
        self.wait(self.base + 2, self.late)
        self.arrived(1)
        self.arrived(3)

    def finish(self):
        self.wait(self.base + 4, self.late)
        self.arrived(4)
        self.arrived(5)

    def passed(self):
        self.wait(self.base + 3, self.mirrored)


class Plane(Line):
    arrivals = Line.arrivals + [None, (3, None, 1), (1, None, 1), (2, 0, 1), (2, 1, 1)]
    number = [0, 2, 1, 2, 3, 4, 5, 6, 6, 6, 6]

    def __init__(self, send, wait, base, kind, ref, plus, minus, late, across):
        super().__init__(send, wait, base, kind, ref, plus, minus, late)
        self.across = across

    def cross(self, half):
        r = self.ref(0, half, 0)
        self.send(self.base + (7, 5)[half], r, r, self.across, self.kind)

    def start_half(self, half):
        if half == 0:
            self.put(0, (0, 0), self.plus)
            self.put(3, (0, 0), self.minus)
        else:
            self.put(2, (0, 1), self.minus)
            self.put(1, (0, 1), self.plus)

    def take_needed(self):
        self.wait(self.base + 5, self.ref(0, 1, 1))

    def other(self):
        self.wait(self.base + 7, self.ref(0, 0, 1))
        self.put(7, (0, None, 1), self.plus)
        self.put(8, (0, None, 1), self.minus)

    def near_half(self, half):
        if half == 0:
            self.take(0)
            self.put(4, (3, 0), self.plus)
        else:
            self.take(2)
            self.put(5, (1, 1), self.minus)

    def far(self):
        self.wait(self.base + 2, self.ref(3, None))
        self.take(4)
        self.put(9, (2, 0, 0), self.across)
        self.take(5)
        self.put(10, (2, 1, 0), self.across)

    def last(self):
        self.wait(self.base + 6, self.late)


def kernel(
    act_ref, grad_ref, out_ref,
    xall, give, gram_part, drecv, y1s, y1r, y2s, y2r, scaled,
    rowbuf, colbuf, sqcol, sq, low_out, low_in, obuf, csend, crecv, totbuf,
    ssem, rsem, lsem,
):
    tok, blk = lax.axis_index("tok"), lax.axis_index("blk")
    c, y, zl = tok % 2, (tok // 2) % 4, tok // 8
    x, zh = blk // 2, blk % 2

    def tok_of(zl_, y_, c_):
        return zl_ * 8 + y_ * 2 + c_

    def blk_of(x_, zh_):
        return x_ * 2 + zh_

    x_plus = (tok, blk_of((x + 1) % 4, zh))
    x_minus = (tok, blk_of((x + 3) % 4, zh))
    zh_mate = (tok, blk_of(x, 1 - zh))
    y_plus = (tok_of(zl, (y + 1) % 4, c), blk)
    y_minus = (tok_of(zl, (y + 3) % 4, c), blk)
    y_far = (tok_of(zl, (y + 2) % 4, c), blk)
    zl_mate = (tok_of(1 - zl, y, c), blk)
    z_cross = (tok_of(1 - zl, y, c), blk_of(x, 1 - zh))
    sibling = (tok_of(zl, y, 1 - c), blk)

    def place(to):
        return {"tok": to[0], "blk": to[1]}

    def row_of(s, y_):
        return ((y_ + s) % 2) * 2 + y_ // 2

    def keep(s, step):
        return row_of(s, (y + step) % 4)

    zh_of = (zh, 1 - zh)

    def out_tok(e, s):
        return 2 * (2 * keep(s, 0) + zh_of[e]) + c

    source_y = ((tok // 4) % 2) * 2 + (tok // 8 + blk // 4) % 2
    home = source_y == y

    def loads(src, dst, first):
        out = []
        for s in range(2):
            for k in range(2):
                cols = pl.ds(HALF * k + PART * s, PART)
                out.append(
                    pltpu.make_async_copy(
                        src.at[:, cols], dst(s).at[:, pl.ds(PART * k, PART)],
                        lsem.at[first + 2 * s + k],
                    )
                )
        return out

    def own_block(s):
        return xall.at[0, x, s]

    def give_block(s):
        return give.at[s]

    def all_loads(own_ref, give_ref):
        return loads(own_ref, own_block, 0) + loads(give_ref, give_block, 4)

    @pl.when(zl == 0)
    def _():
        for copy in all_loads(act_ref, grad_ref):
            copy.start()

    @pl.when(zl == 1)
    def _():
        for copy in all_loads(grad_ref, act_ref):
            copy.start()

    barrier = pltpu.get_barrier_semaphore()

    def greet(to):
        pl.semaphore_signal(barrier, inc=1, device_id=place(to), device_id_type=MESH)

    def greet_tok(j, carry):
        greet(((tok + j) % 16, blk))
        return carry

    lax.fori_loop(1, 16, greet_tok, 0)
    for to in (x_plus, x_minus, zh_mate, z_cross):
        greet(to)
    for copy in all_loads(act_ref, grad_ref):
        copy.wait()
    pl.semaphore_wait(barrier, 15 + 4)

    def remote(k, src, dst, to, kind):
        return pltpu.make_async_remote_copy(
            src_ref=src, dst_ref=dst, send_sem=ssem.at[kind], recv_sem=rsem.at[k],
            device_id=place(to), device_id_type=MESH,
        )

    def send(k, src, dst, to, kind):
        remote(k, src, dst, to, kind).start()

    def wait(k, dst):
        remote(k, dst, dst, sibling, 0).wait_recv()

    def left(kind, src):
        remote(0, src, src, sibling, kind).wait_send()

    token_half = (pl.ds(0, HALF), pl.ds(HALF, HALF))

    def x_line(s, t):
        def ref(step, half):
            return xall.at[t, (x + step) % 4, s, token_half[half]]

        return Line(
            send, wait, X_ID[s][t], TO_X, ref, x_plus, x_minus, xall.at[t, (x + 2) % 4, s]
        )

    lines = [[x_line(s, t) for t in range(2)] for s in range(2)]

    def z_first(s):
        send(Z_ID + s, give.at[s], xall.at[1, x, s], zl_mate, TO_Z)

    def z_rest(s):
        send(Z_ID + 2 + s, give.at[s], xall.at[1, 4, s], z_cross, TO_Z)
        send(Z_ID + 4 + s, xall.at[0, x, s], xall.at[0, 4, s], zh_mate, TO_Z)

    def z_first_take(s):
        wait(Z_ID + s, xall.at[1, x, s])

    def z_rest_take(s):
        wait(Z_ID + 2 + s, xall.at[1, 4, s])
        wait(Z_ID + 4 + s, xall.at[0, 4, s])

    def column_sums():
        for which, ref in ((zl, own_block), (1 - zl, give_block)):
            for s in range(2):
                values = ref(s)[...].astype(F32)
                total = jnp.sum(values * values, axis=0, keepdims=True)
                for k in range(2):
                    csend[which, :, HALF * k + PART * s : HALF * k + PART * (s + 1)] = total[
                        :, PART * k : PART * (k + 1)
                    ]

    def sum_copy(j):
        return remote(SUM_ID, csend, crecv.at[j], ((tok + j) % 16, blk), TO_SUM)

    def sums_start():
        def step(j, carry):
            sum_copy(j).start()
            return carry

        lax.fori_loop(1, 16, step, 0)

    total_to = [(tok, blk_of((x + j) % 4, zh)) for j in (1, 2, 3)] + [zh_mate]

    def total_copy(j):
        slot = x if j < 3 else 4
        return remote(TOTAL_ID, totbuf.at[x], totbuf.at[slot], total_to[j], TO_TOTAL)

    def totals_start():
        wait(SUM_ID, crecv.at[pl.ds(1, 15)])
        total = csend[...]
        for j in range(1, 16):
            total = total + crecv[j]
        totbuf[x] = total
        for j in range(4):
            total_copy(j).start()

    def totals_finish():
        wait(TOTAL_ID, totbuf.at[pl.ds(0, 4)])

    def gram(s, gs, begin, end):
        def step(i, carry):
            to = (x + 3 + i) % 4
            for g in gs:
                for s2 in range(2):
                    value = None
                    for t in range(2):
                        term = lax.dot_general(
                            xall[t, to, s], xall[t, (x, 4)[g], s2],
                            (((0,), (0,)), ((), ())), preferred_element_type=F32,
                        )
                        value = term if value is None else value + term
                    value = value.astype(BF16)
                    for k in range(2):
                        for k2 in range(2):
                            start = HALF * k2 + PART * s2
                            gram_part[s, g, to, k, :, start : start + PART] = value[
                                PART * k : PART * (k + 1), PART * k2 : PART * (k2 + 1)
                            ]
                d_copy(s, g, to).start()
            return carry

        lax.fori_loop(begin, end, step, 0)

    def d_copy(s, g, to):
        return remote(
            D_ID[s][g], gram_part.at[s, g, to, 1 - c], drecv.at[s, g, to], sibling, TO_SIBLING
        )

    halves = (pl.ds(0, PART // 2), pl.ds(PART // 2, PART // 2))

    def both(s, g, to, half):
        mine = gram_part[s, g, to, c, halves[half]].astype(F32)
        return mine + drecv[s, g, to, halves[half]].astype(F32)

    def reduce_first(s, g):
        y1, far = Y1_ID[s][g], keep(s, 2)
        wait(D_ID[s][g], drecv.at[s, g])
        y1s[s, g, 0] = both(s, g, far, 0).astype(BF16)
        send(y1, y1s.at[s, g, 0], y1r.at[s, g, 0], y_plus, TO_Y1)
        y1s[s, g, 1] = both(s, g, far, 1).astype(BF16)
        send(y1 + 1, y1s.at[s, g, 1], y1r.at[s, g, 1], y_minus, TO_Y1)

    def reduce_own(s, g):
        y2, up, down = Y2_ID[s][g], keep(s, 1), keep(s, 3)
        y2s[s, g, 0] = both(s, g, up, 1).astype(BF16)
        send(y2, y2s.at[s, g, 0], y2r.at[s, g, 0], y_plus, TO_Y2)
        y2s[s, g, 2] = both(s, g, down, 0).astype(BF16)
        send(y2, y2s.at[s, g, 2], y2r.at[s, g, 2], y_minus, TO_Y2)

    def reduce_middle(s, g):
        y1, y2, up, down = Y1_ID[s][g], Y2_ID[s][g], keep(s, 1), keep(s, 3)
        wait(y1, y1r.at[s, g, 0])
        y2s[s, g, 1] = (both(s, g, up, 0) + y1r[s, g, 0].astype(F32)).astype(BF16)
        send(y2, y2s.at[s, g, 1], y2r.at[s, g, 1], y_plus, TO_Y2)
        wait(y1 + 1, y1r.at[s, g, 1])
        y2s[s, g, 3] = (both(s, g, down, 1) + y1r[s, g, 1].astype(F32)).astype(BF16)
        send(y2, y2s.at[s, g, 3], y2r.at[s, g, 3], y_minus, TO_Y2)

    def eye(s, zh_, h):
        shape = (PART, BLOCK)
        r = lax.broadcasted_iota(jnp.int32, shape, 0) + HALF * c + PART * s
        k = lax.broadcasted_iota(jnp.int32, shape, 1)
        return (r + BLOCK * (2 * keep(s, 0) + zh_) == k + BLOCK * (2 * x + h)).astype(F32)

    def inverse(sums):
        return lax.rsqrt(sums / TOKENS + epsilon)

    def lane_block(block):
        return pl.ds(pl.multiple_of(block * BLOCK, BLOCK), BLOCK)

    def normalise(s, g):
        rows = pl.ds(pl.multiple_of(HALF * c + PART * s, PART), PART)
        inv_row = jnp.broadcast_to(inverse(totbuf[keep(s, 0), zl, :, rows]), (PART, PART))
        inv_row = jnp.concatenate([jnp.transpose(inv_row)] * 4, axis=1)
        wait(Y2_ID[s][g], y2r.at[s, g])
        inv_col = inverse(totbuf[(x, 4)[g], zl])
        low = both(s, g, keep(s, 0), 0) + y2r[s, g, 1].astype(F32) + y2r[s, g, 2].astype(F32)
        high = both(s, g, keep(s, 0), 1) + y2r[s, g, 0].astype(F32) + y2r[s, g, 3].astype(F32)
        total = jnp.concatenate([low, high], axis=0)
        damped = total / TOKENS * inv_row * inv_col + damping * eye(s, zh, zh_of[g])
        value = damped / divisor
        half = value.astype(BF16)
        rowbuf[zh, s, zh_of[g], :, lane_block(x)] = half
        if g == 0:
            scaled[0, s] = value
            colbuf[keep(s, 0), zh, c, s] = half
            cols[s][0].start()
        else:
            rows_of[s].cross(1)
            low_out[s] = (value - half.astype(F32)).astype(BF16)
        rows_of[s].start_half(g)

    def rows_start(s):
        rows_of[s].cross(0)
        if s == 0:
            low_send(s)

    def low_send(s):
        send(LOW_ID[s], low_out.at[s], low_in.at[s], zh_mate, TO_LOW)

    def partner(s):
        half = rowbuf[1 - zh, s, zh, :, lane_block(x)]
        colbuf[keep(s, 0), 1 - zh, c, s] = half
        if s == 0:
            cols[s][1].start()
        else:
            cols[s][1].start_direct(y_far)

    def partner_low(s):
        wait(LOW_ID[s], low_in.at[s])
        half = rowbuf[1 - zh, s, zh, :, lane_block(x)].astype(F32)
        scaled[1, s] = half + low_in[s].astype(F32)

    def row_plane(s):
        def ref(step, half, other=0):
            lanes = lane_block((x + step) % 4)
            r = rowbuf.at[zh_of[other], s]
            return r.at[:, :, lanes] if half is None else r.at[zh_of[(half + other) % 2], :, lanes]

        late = rowbuf.at[1 - zh, s, :, :, pl.ds(0, 3 * BLOCK)]
        return Plane(
            send, wait, ROW_ID[s], TO_ROWS, ref, x_plus, x_minus, late, zh_mate
        )

    def col_line(s, e):
        def ref(step, half):
            return colbuf.at[keep(s, step), zh_of[e], c, s, halves[half]]

        late = colbuf.at[0, zh_of[e], c, s]
        return Passed(
            send, wait, COL_ID[s][e], TO_COLS, ref, y_plus, y_minus, late, sibling, TO_PASS,
            colbuf.at[:, zh_of[e], 1 - c, s],
        )

    def sq_line(e):
        def ref(step, half):
            return sqcol.at[keep(half, step), zh_of[e], c, half]

        late = sqcol.at[0, zh_of[e], c]
        return Passed(
            send, wait, SQ_ID[e], TO_SQ, ref, y_plus, y_minus, late, sibling, TO_SQ_PASS,
            sqcol.at[:, zh_of[e], 1 - c],
        )

    rows_of = [row_plane(s) for s in range(2)]
    cols = [[col_line(s, e) for e in range(2)] for s in range(2)]
    sq_cols = [sq_line(e) for e in range(2)]

    def dot(e, p, right, lanes):
        return jnp.dot(
            rowbuf[zh_of[e], :, p].reshape(HALF, D // 2),
            right[:, p, :, :, :, lanes].reshape(D // 2, HALF),
            preferred_element_type=F32,
        )

    def over_lanes(body):
        def step(k, carry):
            body(pl.ds(pl.multiple_of(k * HALF, HALF), HALF))
            return carry

        lax.fori_loop(0, 2, step, 0)

    def square_first():
        def some(lanes):
            sq[0, :, lanes] = dot(0, zh, colbuf, lanes)

        over_lanes(some)

    def square(e):
        if e == 1:
            def some(lanes):
                sq[e, :, lanes] = dot(e, 0, colbuf, lanes) + dot(e, 1, colbuf, lanes)

            over_lanes(some)
            for s in range(2):
                sqcol[keep(s, 0), zh_of[e], c, s] = sq[e, PART * s : PART * (s + 1)].astype(BF16)
            sq_cols[e].start()
            return
        for s in range(2):
            rows = pl.ds(PART * s, PART)

            def some_rows(lanes):
                sq[e, rows, lanes] = sq[e, rows, lanes] + jnp.dot(
                    rowbuf[zh_of[e], s, 1 - zh],
                    colbuf[:, 1 - zh, :, :, :, lanes].reshape(D // 2, HALF),
                    preferred_element_type=F32,
                )

            over_lanes(some_rows)
            sqcol[keep(s, 0), zh_of[e], c, s] = sq[e, rows].astype(BF16)
            sq_cols[e].start_set(s)

    def combine(e):
        for s in range(2):
            scaled[e, s] = (
                4.0 * eye(s, zh_of[e], zh) - 6.0 * scaled[e, s]
                + 4.0 * sq[e, PART * s : PART * (s + 1)]
            )

    def cube_first():
        for e in range(2):
            def some(lanes):
                sq[e, :, lanes] = dot(e, zh, sqcol, lanes)

            over_lanes(some)

    def cube_second(e):
        def some(lanes):
            value = scaled[e, :, :, lanes].reshape(HALF, HALF) - sq[e, :, lanes]
            obuf[e, :, lanes] = (value - dot(e, 1 - zh, sqcol, lanes)).astype(BF16)

        over_lanes(some)
        for b in (0, 4, 2, 6, 1, 5, 3, 7):
            me = (out_tok(e, b // 4) == tok) & (blk == b)

            @pl.when(me)
            def _():
                out_ref[zl, :, lane_block(2 * x + zh)] = obuf[e, b * 32 : (b + 1) * 32]

            @pl.when(jnp.logical_not(me))
            def _():
                out_copy(e, b).start()

    def out_copy(e, b):
        return remote(
            OUT_ID, obuf.at[e, pl.ds(b * 32, 32)], out_ref.at[zl, :, lane_block(2 * x + zh)],
            (out_tok(e, b // 4), b), TO_OUT,
        )

    def emit():
        @pl.when(home)
        def _():
            wait(OUT_ID, out_ref.at[:, :, pl.ds(0, 15 * HALF)])
            left(TO_OUT, obuf.at[:, pl.ds(0, 15 * 16)])

        @pl.when(jnp.logical_not(home))
        def _():
            wait(OUT_ID, out_ref)
            left(TO_OUT, obuf)

    def all_left():
        left(TO_X, xall.at[:, pl.ds(0, 3)])
        left(TO_Z, xall.at[0, pl.ds(0, 3)])
        left(TO_SIBLING, gram_part.at[0])
        left(TO_Y1, y1s)
        left(TO_Y2, y2s)
        left(TO_ROWS, rowbuf.at[:, :, :, pl.ds(0, 112)])
        left(TO_LOW, low_out)
        left(TO_PASS, colbuf.at[pl.ds(0, 2)])
        left(TO_COLS, colbuf.at[pl.ds(0, 3), 0])
        left(TO_SQ, sqcol.at[pl.ds(0, 3), 0])
        left(TO_SQ_PASS, sqcol.at[pl.ds(0, 2)])
        left(TO_SUM, crecv.at[pl.ds(1, 15)])
        left(TO_TOTAL, totbuf.at[pl.ds(0, 4)])

    z_first(0)
    lines[0][0].start()
    column_sums()
    sums_start()
    z_first(1)
    z_rest(0)
    z_rest(1)
    lines[0][0].near()
    z_first_take(0)
    lines[0][1].start()
    totals_start()
    lines[0][1].near()
    lines[1][0].start()
    z_first_take(1)
    lines[1][1].start()
    lines[0][0].rest()
    lines[0][0].finish()
    lines[0][1].rest()
    lines[0][1].finish()
    gram(0, (0,), 0, 4)
    reduce_first(0, 0)
    reduce_own(0, 0)
    lines[1][0].near()
    z_rest_take(0)
    z_rest_take(1)
    gram(0, (1,), 0, 4)
    reduce_middle(0, 0)
    reduce_first(0, 1)
    reduce_own(0, 1)
    lines[1][1].near()
    totals_finish()
    reduce_middle(0, 1)
    normalise(0, 0)
    lines[1][0].rest()
    lines[1][1].rest()
    gram(1, (1, 0), 0, 3)
    normalise(0, 1)
    rows_start(0)
    lines[1][0].finish()
    lines[1][1].finish()
    gram(1, (1, 0), 3, 4)
    reduce_first(1, 1)
    reduce_first(1, 0)
    reduce_own(1, 1)
    reduce_own(1, 0)
    rows_of[0].near_half(0)
    cols[0][0].near()
    reduce_middle(1, 1)
    rows_of[0].near_half(1)
    reduce_middle(1, 0)
    rows_of[0].take_needed()
    partner(0)
    rows_of[0].other()
    cols[0][0].rest()
    rows_of[0].far()
    normalise(1, 1)
    normalise(1, 0)
    rows_start(1)
    cols[0][1].near()
    cols[0][0].finish()
    cols[1][0].near()
    rows_of[1].take_needed()
    partner(1)
    rows_of[1].near_half(1)
    cols[0][1].rest()
    rows_of[1].near_half(0)
    rows_of[1].other()
    cols[1][0].rest()
    cols[1][1].near_direct()
    cols[0][1].finish()
    cols[1][0].finish()
    rows_of[1].far()
    low_send(1)
    cols[0][0].passed()
    cols[1][0].passed()
    square_first()
    cols[1][1].rest()
    cols[1][1].finish()
    cols[0][1].passed()
    cols[1][1].passed()
    square(0)
    rows_of[0].last()
    rows_of[1].last()
    square(1)
    sq_cols[0].near()
    combine(0)
    partner_low(0)
    partner_low(1)
    combine(1)
    sq_cols[1].near()
    sq_cols[0].rest()
    sq_cols[0].finish()
    sq_cols[1].rest()
    sq_cols[0].passed()
    cube_first()
    sq_cols[1].finish()
    sq_cols[1].passed()
    cube_second(0)
    cube_second(1)
    all_left()
    emit()


def body(activations, out_grads):
    hbm = pl.BlockSpec(memory_space=pltpu.HBM)
    vmem = pl.BlockSpec(memory_space=pltpu.VMEM)
    part = (PART, BLOCK)
    half_part = (PART // 2, BLOCK)
    scratch = [
        pltpu.VMEM((2, 5, 2, BLOCK, HALF), BF16),
        pltpu.VMEM((2, BLOCK, HALF), BF16),
        pltpu.VMEM((2, 2, 4, 2, *part), BF16),
        pltpu.VMEM((2, 2, 4, *part), BF16),
        pltpu.VMEM((2, 2, 2, *half_part), BF16),
        pltpu.VMEM((2, 2, 2, *half_part), BF16),
        pltpu.VMEM((2, 2, 4, *half_part), BF16),
        pltpu.VMEM((2, 2, 4, *half_part), BF16),
        pltpu.VMEM((2, 2, *part), F32),
        pltpu.VMEM((2, 2, 2, PART, D // 2), BF16),
        pltpu.VMEM((4, 2, 2, 2, *part), BF16),
        pltpu.VMEM((4, 2, 2, 2, *part), BF16),
        pltpu.VMEM((2, HALF, BLOCK), F32),
        pltpu.VMEM((2, *part), BF16),
        pltpu.VMEM((2, *part), BF16),
        pltpu.VMEM((2, HALF, BLOCK), BF16),
        pltpu.VMEM((2, 1, BLOCK), F32),
        pltpu.VMEM((16, 2, 1, BLOCK), F32),
        pltpu.VMEM((5, 2, 1, BLOCK), F32),
        pltpu.SemaphoreType.DMA((N_TO,)),
        pltpu.SemaphoreType.DMA((N_ID,)),
        pltpu.SemaphoreType.DMA((8,)),
    ]
    out = pl.pallas_call(
        kernel,
        out_shape=pltpu.VMEM((2, 32, D), BF16),
        in_specs=[hbm, hbm],
        out_specs=vmem,
        scratch_shapes=scratch,
        compiler_params=pltpu.CompilerParams(
            collective_id=0, has_side_effects=True, vmem_limit_bytes=60 * 1024 * 1024
        ),
    )(activations, out_grads)
    return out[0].astype(F32), out[1].astype(F32)


def solution(mesh):
    placed = (P("tok", "blk"), P("tok", "blk"))
    return jax.shard_map(
        body,
        mesh=mesh,
        in_specs=placed,
        out_specs=(P(("tok", "blk"), None), P(("tok", "blk"), None)),
        check_vma=False,
    )
```

```python
import jax
import jax.numpy as jnp
from jax import lax
from jax.experimental import pallas as pl
from jax.experimental.pallas import tpu as pltpu
from jax.sharding import PartitionSpec as P

D = 4096
TOKENS = 8192
BLOCK = 512
HALF = 256
PART = 128

damping = 0.3
epsilon = 1e-06
divisor = 2.0

MESH = pl.DeviceIdType.MESH
F32 = jnp.float32
BF16 = jnp.bfloat16


class Ids:
    def __init__(self):
        self.next = 0

    def take(self, n):
        first = self.next
        self.next += n
        return first


IDS = Ids()
Z_ID = IDS.take(6)
X_ID = [[IDS.take(4) for _ in range(2)] for _ in range(2)]
D_ID = [[IDS.take(1) for _ in range(2)] for _ in range(2)]
Y1_ID = [[IDS.take(2) for _ in range(2)] for _ in range(2)]
Y2_ID = [[IDS.take(1) for _ in range(2)] for _ in range(2)]
ROW_ID = [IDS.take(8) for _ in range(2)]
LOW_ID = [IDS.take(1) for _ in range(2)]
COL_ID = [[IDS.take(5) for _ in range(2)] for _ in range(2)]
SQ_ID = [IDS.take(5) for _ in range(2)]
OUT_ID = IDS.take(1)
SUM_ID = IDS.take(1)
TOTAL_ID = IDS.take(1)
N_ID = IDS.next

(TO_X, TO_Z, TO_SIBLING, TO_Y1, TO_Y2, TO_ROWS, TO_LOW, TO_PASS, TO_COLS, TO_SQ, TO_SQ_PASS,
 TO_OUT, TO_SUM, TO_TOTAL, N_TO) = range(15)


class Line:
    arrivals = [(3, 0), (3, 1), (1, 1), (1, 0), (2, 0), (2, 1)]
    number = [0, 2, 1, 2, 3, 3]

    def __init__(self, send, wait, base, kind, ref, plus, minus, late):
        self.send, self.wait, self.base, self.kind, self.ref = send, wait, base, kind, ref
        self.plus, self.minus, self.late = plus, minus, late

    def put(self, k, where, to):
        r = self.ref(*where)
        self.send(self.base + self.number[k], r, r, to, self.kind)

    def arrived(self, k):
        pass

    def take(self, k):
        self.wait(self.base + self.number[k], self.ref(*self.arrivals[k]))
        self.arrived(k)

    def start(self):
        self.put(0, (0, 0), self.plus)
        self.put(2, (0, 1), self.minus)
        self.put(1, (0, 1), self.plus)
        self.put(3, (0, 0), self.minus)

    def near(self):
        self.take(0)
        self.put(4, (3, 0), self.plus)
        self.take(2)
        self.put(5, (1, 1), self.minus)

    def rest(self):
        self.wait(self.base + 2, self.late)

    def finish(self):
        self.wait(self.base + 3, self.late)


class Passed(Line):
    number = [0, 2, 1, 2, 4, 4]

    def __init__(self, send, wait, base, kind, ref, plus, minus, late, sibling, pass_kind, mirrored):
        super().__init__(send, wait, base, kind, ref, plus, minus, late)
        self.sibling, self.pass_kind, self.mirrored = sibling, pass_kind, mirrored

    def pass_on(self, where):
        r = self.ref(*where)
        self.send(self.base + 3, r, r, self.sibling, self.pass_kind)

    def arrived(self, k):
        self.pass_on(self.arrivals[k])

    def start(self):
        super().start()
        self.pass_on((0, 0))
        self.pass_on((0, 1))

    def start_set(self, half):
        for k, to in ((0, self.plus), (3, self.minus)) if half == 0 else (
            (2, self.minus), (1, self.plus)
        ):
            self.put(k, (0, half), to)
        self.pass_on((0, half))

    def start_direct(self, far):
        self.start()
        self.put(4, (0, 0), far)
        self.put(5, (0, 1), far)

    def near_direct(self):
        self.take(0)
        self.take(2)

    def rest(self):
        self.wait(self.base + 2, self.late)
        self.arrived(1)
        self.arrived(3)

    def finish(self):
        self.wait(self.base + 4, self.late)
        self.arrived(4)
        self.arrived(5)

    def passed(self):
        self.wait(self.base + 3, self.mirrored)


class Plane(Line):
    arrivals = Line.arrivals + [None, (3, None, 1), (1, None, 1), (2, 0, 1), (2, 1, 1)]
    number = [0, 2, 1, 2, 3, 4, 5, 6, 6, 6, 6]

    def __init__(self, send, wait, base, kind, ref, plus, minus, late, across):
        super().__init__(send, wait, base, kind, ref, plus, minus, late)
        self.across = across

    def cross(self, half):
        r = self.ref(0, half, 0)
        self.send(self.base + (7, 5)[half], r, r, self.across, self.kind)

    def start_half(self, half):
        if half == 0:
            self.put(0, (0, 0), self.plus)
            self.put(3, (0, 0), self.minus)
        else:
            self.put(2, (0, 1), self.minus)
            self.put(1, (0, 1), self.plus)

    def take_needed(self):
        self.wait(self.base + 5, self.ref(0, 1, 1))

    def other(self):
        self.wait(self.base + 7, self.ref(0, 0, 1))
        self.put(7, (0, None, 1), self.plus)
        self.put(8, (0, None, 1), self.minus)

    def near_half(self, half):
        if half == 0:
            self.take(0)
            self.put(4, (3, 0), self.plus)
        else:
            self.take(2)
            self.put(5, (1, 1), self.minus)

    def far(self):
        self.wait(self.base + 2, self.ref(3, None))
        self.take(4)
        self.put(9, (2, 0, 0), self.across)
        self.take(5)
        self.put(10, (2, 1, 0), self.across)

    def last(self):
        self.wait(self.base + 6, self.late)


def kernel(
    act_ref, grad_ref, out_ref,
    xall, give, gram_part, drecv, y1s, y1r, y2s, y2r, scaled,
    rowbuf, colbuf, sqcol, sq, low_out, low_in, obuf, csend, crecv, totbuf,
    ssem, rsem, lsem,
):
    tok, blk = lax.axis_index("tok"), lax.axis_index("blk")
    c, y, zl = tok % 2, (tok // 2) % 4, tok // 8
    x, zh = blk // 2, blk % 2

    def tok_of(zl_, y_, c_):
        return zl_ * 8 + y_ * 2 + c_

    def blk_of(x_, zh_):
        return x_ * 2 + zh_

    x_plus = (tok, blk_of((x + 1) % 4, zh))
    x_minus = (tok, blk_of((x + 3) % 4, zh))
    zh_mate = (tok, blk_of(x, 1 - zh))
    y_plus = (tok_of(zl, (y + 1) % 4, c), blk)
    y_minus = (tok_of(zl, (y + 3) % 4, c), blk)
    y_far = (tok_of(zl, (y + 2) % 4, c), blk)
    zl_mate = (tok_of(1 - zl, y, c), blk)
    z_cross = (tok_of(1 - zl, y, c), blk_of(x, 1 - zh))
    sibling = (tok_of(zl, y, 1 - c), blk)

    def place(to):
        return {"tok": to[0], "blk": to[1]}

    def row_of(s, y_):
        return ((y_ + s) % 2) * 2 + y_ // 2

    def keep(s, step):
        return row_of(s, (y + step) % 4)

    zh_of = (zh, 1 - zh)

    def out_tok(e, s):
        return 2 * (2 * keep(s, 0) + zh_of[e]) + c

    source_y = ((tok // 4) % 2) * 2 + (tok // 8 + blk // 4) % 2
    home = source_y == y

    def loads(src, dst, first):
        out = []
        for s in range(2):
            for k in range(2):
                cols = pl.ds(HALF * k + PART * s, PART)
                out.append(
                    pltpu.make_async_copy(
                        src.at[:, cols], dst(s).at[:, pl.ds(PART * k, PART)],
                        lsem.at[first + 2 * s + k],
                    )
                )
        return out

    def own_block(s):
        return xall.at[0, x, s]

    def give_block(s):
        return give.at[s]

    def all_loads(own_ref, give_ref):
        return loads(own_ref, own_block, 0) + loads(give_ref, give_block, 4)

    @pl.when(zl == 0)
    def _():
        for copy in all_loads(act_ref, grad_ref):
            copy.start()

    @pl.when(zl == 1)
    def _():
        for copy in all_loads(grad_ref, act_ref):
            copy.start()

    barrier = pltpu.get_barrier_semaphore()

    def greet(to):
        pl.semaphore_signal(barrier, inc=1, device_id=place(to), device_id_type=MESH)

    def greet_tok(j, carry):
        greet(((tok + j) % 16, blk))
        return carry

    lax.fori_loop(1, 16, greet_tok, 0)
    for to in (x_plus, x_minus, zh_mate, z_cross):
        greet(to)
    for copy in all_loads(act_ref, grad_ref):
        copy.wait()
    pl.semaphore_wait(barrier, 15 + 4)

    def remote(k, src, dst, to, kind):
        return pltpu.make_async_remote_copy(
            src_ref=src, dst_ref=dst, send_sem=ssem.at[kind], recv_sem=rsem.at[k],
            device_id=place(to), device_id_type=MESH,
        )

    def send(k, src, dst, to, kind):
        remote(k, src, dst, to, kind).start()

    def wait(k, dst):
        remote(k, dst, dst, sibling, 0).wait_recv()

    def left(kind, src):
        remote(0, src, src, sibling, kind).wait_send()

    token_half = (pl.ds(0, HALF), pl.ds(HALF, HALF))

    def x_line(s, t):
        def ref(step, half):
            return xall.at[t, (x + step) % 4, s, token_half[half]]

        return Line(
            send, wait, X_ID[s][t], TO_X, ref, x_plus, x_minus, xall.at[t, (x + 2) % 4, s]
        )

    lines = [[x_line(s, t) for t in range(2)] for s in range(2)]

    def z_first(s):
        send(Z_ID + s, give.at[s], xall.at[1, x, s], zl_mate, TO_Z)

    def z_rest(s):
        send(Z_ID + 2 + s, give.at[s], xall.at[1, 4, s], z_cross, TO_Z)
        send(Z_ID + 4 + s, xall.at[0, x, s], xall.at[0, 4, s], zh_mate, TO_Z)

    def z_first_take(s):
        wait(Z_ID + s, xall.at[1, x, s])

    def z_rest_take(s):
        wait(Z_ID + 2 + s, xall.at[1, 4, s])
        wait(Z_ID + 4 + s, xall.at[0, 4, s])

    def column_sums():
        for which, ref in ((zl, own_block), (1 - zl, give_block)):
            for s in range(2):
                values = ref(s)[...].astype(F32)
                total = jnp.sum(values * values, axis=0, keepdims=True)
                for k in range(2):
                    csend[which, :, HALF * k + PART * s : HALF * k + PART * (s + 1)] = total[
                        :, PART * k : PART * (k + 1)
                    ]

    def sum_copy(j):
        return remote(SUM_ID, csend, crecv.at[j], ((tok + j) % 16, blk), TO_SUM)

    def sums_start():
        def step(j, carry):
            sum_copy(j).start()
            return carry

        lax.fori_loop(1, 16, step, 0)

    total_to = [(tok, blk_of((x + j) % 4, zh)) for j in (1, 2, 3)] + [zh_mate]

    def total_copy(j):
        slot = x if j < 3 else 4
        return remote(TOTAL_ID, totbuf.at[x], totbuf.at[slot], total_to[j], TO_TOTAL)

    def totals_start():
        wait(SUM_ID, crecv.at[pl.ds(1, 15)])
        total = csend[...]
        for j in range(1, 16):
            total = total + crecv[j]
        totbuf[x] = total
        for j in range(4):
            total_copy(j).start()

    def totals_finish():
        wait(TOTAL_ID, totbuf.at[pl.ds(0, 4)])

    def gram(s, gs, begin, end):
        def step(i, carry):
            to = (x + 3 + i) % 4
            for g in gs:
                for s2 in range(2):
                    value = None
                    for t in range(2):
                        term = lax.dot_general(
                            xall[t, to, s], xall[t, (x, 4)[g], s2],
                            (((0,), (0,)), ((), ())), preferred_element_type=F32,
                        )
                        value = term if value is None else value + term
                    value = value.astype(BF16)
                    for k in range(2):
                        for k2 in range(2):
                            start = HALF * k2 + PART * s2
                            gram_part[s, g, to, k, :, start : start + PART] = value[
                                PART * k : PART * (k + 1), PART * k2 : PART * (k2 + 1)
                            ]
                d_copy(s, g, to).start()
            return carry

        lax.fori_loop(begin, end, step, 0)

    def d_copy(s, g, to):
        return remote(
            D_ID[s][g], gram_part.at[s, g, to, 1 - c], drecv.at[s, g, to], sibling, TO_SIBLING
        )

    halves = (pl.ds(0, PART // 2), pl.ds(PART // 2, PART // 2))

    def both(s, g, to, half):
        mine = gram_part[s, g, to, c, halves[half]].astype(F32)
        return mine + drecv[s, g, to, halves[half]].astype(F32)

    def reduce_first(s, g):
        y1, far = Y1_ID[s][g], keep(s, 2)
        wait(D_ID[s][g], drecv.at[s, g])
        y1s[s, g, 0] = both(s, g, far, 0).astype(BF16)
        send(y1, y1s.at[s, g, 0], y1r.at[s, g, 0], y_plus, TO_Y1)
        y1s[s, g, 1] = both(s, g, far, 1).astype(BF16)
        send(y1 + 1, y1s.at[s, g, 1], y1r.at[s, g, 1], y_minus, TO_Y1)

    def reduce_own(s, g):
        y2, up, down = Y2_ID[s][g], keep(s, 1), keep(s, 3)
        y2s[s, g, 0] = both(s, g, up, 1).astype(BF16)
        send(y2, y2s.at[s, g, 0], y2r.at[s, g, 0], y_plus, TO_Y2)
        y2s[s, g, 2] = both(s, g, down, 0).astype(BF16)
        send(y2, y2s.at[s, g, 2], y2r.at[s, g, 2], y_minus, TO_Y2)

    def reduce_middle(s, g):
        y1, y2, up, down = Y1_ID[s][g], Y2_ID[s][g], keep(s, 1), keep(s, 3)
        wait(y1, y1r.at[s, g, 0])
        y2s[s, g, 1] = (both(s, g, up, 0) + y1r[s, g, 0].astype(F32)).astype(BF16)
        send(y2, y2s.at[s, g, 1], y2r.at[s, g, 1], y_plus, TO_Y2)
        wait(y1 + 1, y1r.at[s, g, 1])
        y2s[s, g, 3] = (both(s, g, down, 1) + y1r[s, g, 1].astype(F32)).astype(BF16)
        send(y2, y2s.at[s, g, 3], y2r.at[s, g, 3], y_minus, TO_Y2)

    def eye(s, zh_, h):
        shape = (PART, BLOCK)
        r = lax.broadcasted_iota(jnp.int32, shape, 0) + HALF * c + PART * s
        k = lax.broadcasted_iota(jnp.int32, shape, 1)
        return (r + BLOCK * (2 * keep(s, 0) + zh_) == k + BLOCK * (2 * x + h)).astype(F32)

    def inverse(sums):
        return lax.rsqrt(sums / TOKENS + epsilon)

    def lane_block(block):
        return pl.ds(pl.multiple_of(block * BLOCK, BLOCK), BLOCK)

    def normalise(s, g):
        rows = pl.ds(pl.multiple_of(HALF * c + PART * s, PART), PART)
        inv_row = jnp.broadcast_to(inverse(totbuf[keep(s, 0), zl, :, rows]), (PART, PART))
        inv_row = jnp.concatenate([jnp.transpose(inv_row)] * 4, axis=1)
        wait(Y2_ID[s][g], y2r.at[s, g])
        inv_col = inverse(totbuf[(x, 4)[g], zl])
        low = both(s, g, keep(s, 0), 0) + y2r[s, g, 1].astype(F32) + y2r[s, g, 2].astype(F32)
        high = both(s, g, keep(s, 0), 1) + y2r[s, g, 0].astype(F32) + y2r[s, g, 3].astype(F32)
        total = jnp.concatenate([low, high], axis=0)
        damped = total / TOKENS * inv_row * inv_col + damping * eye(s, zh, zh_of[g])
        value = damped / divisor
        half = value.astype(BF16)
        rowbuf[zh, s, zh_of[g], :, lane_block(x)] = half
        if g == 0:
            scaled[0, s] = value
            colbuf[keep(s, 0), zh, c, s] = half
            if s == 0:
                cols[s][0].start()
            else:
                cols[s][0].start_direct(y_far)
        else:
            rows_of[s].cross(1)
            low_out[s] = (value - half.astype(F32)).astype(BF16)
        rows_of[s].start_half(g)

    def rows_start(s):
        rows_of[s].cross(0)
        if s == 0:
            low_send(s)

    def low_send(s):
        send(LOW_ID[s], low_out.at[s], low_in.at[s], zh_mate, TO_LOW)

    def partner(s):
        half = rowbuf[1 - zh, s, zh, :, lane_block(x)]
        colbuf[keep(s, 0), 1 - zh, c, s] = half
        if s == 0:
            cols[s][1].start()
        else:
            cols[s][1].start_direct(y_far)

    def partner_low(s):
        wait(LOW_ID[s], low_in.at[s])
        half = rowbuf[1 - zh, s, zh, :, lane_block(x)].astype(F32)
        scaled[1, s] = half + low_in[s].astype(F32)

    def row_plane(s):
        def ref(step, half, other=0):
            lanes = lane_block((x + step) % 4)
            r = rowbuf.at[zh_of[other], s]
            return r.at[:, :, lanes] if half is None else r.at[zh_of[(half + other) % 2], :, lanes]

        late = rowbuf.at[1 - zh, s, :, :, pl.ds(0, 3 * BLOCK)]
        return Plane(
            send, wait, ROW_ID[s], TO_ROWS, ref, x_plus, x_minus, late, zh_mate
        )

    def col_line(s, e):
        def ref(step, half):
            return colbuf.at[keep(s, step), zh_of[e], c, s, halves[half]]

        late = colbuf.at[0, zh_of[e], c, s]
        return Passed(
            send, wait, COL_ID[s][e], TO_COLS, ref, y_plus, y_minus, late, sibling, TO_PASS,
            colbuf.at[:, zh_of[e], 1 - c, s],
        )

    def sq_line(e):
        def ref(step, half):
            return sqcol.at[keep(half, step), zh_of[e], c, half]

        late = sqcol.at[0, zh_of[e], c]
        return Passed(
            send, wait, SQ_ID[e], TO_SQ, ref, y_plus, y_minus, late, sibling, TO_SQ_PASS,
            sqcol.at[:, zh_of[e], 1 - c],
        )

    rows_of = [row_plane(s) for s in range(2)]
    cols = [[col_line(s, e) for e in range(2)] for s in range(2)]
    sq_cols = [sq_line(e) for e in range(2)]

    def dot(e, p, right, lanes):
        return jnp.dot(
            rowbuf[zh_of[e], :, p].reshape(HALF, D // 2),
            right[:, p, :, :, :, lanes].reshape(D // 2, HALF),
            preferred_element_type=F32,
        )

    def over_lanes(body):
        def step(k, carry):
            body(pl.ds(pl.multiple_of(k * HALF, HALF), HALF))
            return carry

        lax.fori_loop(0, 2, step, 0)

    def square_first():
        def some(lanes):
            sq[0, :, lanes] = dot(0, zh, colbuf, lanes)

        over_lanes(some)

    def square(e):
        if e == 1:
            def some(lanes):
                sq[e, :, lanes] = dot(e, 0, colbuf, lanes) + dot(e, 1, colbuf, lanes)

            over_lanes(some)
            for s in range(2):
                sqcol[keep(s, 0), zh_of[e], c, s] = sq[e, PART * s : PART * (s + 1)].astype(BF16)
            sq_cols[e].start()
            return
        for s in range(2):
            rows = pl.ds(PART * s, PART)

            def some_rows(lanes):
                sq[e, rows, lanes] = sq[e, rows, lanes] + jnp.dot(
                    rowbuf[zh_of[e], s, 1 - zh],
                    colbuf[:, 1 - zh, :, :, :, lanes].reshape(D // 2, HALF),
                    preferred_element_type=F32,
                )

            over_lanes(some_rows)
            sqcol[keep(s, 0), zh_of[e], c, s] = sq[e, rows].astype(BF16)
            sq_cols[e].start_set(s)

    def combine(e):
        for s in range(2):
            scaled[e, s] = (
                4.0 * eye(s, zh_of[e], zh) - 6.0 * scaled[e, s]
                + 4.0 * sq[e, PART * s : PART * (s + 1)]
            )

    def cube_first():
        for e in range(2):
            def some(lanes):
                sq[e, :, lanes] = dot(e, zh, sqcol, lanes)

            over_lanes(some)

    def cube_second(e):
        def some(lanes):
            value = scaled[e, :, :, lanes].reshape(HALF, HALF) - sq[e, :, lanes]
            obuf[e, :, lanes] = (value - dot(e, 1 - zh, sqcol, lanes)).astype(BF16)

        over_lanes(some)
        for b in (0, 4, 2, 6, 1, 5, 3, 7):
            me = (out_tok(e, b // 4) == tok) & (blk == b)

            @pl.when(me)
            def _():
                out_ref[zl, :, lane_block(2 * x + zh)] = obuf[e, b * 32 : (b + 1) * 32]

            @pl.when(jnp.logical_not(me))
            def _():
                out_copy(e, b).start()

    def out_copy(e, b):
        return remote(
            OUT_ID, obuf.at[e, pl.ds(b * 32, 32)], out_ref.at[zl, :, lane_block(2 * x + zh)],
            (out_tok(e, b // 4), b), TO_OUT,
        )

    def emit():
        @pl.when(home)
        def _():
            wait(OUT_ID, out_ref.at[:, :, pl.ds(0, 15 * HALF)])
            left(TO_OUT, obuf.at[:, pl.ds(0, 15 * 16)])

        @pl.when(jnp.logical_not(home))
        def _():
            wait(OUT_ID, out_ref)
            left(TO_OUT, obuf)

    def all_left():
        left(TO_X, xall.at[:, pl.ds(0, 3)])
        left(TO_Z, xall.at[0, pl.ds(0, 3)])
        left(TO_SIBLING, gram_part.at[0])
        left(TO_Y1, y1s)
        left(TO_Y2, y2s)
        left(TO_ROWS, rowbuf.at[:, :, :, pl.ds(0, 112)])
        left(TO_LOW, low_out)
        left(TO_PASS, colbuf.at[pl.ds(0, 2)])
        left(TO_COLS, colbuf.at[pl.ds(0, 3), 0])
        left(TO_SQ, sqcol.at[pl.ds(0, 3), 0])
        left(TO_SQ_PASS, sqcol.at[pl.ds(0, 2)])
        left(TO_SUM, crecv.at[pl.ds(1, 15)])
        left(TO_TOTAL, totbuf.at[pl.ds(0, 4)])

    z_first(0)
    lines[0][0].start()
    column_sums()
    sums_start()
    z_first(1)
    z_rest(0)
    z_rest(1)
    lines[0][0].near()
    z_first_take(0)
    lines[0][1].start()
    totals_start()
    lines[0][1].near()
    lines[1][0].start()
    z_first_take(1)
    lines[1][1].start()
    lines[0][0].rest()
    lines[0][0].finish()
    lines[0][1].rest()
    lines[0][1].finish()
    gram(0, (0,), 0, 4)
    reduce_first(0, 0)
    reduce_own(0, 0)
    lines[1][0].near()
    z_rest_take(0)
    z_rest_take(1)
    gram(0, (1,), 0, 4)
    reduce_middle(0, 0)
    reduce_first(0, 1)
    reduce_own(0, 1)
    lines[1][1].near()
    totals_finish()
    reduce_middle(0, 1)
    normalise(0, 0)
    lines[1][0].rest()
    lines[1][1].rest()
    gram(1, (1, 0), 0, 3)
    normalise(0, 1)
    rows_start(0)
    lines[1][0].finish()
    lines[1][1].finish()
    gram(1, (1, 0), 3, 4)
    reduce_first(1, 1)
    reduce_first(1, 0)
    reduce_own(1, 1)
    reduce_own(1, 0)
    rows_of[0].near_half(0)
    cols[0][0].near()
    reduce_middle(1, 1)
    rows_of[0].near_half(1)
    reduce_middle(1, 0)
    rows_of[0].take_needed()
    partner(0)
    rows_of[0].other()
    cols[0][0].rest()
    rows_of[0].far()
    normalise(1, 1)
    normalise(1, 0)
    rows_start(1)
    cols[0][1].near()
    cols[0][0].finish()
    rows_of[1].take_needed()
    partner(1)
    cols[1][0].near_direct()
    rows_of[1].near_half(1)
    cols[0][1].rest()
    rows_of[1].near_half(0)
    rows_of[1].other()
    cols[1][0].rest()
    cols[1][1].near_direct()
    cols[0][1].finish()
    cols[1][0].finish()
    rows_of[1].far()
    low_send(1)
    cols[0][0].passed()
    cols[1][0].passed()
    square_first()
    cols[1][1].rest()
    cols[1][1].finish()
    cols[0][1].passed()
    cols[1][1].passed()
    square(0)
    rows_of[0].last()
    rows_of[1].last()
    square(1)
    sq_cols[0].near()
    combine(0)
    partner_low(0)
    partner_low(1)
    combine(1)
    sq_cols[1].near()
    sq_cols[0].rest()
    sq_cols[0].finish()
    sq_cols[1].rest()
    sq_cols[0].passed()
    cube_first()
    sq_cols[1].finish()
    sq_cols[1].passed()
    cube_second(0)
    cube_second(1)
    all_left()
    emit()


def body(activations, out_grads):
    hbm = pl.BlockSpec(memory_space=pltpu.HBM)
    vmem = pl.BlockSpec(memory_space=pltpu.VMEM)
    part = (PART, BLOCK)
    half_part = (PART // 2, BLOCK)
    scratch = [
        pltpu.VMEM((2, 5, 2, BLOCK, HALF), BF16),
        pltpu.VMEM((2, BLOCK, HALF), BF16),
        pltpu.VMEM((2, 2, 4, 2, *part), BF16),
        pltpu.VMEM((2, 2, 4, *part), BF16),
        pltpu.VMEM((2, 2, 2, *half_part), BF16),
        pltpu.VMEM((2, 2, 2, *half_part), BF16),
        pltpu.VMEM((2, 2, 4, *half_part), BF16),
        pltpu.VMEM((2, 2, 4, *half_part), BF16),
        pltpu.VMEM((2, 2, *part), F32),
        pltpu.VMEM((2, 2, 2, PART, D // 2), BF16),
        pltpu.VMEM((4, 2, 2, 2, *part), BF16),
        pltpu.VMEM((4, 2, 2, 2, *part), BF16),
        pltpu.VMEM((2, HALF, BLOCK), F32),
        pltpu.VMEM((2, *part), BF16),
        pltpu.VMEM((2, *part), BF16),
        pltpu.VMEM((2, HALF, BLOCK), BF16),
        pltpu.VMEM((2, 1, BLOCK), F32),
        pltpu.VMEM((16, 2, 1, BLOCK), F32),
        pltpu.VMEM((5, 2, 1, BLOCK), F32),
        pltpu.SemaphoreType.DMA((N_TO,)),
        pltpu.SemaphoreType.DMA((N_ID,)),
        pltpu.SemaphoreType.DMA((8,)),
    ]
    out = pl.pallas_call(
        kernel,
        out_shape=pltpu.VMEM((2, 32, D), BF16),
        in_specs=[hbm, hbm],
        out_specs=vmem,
        scratch_shapes=scratch,
        compiler_params=pltpu.CompilerParams(
            collective_id=0, has_side_effects=True, vmem_limit_bytes=60 * 1024 * 1024
        ),
    )(activations, out_grads)
    return out[0].astype(F32), out[1].astype(F32)


def solution(mesh):
    placed = (P("tok", "blk"), P("tok", "blk"))
    return jax.shard_map(
        body,
        mesh=mesh,
        in_specs=placed,
        out_specs=(P(("tok", "blk"), None), P(("tok", "blk"), None)),
        check_vma=False,
    )
```
